256 devices in a mesh: ta: 32 (over z, y_lo, core), gz: 4 (over x), gy: 2 (over y_hi).
Axes of the slice: x: 4, y: 4 (y_hi: 2, y_lo: 2; y = y_hi * 2 + y_lo), z: 8, core: 2. Of those that a mesh axis runs over, the one named last changes fastest.
Arguments:
- right_side: float32 [256, 32, 32, 128], P('ta', 'gz', 'gy'), may hold values from -12 to 12, as said below
- mass_field: float32 [256, 32, 32, 128], P('ta', 'gz', 'gy'), may hold values from 0.05 to 0.8
Outputs:
- solution: float32 [256, 32, 32, 128], P('ta', 'gz', 'gy')
- residual: float32 [256, 32, 32, 128], P('ta', 'gz', 'gy')
The draws below stay inside these ranges and needn't reach their ends.
Inputs may be any that keep to these rules, and one draw needn't show every extreme that they name: right_side is twice a field constant on aligned blocks of 8 x 8 x 8 x 8 sites plus site-by-site noise, each part within -4 to 4.
All inputs are finite; a program needn't handle non-finite values.
Results may differ from the reference program's by a relative error of at most 0.0003.
Values sent between devices are 32-bit elements.
A program may use at most 128 MiB of HBM per device.

```python
import math
import jax
import jax.numpy as jnp

LEVELS = 4
PRE = 2
POST = 2
COARSE_STEPS = 4
NT = 256
NZ = 32
NY = 32
NX = 128


def draw_right_side(key, part):
    coarse_key = jax.random.fold_in(key, 11)
    detail_key = jax.random.fold_in(key, 23)
    coarse_shape = (NT // 8, NZ // 8, NY // 8, NX // 8)
    whole_shape = (NT, NZ, NY, NX)
    coarse = jnp.clip(jax.random.normal(coarse_key, coarse_shape, jnp.float32), -4.0, 4.0)
    detail = jnp.clip(jax.random.normal(detail_key, whole_shape, jnp.float32), -4.0, 4.0)
    filled = coarse
    for dimension in range(4):
        filled = jnp.repeat(filled, 8, axis=dimension)
    return (2.0 * filled + detail).astype(jnp.float32)


def shard_levels(key, extent, shards, low, top_value):
    loudness = 1.0
    for position, blocks in shards:
        steps = jax.random.uniform(jax.random.fold_in(jax.random.fold_in(key, 6), position), (blocks,), jnp.float32, low / len(shards), top_value / len(shards))
        loudness = loudness * jnp.repeat(jnp.exp(steps), extent[position] // blocks).reshape((-1,) + (1,) * (len(extent) - 1 - position))
    return loudness


def setup_inputs(seed: int = 0) -> dict:
    keys = jax.random.split(jax.random.key(seed), 3)
    return {
        "right_side": draw_right_side(jax.random.fold_in(keys[2], 71), 0),
        "mass_field": jnp.clip(jnp.exp(math.log(0.8) - 2.7725887 * jax.random.uniform(keys[1], (NT, NZ, NY, NX), jnp.float32) ** shard_levels(keys[1], (NT, NZ, NY, NX), ((0, 32), (1, 4), (2, 2)), -0.2, 0.2)), 0.05, 0.8),
    }


DAMPING = 0.7


def neighbours(values):
    summed = jnp.zeros_like(values)
    for dimension in range(4):
        summed = summed + jnp.roll(values, 1, dimension) + jnp.roll(values, -1, dimension)
    return summed


def operate(values, mass_level, coarse_level):
    factor = 0.5 ** coarse_level
    return factor * (8.0 * values - neighbours(values)) + mass_level * values


def coarsen(values):
    first, second, third, fourth = values.shape
    blocks = values.reshape(first // 2, 2, second // 2, 2, third // 2, 2, fourth // 2, 2)
    return jnp.mean(blocks, axis=(1, 3, 5, 7))


def refine(values):
    for dimension in range(4):
        values = jnp.repeat(values, 2, axis=dimension)
    return values


def sweeps(values, source, mass_level, coarse_level, count_steps):
    diagonal = 8.0 * (0.5 ** coarse_level) + mass_level
    for sweep_no in range(count_steps):
        values = values + DAMPING * (source - operate(values, mass_level, coarse_level)) / diagonal
    return values


def cycle(source, mass_level, coarse_level):
    diagonal = 8.0 * (0.5 ** coarse_level) + mass_level
    values = DAMPING * source / diagonal
    if coarse_level == LEVELS - 1:
        return sweeps(values, source, mass_level, coarse_level, COARSE_STEPS - 1)
    values = sweeps(values, source, mass_level, coarse_level, PRE - 1)
    remainder = source - operate(values, mass_level, coarse_level)
    correction = cycle(coarsen(remainder), coarsen(mass_level), coarse_level + 1)
    values = values + refine(correction)
    return sweeps(values, source, mass_level, coarse_level, POST)


def reference(right_side, mass_field):
    solution = cycle(right_side, mass_field, 0)
    residual = right_side - operate(solution, mass_field, 0)
    return solution, residual
```

```python
import functools

import jax
import jax.numpy as jnp
from jax import lax
from jax.experimental import pallas as pl
from jax.experimental.pallas import tpu as pltpu
from jax.sharding import PartitionSpec as P

DAMPING = 0.7
KEEP = 1.0 - DAMPING
MESH = pl.DeviceIdType.MESH


def rolled(values, shift, axis):
    return pltpu.roll(values, shift % values.shape[axis], axis)


def pair_swap(values, step, axis):
    index = lax.broadcasted_iota(jnp.int32, values.shape, axis)
    return jnp.where((index // step) % 2 == 0, rolled(values, -step, axis), rolled(values, step, axis))


def z_pairs(summed):
    count, rows, lanes = summed.shape
    summed = summed.reshape(count // 2, 2, rows, lanes)
    return summed[:, 0] + summed[:, 1]


def refined_z(slab):
    return jnp.repeat(slab, 2, axis=0)


def shifted_z(slab, forward):
    if forward:
        return jnp.concatenate([slab[-1:], slab[:-1]], axis=0)
    return jnp.concatenate([slab[1:], slab[:1]], axis=0)


def kernel(sizes, s_hbm, m_hbm, sol_ref, res_ref, *scratch):
    nta, ngz, ngy = sizes
    (g0, v0a, v0b, v0w, v0x, v0s, y0, ys0, fold,
     s1, m1, g1, v1a, v1b, v1w, v1x, e1, e2,
     m2, s2, g2, u2, w2, m3, s3,
     f0s, f0r, f1s, f1r, fxs, fxr, gsend, grecv, s_ref, m_ref, loaded) = scratch
    size_t, size_z, rows, lanes = s_ref.shape
    size_t1, size_z1, rows1 = size_t // 2, size_z // 2, rows // 2
    part_t, part_z, rows2 = size_t // 4, size_z // 4, rows // 4
    stages = plan(nta, ngz)
    slots = {cell: number for number, cell in enumerate(stages["source"])}
    ta, gz, gy = lax.axis_index("ta"), lax.axis_index("gz"), lax.axis_index("gy")

    first_up = lax.min(ta, 1)

    def device(dt, dz, dy):
        return {
            "ta": lax.rem(ta + dt + nta, nta),
            "gz": lax.rem(gz + dz + ngz, ngz),
            "gy": lax.rem(gy + dy + ngy, ngy),
        }

    near = [(dt, dz, dy) for dt in (-1, 0, 1) for dz in (-1, 0, 1) for dy in range(ngy)]
    centred = lambda d, n: (d + n // 2) % n - n // 2
    across = sorted(
        (cell for cell in slots if cell != (0, 0)),
        key=lambda c: -(abs(centred(c[0], nta)) + 2 * abs(centred(c[1], ngz))),
    )
    loads = []
    for t in range(size_t):
        loads.append((
            pltpu.make_async_copy(m_hbm.at[pl.ds(t, 1)], m_ref.at[pl.ds(t, 1)], loaded.at[0, t]),
            pltpu.make_async_copy(s_hbm.at[pl.ds(t, 1)], s_ref.at[pl.ds(t, 1)], loaded.at[1, t]),
        ))
    met = sorted({(dt % nta, dz % ngz, dy % ngy) for dt, dz, dy in near + [(-t, -z, 0) for t, z in across]} - {(0, 0, 0)})
    barrier = pltpu.get_barrier_semaphore()
    for offset in met:
        pl.semaphore_signal(barrier, inc=1, device_id=device(*offset), device_id_type=MESH)
    for t in [0, size_t - 1] + list(range(1, size_t - 1)):
        for load in loads[t]:
            load.start()

    def send(moves, sends, receives):
        copies = [
            pltpu.make_async_remote_copy(
                src_ref=source, dst_ref=target, send_sem=sends(place), recv_sem=receives(place),
                device_id=device(*offset), device_id_type=MESH,
            )
            for place, source, target, offset in moves
        ]
        for copy in copies:
            copy.start()
        sent.extend(copies)
        return copies

    def finish(copies):
        for copy in copies:
            copy.wait_recv()

    sent = []

    def finish_sends(copies):
        for copy in copies:
            copy.wait_send()

    inner_t, inner_z = pl.ds(1, size_t), pl.ds(1, size_z)

    def send0(number, moves):
        return send(moves, lambda place: f0s.at[number, place], lambda place: f0r.at[number, place])

    def exchange_t(number, field):
        moves = []
        for up in (first_up, 1 - first_up):
            here, there = pl.ds(1 + (size_t - 1) * up, 1), pl.ds((size_t + 1) * (1 - up), 1)
            moves.append((up, field.at[here, inner_z], field.at[there, inner_z], (2 * up - 1, 0, 0)))
        return send0(number, moves)

    def exchange_sides(number, field, faces, halos):
        return send0(number, [
            (2, field.at[inner_t, pl.ds(size_z, 1)], field.at[inner_t, pl.ds(0, 1)], (0, 1, 0)),
            (3, field.at[inner_t, pl.ds(1, 1)], field.at[inner_t, pl.ds(size_z + 1, 1)], (0, -1, 0)),
            (4, faces.at[1], halos.at[0], (0, 0, 1)),
            (5, faces.at[0], halos.at[1], (0, 0, -1)),
        ])

    def around(field, part, dys):
        own_t, own_z = pl.ds(2, size_t1), pl.ds(2, size_z1)

        def span(size, deep, up):
            return pl.ds(2 + (size - deep) * up, deep), pl.ds(2 + size - (size + deep) * up, deep)

        moves = []
        for up in (first_up, 1 - first_up):
            here, there = span(size_t1, 2, up)
            for dy in dys:
                moves.append((
                    8 * dy + up, field.at[(here, own_z) + part], field.at[(there, own_z) + part],
                    (2 * up - 1, 0, dy),
                ))
        for up in (1, 0):
            here_t, there_t = span(size_t1, 1, up)
            for up_z in (1, 0):
                here_z, there_z = span(size_z1, 1, up_z)
                for dy in dys:
                    moves.append((
                        8 * dy + 2 + 2 * up + up_z,
                        field.at[(here_t, here_z) + part], field.at[(there_t, there_z) + part],
                        (2 * up - 1, 2 * up_z - 1, dy),
                    ))
        for up in (1, 0):
            here, there = span(size_z1, 2, up)
            for dy in dys:
                moves.append((
                    8 * dy + 6 + up, field.at[(own_t, here) + part], field.at[(own_t, there) + part],
                    (0, 2 * up - 1, dy),
                ))
        return moves

    def spread1(number, field):
        own = field.at[pl.ds(2, size_t1), pl.ds(2, size_z1), pl.ds(gy, 1)]
        moves = around(field, (pl.ds(gy, 1),), range(ngy))
        moves += [(8 * ngy + dy - 1, own, own, (0, 0, dy)) for dy in range(1, ngy)]
        return send(moves, lambda place: f1s.at[number, place], lambda place: f1r.at[number, place])

    def gather(number, field):
        own = field.at[slots[0, 0]]
        return send(
            [(slots[cell], own, field.at[slots[cell]], (-cell[0], -cell[1], 0)) for cell in across],
            lambda place: gsend.at[number, place], lambda place: grecv.at[number, place],
        )

    def put(field, faces, t, slab):
        field[t + 1, pl.ds(1, size_z)] = slab
        faces[0, t] = slab[:, :1]
        faces[1, t] = slab[:, rows - 1:]

    def sum0(field, halos, t):
        slab = field[t + 1, pl.ds(1, size_z)]
        row = lax.broadcasted_iota(jnp.int32, slab.shape, 1)
        summed = field[t, pl.ds(1, size_z)] + field[t + 2, pl.ds(1, size_z)]
        summed = summed + field[t + 1, pl.ds(0, size_z)] + field[t + 1, pl.ds(2, size_z)]
        summed = summed + jnp.where(row == 0, halos[0, t], rolled(slab, 1, 1))
        summed = summed + jnp.where(row == rows - 1, halos[1, t], rolled(slab, -1, 1))
        return slab, summed + rolled(slab, 1, 2) + rolled(slab, -1, 2)

    def halved(summed, place, step):
        count, high, _ = summed.shape
        view = fold.at[place, pl.ds(0, count)]
        view[...] = summed
        summed = view[:, pl.ds(0, high // 2, stride=2), :] + view[:, pl.ds(1, high // 2, stride=2), :]
        return (summed + pair_swap(summed, step, 2)) * 0.0625

    def doubled(slab, place):
        count, high, _ = slab.shape
        view = fold.at[place, pl.ds(0, count)]
        view[:, pl.ds(0, high, stride=2), :] = slab
        view[:, pl.ds(1, high, stride=2), :] = slab
        return view[...]

    full = ngy * rows1

    def near1(radius):
        for a in range(2 - radius, 2 + size_t1 + radius):
            reach = radius - max(2 - a, a - 1 - size_t1, 0)
            yield a, 2 - reach, size_z1 + 2 * reach

    def read1(field, a, b, count):
        return field[a, pl.ds(b, count)].reshape(count, full, lanes)

    def write1(field, a, b, slab):
        field[a, pl.ds(b, slab.shape[0])] = slab.reshape(slab.shape[0], ngy, rows1, lanes)

    def sum1(field, a, b, count):
        slab = read1(field, a, b, count)
        summed = read1(field, a - 1, b, count) + read1(field, a + 1, b, count)
        summed = summed + read1(field, a, b - 1, count) + read1(field, a, b + 1, count)
        summed = summed + rolled(slab, 1, 1) + rolled(slab, -1, 1)
        return slab, summed + rolled(slab, 2, 2) + rolled(slab, -2, 2)

    def sweep1(field, out, radius):
        for a, b, count in near1(radius):
            slab, summed = sum1(field, a, b, count)
            fresh = KEEP * slab + read1(g1, a, b, count) * (read1(s1, a, b, count) + 0.5 * summed)
            write1(out, a, b, fresh)

    def packed(out, slabs):
        parts = [slab[z] for slab in slabs for z in range(part_z)]
        lane = lax.broadcasted_iota(jnp.int32, parts[0].shape, 1)
        values = parts[0]
        for k in range(1, len(parts)):
            values = jnp.where(lane % 4 == k, parts[k], values)
        out[slots[0, 0]] = values

    inside = list(range(1, size_t - 1))
    ends = [0, size_t - 1]

    def first0(ts):
        for t in ts:
            for load in loads[t]:
                load.wait()
            weight = DAMPING / (8.0 + m_ref[t])
            g0[t] = weight
            put(v0a, ys0.at[0], t, weight * s_ref[t])

    first0(ends + inside)
    pl.semaphore_wait(barrier, len(met))
    over_t = exchange_t(0, v0a)
    sides = exchange_sides(0, v0a, ys0.at[0], y0.at[0])
    for t in range(size_t1):
        mean = halved(z_pairs(m_ref[2 * t] + m_ref[2 * t + 1]), t, 1)
        m1[t + 2, pl.ds(2, size_z1), gy] = mean
    mass_copies = spread1(0, m1)

    def sweep0(field, halos, out, faces, ts, also=None):
        for t in ts:
            slab, summed = sum0(field, halos, t)
            fresh = KEEP * slab + g0[t] * (s_ref[t] + summed)
            put(out, faces, t, fresh)
            if also is not None:
                also[t] = fresh

    finish(sides)
    sweep0(v0a, y0.at[0], v0b, ys0.at[1], inside)
    finish(over_t)
    sweep0(v0a, y0.at[0], v0b, ys0.at[1], ends)
    over_t = exchange_t(1, v0b)
    sides = exchange_sides(1, v0b, ys0.at[1], y0.at[1])
    finish(mass_copies)
    for a, b, count in near1(2):
        write1(g1, a, b, DAMPING / (4.0 + read1(m1, a, b, count)))

    def to_level2(slabs):
        return [
            halved(z_pairs(slabs[2 * t] + slabs[2 * t + 1]), t, 2) for t in range(part_t)
        ]

    packed(m2, to_level2([read1(m1, 2 + t, 2, size_z1) for t in range(size_t1)]))
    mass_copies = gather(0, m2)

    def remainder0(ts):
        for t in ts:
            remainder = []
            for odd in range(2):
                slab, summed = sum0(v0b, y0.at[1], 2 * t + odd)
                remainder.append(s_ref[2 * t + odd] + summed - (8.0 + m_ref[2 * t + odd]) * slab)
            s1[t + 2, pl.ds(2, size_z1), gy] = halved(z_pairs(remainder[0] + remainder[1]), t, 1)

    finish(sides)
    remainder0(range(1, size_t1 - 1))
    finish(over_t)
    remainder0((0, size_t1 - 1))
    source_copies = spread1(1, s1)
    finish(mass_copies)
    for cell in stages["source"]:
        g2[slots[cell]] = DAMPING / (2.0 + m2[slots[cell]])
    for cell in stages["coarse"][3]:
        m3[slots[cell]] = DAMPING / (1.0 + coarsened3(m2[slots[cell]]))
    finish(source_copies)

    for a, b, count in near1(2):
        write1(v1a, a, b, read1(g1, a, b, count) * read1(s1, a, b, count))
    sweep1(v1a, v1b, 1)
    remainder = []
    for a, b, count in near1(0):
        slab, summed = sum1(v1b, a, b, count)
        remainder.append(
            read1(s1, a, b, count) + 0.5 * summed - (4.0 + read1(m1, a, b, count)) * slab
        )
    packed(s2, to_level2(remainder))
    finish(gather(1, s2))

    def around2(cell):
        t, z = cell
        return [((t + dt) % nta, (z + dz) % ngz) for dt, dz in ((-1, 0), (1, 0), (0, -1), (0, 1))]

    def sum2(field, cell):
        slab = field[slots[cell]]
        before_t, after_t, before_z, after_z = [
            slab + field[slots[other]] if other in slots else slab for other in around2(cell)
        ]
        lane = lane_of(slab)
        summed = jnp.where(lane % 4 >= 2, rolled(after_t, 2, 1), rolled(before_t, -2, 1))
        summed = summed + jnp.where(lane % 2 == 1, rolled(after_z, 1, 1), rolled(before_z, -1, 1))
        summed = summed + rolled(slab, 1, 0) + rolled(slab, -1, 0)
        return slab, summed + rolled(slab, 4, 1) + rolled(slab, -4, 1)

    def sweep2(field, out, cells):
        for cell in cells:
            slab, summed = sum2(field, cell)
            at = slots[cell]
            out[at] = KEEP * slab + g2[at] * (s2[at] + 0.25 * summed)

    for cell in stages["source"]:
        at = slots[cell]
        u2[at] = g2[at] * s2[at]
        w2[at] = u2[at]
    sweep2(u2, w2, stages["swept"])
    values = {}
    for cell in stages["coarse"][3]:
        slab, summed = sum2(w2, cell)
        at = slots[cell]
        source = coarsened3(s2[at] + 0.25 * summed - (2.0 + m2[at]) * slab)
        s3[at] = source
        values[cell] = m3[at] * source
    for steps in (2, 1, 0):
        fresh = {}
        for cell in stages["coarse"][steps]:
            slab = values[cell]
            before_t, after_t, before_z, after_z = [values[other] for other in around2(cell)]
            summed = before_t + after_t + before_z + after_z
            summed = summed + rolled(slab, 2, 0) + rolled(slab, -2, 0)
            summed = summed + rolled(slab, 8, 1) + rolled(slab, -8, 1)
            fresh[cell] = KEEP * slab + m3[slots[cell]] * (s3[slots[cell]] + 0.125 * summed)
        values = fresh
    for cell in stages["base"]:
        w2[slots[cell]] = w2[slots[cell]] + refined3(values[cell])
    for cell in stages["base"]:
        u2[slots[cell]] = w2[slots[cell]]
    sweep2(w2, u2, stages["first"])
    sweep2(u2, w2, stages["last"])

    def correct1(t, z):
        piece = piece2(w2[slots[t // 2 % nta, z // 2 % ngz]], t % 2, z % 2)
        e2[t + 1, z + 1, pl.ds(0, full // 2, stride=2), :] = piece
        e2[t + 1, z + 1, pl.ds(1, full // 2, stride=2), :] = piece

    for t in range(-1, part_t + 1):
        for z in range(-1, part_z + 1):
            if 0 <= t < part_t or 0 <= z < part_z:
                correct1(t, z)
    for a, b, count in near1(1):
        low, high = b // 2, (b + count + 1) // 2
        fine = refined_z(e2[a // 2, pl.ds(low, high - low)])[b - 2 * low:][:count]
        write1(v1w, a, b, read1(v1b, a, b, count) + fine)
    sweep1(v1w, v1x, 0)
    finish(send(
        around(v1x, (), (0,)), lambda place: fxs.at[place], lambda place: fxr.at[place],
    ))
    sweep1(v1x, e1, 1)

    under = lax.rem(gy + ngy - 1, ngy)
    over = lax.rem(gy + 1, ngy)
    def corrected0(layers):
        for at_t in layers:
            own = [p for p in (2 * at_t - 3, 2 * at_t - 2) if 1 <= p <= size_t]
            if not own:
                p = 0 if at_t == 1 else size_t + 1
                fine = refined_z(doubled(e1[at_t, pl.ds(2, size_z1), gy], 0))
                v0w[p, inner_z] = v0b[p, inner_z] + fine
                continue
            fine = refined_z(doubled(e1[at_t, pl.ds(1, size_z1 + 2), gy], at_t % 4))
            fine = fine[1:1 + size_z + 2]
            low = refined_z(e1[at_t, pl.ds(2, size_z1), under, pl.ds(rows1 - 1, 1)])
            high = refined_z(e1[at_t, pl.ds(2, size_z1), over, pl.ds(0, 1)])
            for p in own:
                v0w[p] = v0b[p] + fine
                y0[2, 0, p - 1] = y0[1, 0, p - 1] + low
                y0[2, 1, p - 1] = y0[1, 1, p - 1] + high

    corrected0((1, 2, size_t1 + 1, size_t1 + 2))
    sweep0(v0w, y0.at[2], v0x, ys0.at[2], ends)
    over_t = exchange_t(2, v0x)
    corrected0(range(3, size_t1 + 1))
    sweep0(v0w, y0.at[2], v0x, ys0.at[2], inside)
    sides = exchange_sides(2, v0x, ys0.at[2], y0.at[3])
    finish(sides)
    sweep0(v0x, y0.at[3], v0s, ys0.at[3], inside, sol_ref)
    finish(over_t)
    sweep0(v0x, y0.at[3], v0s, ys0.at[3], ends, sol_ref)
    earlier = len(sent)
    over_t = exchange_t(3, v0s)
    sides = exchange_sides(3, v0s, ys0.at[3], y0.at[4])
    finish_sends(sent[:earlier])

    def residual(ts):
        for t in ts:
            slab, summed = sum0(v0s, y0.at[4], t)
            res_ref[t] = s_ref[t] + summed - (8.0 + m_ref[t]) * slab

    finish(sides)
    residual(inside)
    finish(over_t)
    residual(ends)
    finish_sends(sent[earlier:])


def lane_of(values):
    return lax.broadcasted_iota(jnp.int32, values.shape, 1)


def coarsened3(values):
    for step in (1, 2, 4):
        values = values + rolled(values, -step, 1)
    return (values + rolled(values, -1, 0)) * 0.0625


def refined3(values):
    row = lax.broadcasted_iota(jnp.int32, values.shape, 0)
    values = jnp.where((lane_of(values) % 8 == 0) & (row % 2 == 0), values, 0.0)
    for step in (1, 2, 4):
        values = values + rolled(values, step, 1)
    return values + rolled(values, 1, 0)


def piece2(values, odd_t, odd_z):
    values = jnp.where(lane_of(values) % 4 == 2 * odd_t + odd_z, values, 0.0)
    values = values + rolled(values, -1 if odd_z else 1, 1)
    return values + rolled(values, -2 if odd_t else 2, 1)


def grown(cells, steps, count_t, count_z):
    for _ in range(steps):
        cells = cells | {
            ((t + dt) % count_t, (z + dz) % count_z)
            for t, z in cells for dt, dz in ((-1, 0), (1, 0), (0, -1), (0, 1))
        }
    return cells


def plan(nta, ngz):
    sites = lambda cells, steps: grown(cells, steps, 2 * nta, 2 * ngz)
    blocks = lambda cells: {(t // 2, z // 2) for t, z in cells}
    inner = lambda cells: {(2 * t + a, 2 * z + b) for t, z in cells for a in (0, 1) for b in (0, 1)}
    last = sites(inner({(0, 0)}), 1)
    first, base = sites(last, 1), sites(last, 2)
    coarse = [grown(blocks(base), steps, nta, ngz) for steps in range(4)]
    swept = sites(inner(coarse[3]), 1) | base
    ordered = lambda cells: sorted(cells, key=lambda c: ((c[0] + nta // 2) % nta, (c[1] + ngz // 2) % ngz))
    return {
        "last": ordered(blocks(last)), "first": ordered(blocks(first)), "base": ordered(blocks(base)),
        "coarse": [ordered(cells) for cells in coarse], "swept": ordered(blocks(swept)),
        "source": ordered(blocks(sites(swept, 1))),
    }


def per_device(sizes, right_side, mass_field):
    nta, ngz, ngy = sizes
    size_t, size_z, rows, lanes = right_side.shape
    size_t1, size_z1, rows1 = size_t // 2, size_z // 2, rows // 2
    part_t, part_z, rows2 = size_t // 4, size_z // 4, rows // 4
    vmem = lambda *shape: pltpu.VMEM(shape, jnp.float32)
    dma = lambda *shape: pltpu.SemaphoreType.DMA(shape)
    padded0 = vmem(size_t + 2, size_z + 2, rows, lanes)
    padded1 = vmem(size_t1 + 4, size_z1 + 4, ngy, rows1, lanes)
    window = len(plan(nta, ngz)["source"])
    packs = vmem(window, rows2 * ngy, lanes)
    spreads = 8 * ngy + ngy - 1
    scratch = [
        vmem(size_t, size_z, rows, lanes), padded0, padded0, padded0, padded0, padded0,
        vmem(5, 2, size_t, size_z, 1, lanes), vmem(4, 2, size_t, size_z, 1, lanes),
        vmem(max(size_t1, part_t + 2), size_z, max(rows, ngy * rows1), lanes),
        *[padded1] * 8, vmem(part_t + 2, part_z + 2, ngy * rows1, lanes),
        *[packs] * 7,
        dma(4, 6), dma(4, 6), dma(2, spreads), dma(2, spreads), dma(8), dma(8),
        dma(2, window), dma(2, window),
        vmem(size_t, size_z, rows, lanes), vmem(size_t, size_z, rows, lanes), dma(2, size_t),
    ]
    block = jax.ShapeDtypeStruct(right_side.shape, jnp.float32)
    return pl.pallas_call(
        functools.partial(kernel, sizes),
        out_shape=(block, block),
        in_specs=[pl.BlockSpec(memory_space=pltpu.HBM)] * 2,
        out_specs=(pl.BlockSpec(memory_space=pltpu.VMEM),) * 2,
        scratch_shapes=scratch,
        compiler_params=pltpu.CompilerParams(
            collective_id=0, has_side_effects=True, vmem_limit_bytes=48 * 1024 * 1024
        ),
    )(right_side, mass_field)


def solution(mesh):
    sizes = tuple(mesh.shape[axis] for axis in ("ta", "gz", "gy"))
    spec = P("ta", "gz", "gy", None)
    return jax.shard_map(
        functools.partial(per_device, sizes),
        mesh=mesh,
        in_specs=(spec, spec),
        out_specs=(spec, spec),
        check_vma=False,
    )
```

```python
import functools

import jax
import jax.numpy as jnp
from jax import lax
from jax.experimental import pallas as pl
from jax.experimental.pallas import tpu as pltpu
from jax.sharding import PartitionSpec as P

DAMPING = 0.7
KEEP = 1.0 - DAMPING
MESH = pl.DeviceIdType.MESH


def rolled(values, shift, axis):
    return pltpu.roll(values, shift % values.shape[axis], axis)


def pair_swap(values, step, axis):
    index = lax.broadcasted_iota(jnp.int32, values.shape, axis)
    return jnp.where((index // step) % 2 == 0, rolled(values, -step, axis), rolled(values, step, axis))


def z_pairs(summed):
    count, rows, lanes = summed.shape
    summed = summed.reshape(count // 2, 2, rows, lanes)
    return summed[:, 0] + summed[:, 1]


def refined_z(slab):
    return jnp.repeat(slab, 2, axis=0)


def shifted_z(slab, forward):
    if forward:
        return jnp.concatenate([slab[-1:], slab[:-1]], axis=0)
    return jnp.concatenate([slab[1:], slab[:1]], axis=0)


def kernel(sizes, s_hbm, m_hbm, sol_ref, res_ref, *scratch):
    nta, ngz, ngy = sizes
    (g0, v0a, v0b, v0w, v0x, v0s, y0, ys0, fold,
     s1, m1, g1, v1a, v1b, v1w, v1x, e1, e2,
     m2, s2, g2, u2, w2, m3, s3,
     f0s, f0r, f1s, f1r, fxs, fxr, gsend, grecv, s_ref, m_ref, loaded) = scratch
    size_t, size_z, rows, lanes = s_ref.shape
    size_t1, size_z1, rows1 = size_t // 2, size_z // 2, rows // 2
    part_t, part_z, rows2 = size_t // 4, size_z // 4, rows // 4
    stages = plan(nta, ngz)
    slots = {cell: number for number, cell in enumerate(stages["source"])}
    ta, gz, gy = lax.axis_index("ta"), lax.axis_index("gz"), lax.axis_index("gy")

    places = {}

    def place_of(axis, at, step, count):
        key = axis, step % count
        if key not in places:
            places[key] = at if key[1] == 0 else lax.rem(at + key[1], count)
        return places[key]

    def device(dt, dz, dy):
        return {
            "ta": place_of("ta", ta, dt, nta), "gz": place_of("gz", gz, dz, ngz), "gy": place_of("gy", gy, dy, ngy),
        }

    near = [(dt, dz, dy) for dt in (-1, 0, 1) for dz in (-1, 0, 1) for dy in range(ngy)]
    centred = lambda d, n: (d + n // 2) % n - n // 2
    across = sorted(
        (cell for cell in slots if cell != (0, 0)),
        key=lambda c: -(abs(centred(c[0], nta)) + 2 * abs(centred(c[1], ngz))),
    )
    loads = []
    for t in range(size_t):
        loads.append((
            pltpu.make_async_copy(m_hbm.at[pl.ds(t, 1)], m_ref.at[pl.ds(t, 1)], loaded.at[0, t]),
            pltpu.make_async_copy(s_hbm.at[pl.ds(t, 1)], s_ref.at[pl.ds(t, 1)], loaded.at[1, t]),
        ))
    met = sorted({(dt % nta, dz % ngz, dy % ngy) for dt, dz, dy in near + [(-t, -z, 0) for t, z in across]} - {(0, 0, 0)})
    for t in [0, size_t - 1] + list(range(1, size_t - 1)):
        for load in loads[t]:
            load.start()
    barrier = pltpu.get_barrier_semaphore()
    for offset in met:
        pl.semaphore_signal(barrier, inc=1, device_id=device(*offset), device_id_type=MESH)

    def send(moves, sends, receives):
        copies = [
            pltpu.make_async_remote_copy(
                src_ref=source, dst_ref=target, send_sem=sends(place), recv_sem=receives(place),
                device_id=device(*offset), device_id_type=MESH,
            )
            for place, source, target, offset in moves
        ]
        for copy in copies:
            copy.start()
        sent.extend(copies)
        return copies

    def finish(copies):
        for copy in copies:
            copy.wait_recv()

    sent = []

    def finish_sends(copies):
        for copy in copies:
            copy.wait_send()

    inner_t, inner_z = pl.ds(1, size_t), pl.ds(1, size_z)

    def send0(number, moves):
        return send(moves, lambda place: f0s.at[number, place], lambda place: f0r.at[number, place])

    def exchange(number, field, faces, halos):
        copies = send0(number, [
            (4, faces.at[1], halos.at[0], (0, 0, 1)),
            (5, faces.at[0], halos.at[1], (0, 0, -1)),
            (2, field.at[inner_t, pl.ds(size_z, 1)], field.at[inner_t, pl.ds(0, 1)], (0, 1, 0)),
            (3, field.at[inner_t, pl.ds(1, 1)], field.at[inner_t, pl.ds(size_z + 1, 1)], (0, -1, 0)),
            (1, field.at[pl.ds(size_t, 1), inner_z], field.at[pl.ds(0, 1), inner_z], (1, 0, 0)),
            (0, field.at[pl.ds(1, 1), inner_z], field.at[pl.ds(size_t + 1, 1), inner_z], (-1, 0, 0)),
        ])
        return copies[:4], copies[4:]

    def around(field, part, dys):
        own_t, own_z = pl.ds(2, size_t1), pl.ds(2, size_z1)

        def span(size, deep, up):
            return pl.ds(2 + (size - deep) * up, deep), pl.ds(2 + size - (size + deep) * up, deep)

        corners, layers = [], []
        for up in (1, 0):
            for up_z in (1, 0):
                here_t, there_t = span(size_t1, 1, up)
                here_z, there_z = span(size_z1, 1, up_z)
                corners.append((2 + 2 * up + up_z, here_t, here_z, there_t, there_z, 2 * up - 1, 2 * up_z - 1))
        for up in (1, 0):
            here, there = span(size_t1, 2, up)
            layers.append((up, here, own_z, there, own_z, 2 * up - 1, 0))
            here, there = span(size_z1, 2, up)
            layers.append((6 + up, own_t, here, own_t, there, 0, 2 * up - 1))
        moves = []
        for dy in reversed(dys):
            for number, here_t, here_z, there_t, there_z, dt, dz in corners + layers:
                moves.append((
                    8 * dy + number, field.at[(here_t, here_z) + part], field.at[(there_t, there_z) + part], (dt, dz, dy),
                ))
        return moves

    def spread1(number, field):
        own = field.at[pl.ds(2, size_t1), pl.ds(2, size_z1), pl.ds(gy, 1)]
        moves = [(8 * ngy + dy - 1, own, own, (0, 0, dy)) for dy in range(1, ngy)]
        moves += around(field, (pl.ds(gy, 1),), range(ngy))
        return send(moves, lambda place: f1s.at[number, place], lambda place: f1r.at[number, place])

    def gather(number, field):
        own = field.at[slots[0, 0]]
        return send(
            [(slots[cell], own, field.at[slots[cell]], (-cell[0], -cell[1], 0)) for cell in across],
            lambda place: gsend.at[number, place], lambda place: grecv.at[number, place],
        )

    def put(field, faces, t, slab):
        field[t + 1, pl.ds(1, size_z)] = slab
        faces[0, t] = slab[:, :1]
        faces[1, t] = slab[:, rows - 1:]

    def sum0(field, halos, t):
        slab = field[t + 1, pl.ds(1, size_z)]
        row = lax.broadcasted_iota(jnp.int32, slab.shape, 1)
        summed = field[t, pl.ds(1, size_z)] + field[t + 2, pl.ds(1, size_z)]
        summed = summed + field[t + 1, pl.ds(0, size_z)] + field[t + 1, pl.ds(2, size_z)]
        summed = summed + jnp.where(row == 0, halos[0, t], rolled(slab, 1, 1))
        summed = summed + jnp.where(row == rows - 1, halos[1, t], rolled(slab, -1, 1))
        return slab, summed + rolled(slab, 1, 2) + rolled(slab, -1, 2)

    def halved(summed, place, step):
        count, high, _ = summed.shape
        view = fold.at[place, pl.ds(0, count)]
        view[...] = summed
        summed = view[:, pl.ds(0, high // 2, stride=2), :] + view[:, pl.ds(1, high // 2, stride=2), :]
        return (summed + pair_swap(summed, step, 2)) * 0.0625

    def doubled(slab, place):
        count, high, _ = slab.shape
        view = fold.at[place, pl.ds(0, count)]
        view[:, pl.ds(0, high, stride=2), :] = slab
        view[:, pl.ds(1, high, stride=2), :] = slab
        return view[...]

    full = ngy * rows1

    def near1(radius):
        for a in range(2 - radius, 2 + size_t1 + radius):
            reach = radius - max(2 - a, a - 1 - size_t1, 0)
            yield a, 2 - reach, size_z1 + 2 * reach

    def read1(field, a, b, count):
        return field[a, pl.ds(b, count)].reshape(count, full, lanes)

    def write1(field, a, b, slab):
        field[a, pl.ds(b, slab.shape[0])] = slab.reshape(slab.shape[0], ngy, rows1, lanes)

    def sum1(field, a, b, count):
        slab = read1(field, a, b, count)
        summed = read1(field, a - 1, b, count) + read1(field, a + 1, b, count)
        summed = summed + read1(field, a, b - 1, count) + read1(field, a, b + 1, count)
        summed = summed + rolled(slab, 1, 1) + rolled(slab, -1, 1)
        return slab, summed + rolled(slab, 2, 2) + rolled(slab, -2, 2)

    def sweep1(field, out, radius):
        for a, b, count in near1(radius):
            slab, summed = sum1(field, a, b, count)
            fresh = KEEP * slab + read1(g1, a, b, count) * (read1(s1, a, b, count) + 0.5 * summed)
            write1(out, a, b, fresh)

    def packed(out, slabs):
        parts = [slab[z] for slab in slabs for z in range(part_z)]
        lane = lax.broadcasted_iota(jnp.int32, parts[0].shape, 1)
        values = parts[0]
        for k in range(1, len(parts)):
            values = jnp.where(lane % 4 == k, parts[k], values)
        out[slots[0, 0]] = values

    inside = list(range(1, size_t - 1))
    ends = [0, size_t - 1]

    def first0(ts):
        for t in ts:
            for load in loads[t]:
                load.wait()
            weight = DAMPING / (8.0 + m_ref[t])
            g0[t] = weight
            put(v0a, ys0.at[0], t, weight * s_ref[t])

    first0(ends + inside)
    pl.semaphore_wait(barrier, len(met))
    sides, over_t = exchange(0, v0a, ys0.at[0], y0.at[0])
    for t in range(size_t1):
        mean = halved(z_pairs(m_ref[2 * t] + m_ref[2 * t + 1]), t, 1)
        m1[t + 2, pl.ds(2, size_z1), gy] = mean
    mass_copies = spread1(0, m1)

    def sweep0(field, halos, out, faces, ts, also=None):
        for t in ts:
            slab, summed = sum0(field, halos, t)
            fresh = KEEP * slab + g0[t] * (s_ref[t] + summed)
            put(out, faces, t, fresh)
            if also is not None:
                also[t] = fresh

    finish(sides)
    sweep0(v0a, y0.at[0], v0b, ys0.at[1], inside)
    finish(over_t)
    sweep0(v0a, y0.at[0], v0b, ys0.at[1], ends)
    sides, over_t = exchange(1, v0b, ys0.at[1], y0.at[1])
    finish(mass_copies)
    for a, b, count in near1(2):
        write1(g1, a, b, DAMPING / (4.0 + read1(m1, a, b, count)))

    def to_level2(slabs):
        return [
            halved(z_pairs(slabs[2 * t] + slabs[2 * t + 1]), t, 2) for t in range(part_t)
        ]

    packed(m2, to_level2([read1(m1, 2 + t, 2, size_z1) for t in range(size_t1)]))
    mass_copies = gather(0, m2)

    def remainder0(ts):
        for t in ts:
            remainder = []
            for odd in range(2):
                slab, summed = sum0(v0b, y0.at[1], 2 * t + odd)
                remainder.append(s_ref[2 * t + odd] + summed - (8.0 + m_ref[2 * t + odd]) * slab)
            s1[t + 2, pl.ds(2, size_z1), gy] = halved(z_pairs(remainder[0] + remainder[1]), t, 1)

    finish(sides)
    remainder0(range(1, size_t1 - 1))
    finish(over_t)
    remainder0((0, size_t1 - 1))
    source_copies = spread1(1, s1)
    finish(mass_copies)
    for cell in stages["source"]:
        g2[slots[cell]] = DAMPING / (2.0 + m2[slots[cell]])
    for cell in stages["coarse"][3]:
        m3[slots[cell]] = DAMPING / (1.0 + coarsened3(m2[slots[cell]]))
    finish(source_copies)

    for a, b, count in near1(2):
        write1(v1a, a, b, read1(g1, a, b, count) * read1(s1, a, b, count))
    sweep1(v1a, v1b, 1)
    remainder = []
    for a, b, count in near1(0):
        slab, summed = sum1(v1b, a, b, count)
        remainder.append(
            read1(s1, a, b, count) + 0.5 * summed - (4.0 + read1(m1, a, b, count)) * slab
        )
    packed(s2, to_level2(remainder))
    finish(gather(1, s2))

    def around2(cell):
        t, z = cell
        return [((t + dt) % nta, (z + dz) % ngz) for dt, dz in ((-1, 0), (1, 0), (0, -1), (0, 1))]

    def sum2(field, cell):
        slab = field[slots[cell]]
        before_t, after_t, before_z, after_z = [
            slab + field[slots[other]] if other in slots else slab for other in around2(cell)
        ]
        lane = lane_of(slab)
        summed = jnp.where(lane % 4 >= 2, rolled(after_t, 2, 1), rolled(before_t, -2, 1))
        summed = summed + jnp.where(lane % 2 == 1, rolled(after_z, 1, 1), rolled(before_z, -1, 1))
        summed = summed + rolled(slab, 1, 0) + rolled(slab, -1, 0)
        return slab, summed + rolled(slab, 4, 1) + rolled(slab, -4, 1)

    def sweep2(field, out, cells):
        for cell in cells:
            slab, summed = sum2(field, cell)
            at = slots[cell]
            out[at] = KEEP * slab + g2[at] * (s2[at] + 0.25 * summed)

    for cell in stages["source"]:
        at = slots[cell]
        u2[at] = g2[at] * s2[at]
        w2[at] = u2[at]
    sweep2(u2, w2, stages["swept"])
    values = {}
    for cell in stages["coarse"][3]:
        slab, summed = sum2(w2, cell)
        at = slots[cell]
        source = coarsened3(s2[at] + 0.25 * summed - (2.0 + m2[at]) * slab)
        s3[at] = source
        values[cell] = m3[at] * source
    for steps in (2, 1, 0):
        fresh = {}
        for cell in stages["coarse"][steps]:
            slab = values[cell]
            before_t, after_t, before_z, after_z = [values[other] for other in around2(cell)]
            summed = before_t + after_t + before_z + after_z
            summed = summed + rolled(slab, 2, 0) + rolled(slab, -2, 0)
            summed = summed + rolled(slab, 8, 1) + rolled(slab, -8, 1)
            fresh[cell] = KEEP * slab + m3[slots[cell]] * (s3[slots[cell]] + 0.125 * summed)
        values = fresh
    for cell in stages["base"]:
        w2[slots[cell]] = w2[slots[cell]] + refined3(values[cell])
    for cell in stages["base"]:
        u2[slots[cell]] = w2[slots[cell]]
    sweep2(w2, u2, stages["first"])
    sweep2(u2, w2, stages["last"])

    def correct1(t, z):
        piece = piece2(w2[slots[t // 2 % nta, z // 2 % ngz]], t % 2, z % 2)
        e2[t + 1, z + 1, pl.ds(0, full // 2, stride=2), :] = piece
        e2[t + 1, z + 1, pl.ds(1, full // 2, stride=2), :] = piece

    for t in range(-1, part_t + 1):
        for z in range(-1, part_z + 1):
            if 0 <= t < part_t or 0 <= z < part_z:
                correct1(t, z)
    for a, b, count in near1(1):
        low, high = b // 2, (b + count + 1) // 2
        fine = refined_z(e2[a // 2, pl.ds(low, high - low)])[b - 2 * low:][:count]
        write1(v1w, a, b, read1(v1b, a, b, count) + fine)
    sweep1(v1w, v1x, 0)
    finish(send(
        around(v1x, (), range(1)), lambda place: fxs.at[place], lambda place: fxr.at[place],
    ))
    sweep1(v1x, e1, 1)

    under = lax.rem(gy + ngy - 1, ngy)
    over = lax.rem(gy + 1, ngy)
    def corrected0(layers):
        for at_t in layers:
            own = [p for p in (2 * at_t - 3, 2 * at_t - 2) if 1 <= p <= size_t]
            if not own:
                p = 0 if at_t == 1 else size_t + 1
                fine = refined_z(doubled(e1[at_t, pl.ds(2, size_z1), gy], 0))
                v0w[p, inner_z] = v0b[p, inner_z] + fine
                continue
            fine = refined_z(doubled(e1[at_t, pl.ds(1, size_z1 + 2), gy], at_t % 4))
            fine = fine[1:1 + size_z + 2]
            low = refined_z(e1[at_t, pl.ds(2, size_z1), under, pl.ds(rows1 - 1, 1)])
            high = refined_z(e1[at_t, pl.ds(2, size_z1), over, pl.ds(0, 1)])
            for p in own:
                v0w[p] = v0b[p] + fine
                y0[2, 0, p - 1] = y0[1, 0, p - 1] + low
                y0[2, 1, p - 1] = y0[1, 1, p - 1] + high

    corrected0(range(1, size_t1 + 3))
    sweep0(v0w, y0.at[2], v0x, ys0.at[2], range(size_t))
    sides, over_t = exchange(2, v0x, ys0.at[2], y0.at[3])
    finish(sides)
    sweep0(v0x, y0.at[3], v0s, ys0.at[3], inside, sol_ref)
    finish(over_t)
    sweep0(v0x, y0.at[3], v0s, ys0.at[3], ends, sol_ref)
    earlier = len(sent)
    sides, over_t = exchange(3, v0s, ys0.at[3], y0.at[4])
    finish_sends(sent[:earlier])

    def residual(ts):
        for t in ts:
            slab, summed = sum0(v0s, y0.at[4], t)
            res_ref[t] = s_ref[t] + summed - (8.0 + m_ref[t]) * slab

    finish(sides)
    residual(inside)
    finish(over_t)
    residual(ends)
    finish_sends(sent[earlier:])


def lane_of(values):
    return lax.broadcasted_iota(jnp.int32, values.shape, 1)


def coarsened3(values):
    for step in (1, 2, 4):
        values = values + rolled(values, -step, 1)
    return (values + rolled(values, -1, 0)) * 0.0625


def refined3(values):
    row = lax.broadcasted_iota(jnp.int32, values.shape, 0)
    values = jnp.where((lane_of(values) % 8 == 0) & (row % 2 == 0), values, 0.0)
    for step in (1, 2, 4):
        values = values + rolled(values, step, 1)
    return values + rolled(values, 1, 0)


def piece2(values, odd_t, odd_z):
    values = jnp.where(lane_of(values) % 4 == 2 * odd_t + odd_z, values, 0.0)
    values = values + rolled(values, -1 if odd_z else 1, 1)
    return values + rolled(values, -2 if odd_t else 2, 1)


def grown(cells, steps, count_t, count_z):
    for _ in range(steps):
        cells = cells | {
            ((t + dt) % count_t, (z + dz) % count_z)
            for t, z in cells for dt, dz in ((-1, 0), (1, 0), (0, -1), (0, 1))
        }
    return cells


def plan(nta, ngz):
    sites = lambda cells, steps: grown(cells, steps, 2 * nta, 2 * ngz)
    blocks = lambda cells: {(t // 2, z // 2) for t, z in cells}
    inner = lambda cells: {(2 * t + a, 2 * z + b) for t, z in cells for a in (0, 1) for b in (0, 1)}
    last = sites(inner({(0, 0)}), 1)
    first, base = sites(last, 1), sites(last, 2)
    coarse = [grown(blocks(base), steps, nta, ngz) for steps in range(4)]
    swept = sites(inner(coarse[3]), 1) | base
    ordered = lambda cells: sorted(cells, key=lambda c: ((c[0] + nta // 2) % nta, (c[1] + ngz // 2) % ngz))
    return {
        "last": ordered(blocks(last)), "first": ordered(blocks(first)), "base": ordered(blocks(base)),
        "coarse": [ordered(cells) for cells in coarse], "swept": ordered(blocks(swept)),
        "source": ordered(blocks(sites(swept, 1))),
    }


def per_device(sizes, right_side, mass_field):
    nta, ngz, ngy = sizes
    size_t, size_z, rows, lanes = right_side.shape
    size_t1, size_z1, rows1 = size_t // 2, size_z // 2, rows // 2
    part_t, part_z, rows2 = size_t // 4, size_z // 4, rows // 4
    vmem = lambda *shape: pltpu.VMEM(shape, jnp.float32)
    dma = lambda *shape: pltpu.SemaphoreType.DMA(shape)
    padded0 = vmem(size_t + 2, size_z + 2, rows, lanes)
    padded1 = vmem(size_t1 + 4, size_z1 + 4, ngy, rows1, lanes)
    window = len(plan(nta, ngz)["source"])
    packs = vmem(window, rows2 * ngy, lanes)
    spreads = 8 * ngy + ngy - 1
    scratch = [
        vmem(size_t, size_z, rows, lanes), padded0, padded0, padded0, padded0, padded0,
        vmem(5, 2, size_t, size_z, 1, lanes), vmem(4, 2, size_t, size_z, 1, lanes),
        vmem(max(size_t1, part_t + 2), size_z, max(rows, ngy * rows1), lanes),
        *[padded1] * 8, vmem(part_t + 2, part_z + 2, ngy * rows1, lanes),
        *[packs] * 7,
        dma(4, 6), dma(4, 6), dma(2, spreads), dma(2, spreads), dma(8), dma(8),
        dma(2, window), dma(2, window),
        vmem(size_t, size_z, rows, lanes), vmem(size_t, size_z, rows, lanes), dma(2, size_t),
    ]
    block = jax.ShapeDtypeStruct(right_side.shape, jnp.float32)
    return pl.pallas_call(
        functools.partial(kernel, sizes),
        out_shape=(block, block),
        in_specs=[pl.BlockSpec(memory_space=pltpu.HBM)] * 2,
        out_specs=(pl.BlockSpec(memory_space=pltpu.VMEM),) * 2,
        scratch_shapes=scratch,
        compiler_params=pltpu.CompilerParams(
            collective_id=0, has_side_effects=True, vmem_limit_bytes=48 * 1024 * 1024
        ),
    )(*[pltpu.with_memory_space_constraint(values, pltpu.HBM) for values in (right_side, mass_field)])


def solution(mesh):
    sizes = tuple(mesh.shape[axis] for axis in ("ta", "gz", "gy"))
    spec = P("ta", "gz", "gy", None)
    return jax.shard_map(
        functools.partial(per_device, sizes),
        mesh=mesh,
        in_specs=(spec, spec),
        out_specs=(spec, spec),
        check_vma=False,
    )
```

```python
import functools

import jax
import jax.numpy as jnp
from jax import lax
from jax.experimental import pallas as pl
from jax.experimental.pallas import tpu as pltpu
from jax.sharding import PartitionSpec as P

DAMPING = 0.7
KEEP = 1.0 - DAMPING
PAD_T, PAD_Z = 3, 2
MESH = pl.DeviceIdType.MESH


def rolled(values, shift, axis):
    return pltpu.roll(values, shift % values.shape[axis], axis)


def odd_lane(values):
    return lax.broadcasted_iota(jnp.int32, values.shape, values.ndim - 1) % 2 == 1


def pair_swap(values, step, axis):
    index = lax.broadcasted_iota(jnp.int32, values.shape, axis)
    return jnp.where((index // step) % 2 == 0, rolled(values, -step, axis), rolled(values, step, axis))


def z_pairs(summed):
    count, rows, lanes = summed.shape
    summed = summed.reshape(count // 2, 2, rows, lanes)
    return summed[:, 0] + summed[:, 1]


def refined_z(slab):
    return jnp.repeat(slab, 2, axis=0)


def kernel(sizes, s_hbm, m_hbm, sol_ref, res_ref, *scratch):
    nta, ngz, ngy = sizes
    (g0, v0a, v0b, v0w, v0x, v0s, y0, ys0, fold,
     s1, m1, g1, v1a, v1b, v1h, v1w, v1x, e1, e2,
     m2, s2, g2, u2, w2, m3, s3,
     f0s, f0r, f1s, f1r, fxs, fxr, gsend, grecv, s_ref, m_ref, loaded) = scratch
    size_t, size_z, rows, lanes = s_ref.shape
    size_t1, pairs1, rows1 = size_t // 2, size_z // 4, rows // 2
    part_t, part_z, rows2 = size_t // 4, size_z // 4, rows // 4
    stages = plan(nta, ngz)
    slots = {cell: number for number, cell in enumerate(stages["source"])}
    ta, gz, gy = lax.axis_index("ta"), lax.axis_index("gz"), lax.axis_index("gy")

    places = {}

    def place_of(axis, at, step, count):
        key = axis, step % count
        if key not in places:
            places[key] = at if key[1] == 0 else lax.rem(at + key[1], count)
        return places[key]

    def device(dt, dz, dy):
        return {
            "ta": place_of("ta", ta, dt, nta), "gz": place_of("gz", gz, dz, ngz), "gy": place_of("gy", gy, dy, ngy),
        }

    near = [(dt, dz, dy) for dt in (-1, 0, 1) for dz in (-1, 0, 1) for dy in range(ngy)]
    centred = lambda d, n: (d + n // 2) % n - n // 2
    across = sorted(
        (cell for cell in slots if cell != (0, 0)),
        key=lambda c: -(abs(centred(c[0], nta)) + 2 * abs(centred(c[1], ngz))),
    )
    loads = []
    for t in range(size_t):
        loads.append((
            pltpu.make_async_copy(m_hbm.at[pl.ds(t, 1)], m_ref.at[pl.ds(t, 1)], loaded.at[0, t]),
            pltpu.make_async_copy(s_hbm.at[pl.ds(t, 1)], s_ref.at[pl.ds(t, 1)], loaded.at[1, t]),
        ))
    met = sorted({(dt % nta, dz % ngz, dy % ngy) for dt, dz, dy in near + [(-t, -z, 0) for t, z in across]} - {(0, 0, 0)})
    for t in [0, size_t - 1] + list(range(1, size_t - 1)):
        for load in loads[t]:
            load.start()
    barrier = pltpu.get_barrier_semaphore()
    for offset in met:
        pl.semaphore_signal(barrier, inc=1, device_id=device(*offset), device_id_type=MESH)

    def send(moves, sends, receives):
        copies = [
            pltpu.make_async_remote_copy(
                src_ref=source, dst_ref=target, send_sem=sends(place), recv_sem=receives(place),
                device_id=device(*offset), device_id_type=MESH,
            )
            for place, source, target, offset in moves
        ]
        for copy in copies:
            copy.start()
        sent.extend(copies)
        return copies

    def finish(copies):
        for copy in copies:
            copy.wait_recv()

    sent = []

    def finish_sends(copies):
        for copy in copies:
            copy.wait_send()

    inner_t, inner_z = pl.ds(1, size_t), pl.ds(1, size_z)

    def send0(number, moves):
        return send(moves, lambda place: f0s.at[number, place], lambda place: f0r.at[number, place])

    def exchange(number, field, faces, halos):
        copies = send0(number, [
            (4, faces.at[1], halos.at[0], (0, 0, 1)),
            (5, faces.at[0], halos.at[1], (0, 0, -1)),
            (2, field.at[inner_t, pl.ds(size_z, 1)], field.at[inner_t, pl.ds(0, 1)], (0, 1, 0)),
            (3, field.at[inner_t, pl.ds(1, 1)], field.at[inner_t, pl.ds(size_z + 1, 1)], (0, -1, 0)),
            (1, field.at[pl.ds(size_t, 1), inner_z], field.at[pl.ds(0, 1), inner_z], (1, 0, 0)),
            (0, field.at[pl.ds(1, 1), inner_z], field.at[pl.ds(size_t + 1, 1), inner_z], (-1, 0, 0)),
        ])
        return copies[:4], copies[4:]

    def layers1(deep_t, deep_z, corner_t):
        own_t, own_z = pl.ds(PAD_T, size_t1), pl.ds(PAD_Z, pairs1)

        def span(pad, size, deep, up):
            return pl.ds(pad + (size - deep) * up, deep), pl.ds(pad + size - (size + deep) * up, deep)

        moves = []
        for up in (1, 0):
            for up_z in (1, 0):
                here_t, there_t = span(PAD_T, size_t1, corner_t, up)
                here_z, there_z = span(PAD_Z, pairs1, 1, up_z)
                moves.append((here_t, here_z, there_t, there_z, 2 * up - 1, 2 * up_z - 1))
        for up in (1, 0):
            here, there = span(PAD_T, size_t1, deep_t, up)
            moves.append((here, own_z, there, own_z, 2 * up - 1, 0))
            here, there = span(PAD_Z, pairs1, deep_z, up)
            moves.append((own_t, here, own_t, there, 0, 2 * up - 1))
        return moves

    def spread1(number, field):
        part = pl.ds(gy, 1)
        own = field.at[pl.ds(PAD_T, size_t1), pl.ds(PAD_Z, pairs1), part]
        moves = [(8 * ngy + dy - 1, own, own, (0, 0, dy)) for dy in range(1, ngy)]
        for dy in reversed(range(ngy)):
            for place, (here_t, here_z, there_t, there_z, dt, dz) in enumerate(layers1(2, 1, 1)):
                moves.append((
                    8 * dy + place, field.at[here_t, here_z, part], field.at[there_t, there_z, part], (dt, dz, dy),
                ))
        return send(moves, lambda place: f1s.at[number, place], lambda place: f1r.at[number, place])

    def widen1(field):
        moves = [
            (place, field.at[here_t, here_z], field.at[there_t, there_z], (dt, dz, 0))
            for place, (here_t, here_z, there_t, there_z, dt, dz) in enumerate(layers1(3, 2, 2))
        ]
        return send(moves, lambda place: fxs.at[place], lambda place: fxr.at[place])

    def gather(number, field):
        own = field.at[slots[0, 0]]
        return send(
            [(slots[cell], own, field.at[slots[cell]], (-cell[0], -cell[1], 0)) for cell in across],
            lambda place: gsend.at[number, place], lambda place: grecv.at[number, place],
        )

    def put(field, faces, t, slab):
        field[t + 1, pl.ds(1, size_z)] = slab
        faces[0, t] = slab[:, :1]
        faces[1, t] = slab[:, rows - 1:]

    def sum0(field, halos, t):
        slab = field[t + 1, pl.ds(1, size_z)]
        row = lax.broadcasted_iota(jnp.int32, slab.shape, 1)
        summed = field[t, pl.ds(1, size_z)] + field[t + 2, pl.ds(1, size_z)]
        summed = summed + field[t + 1, pl.ds(0, size_z)] + field[t + 1, pl.ds(2, size_z)]
        summed = summed + jnp.where(row == 0, halos[0, t], rolled(slab, 1, 1))
        summed = summed + jnp.where(row == rows - 1, halos[1, t], rolled(slab, -1, 1))
        return slab, summed + rolled(slab, 1, 2) + rolled(slab, -1, 2)

    def folded(summed, place):
        count, high, _ = summed.shape
        view = fold.at[place, pl.ds(0, count)]
        view[...] = summed
        return view[:, pl.ds(0, high // 2, stride=2), :] + view[:, pl.ds(1, high // 2, stride=2), :]

    def to_level1(summed, place):
        summed = folded(z_pairs(summed), place)
        summed = summed.reshape(summed.shape[0] // 2, 2, *summed.shape[1:])
        even, odd = summed[:, 0], summed[:, 1]
        even, odd = even + rolled(even, -1, 2), odd + rolled(odd, 1, 2)
        return jnp.where(odd_lane(even), odd, even) * 0.0625

    def doubled(slab, place):
        count, high, _ = slab.shape
        view = fold.at[place, pl.ds(0, count)]
        view[:, pl.ds(0, high, stride=2), :] = slab
        view[:, pl.ds(1, high, stride=2), :] = slab
        return view[...]

    full = ngy * rows1

    def near1(radius):
        for t in range(-radius, size_t1 + radius):
            reach = (radius - max(-t, t - size_t1 + 1, 0) + 1) // 2
            yield t, -reach, pairs1 + 2 * reach

    def read1(field, t, z, count):
        return field[PAD_T + t, pl.ds(PAD_Z + z, count)].reshape(count, full, lanes)

    def write1(field, t, z, slab):
        field[PAD_T + t, pl.ds(PAD_Z + z, slab.shape[0])] = slab.reshape(slab.shape[0], ngy, rows1, lanes)

    def sum1(field, t, z, count, held):
        slab = read1(field, t, z, count)
        summed = read1(field, t - 1, z, count) + read1(field, t + 1, z, count)
        if held[t][0] < z:
            before, after = read1(field, t, z - 1, count), read1(field, t, z + 1, count)
        else:
            before = jnp.concatenate([slab[:1], slab[:-1]], axis=0)
            after = jnp.concatenate([slab[1:], slab[-1:]], axis=0)
        summed = summed + jnp.where(odd_lane(slab), rolled(slab + after, 1, 2), rolled(slab + before, -1, 2))
        summed = summed + rolled(slab, 1, 1) + rolled(slab, -1, 1)
        return slab, summed + rolled(slab, 2, 2) + rolled(slab, -2, 2)

    held1 = [{t: (z, count) for t, z, count in near1(radius)} for radius in range(4)]

    def sweep1(field, out, radius):
        for t, z, count in near1(radius):
            slab, summed = sum1(field, t, z, count, held1[radius + 1])
            fresh = KEEP * slab + read1(g1, t, z, count) * (read1(s1, t, z, count) + 0.5 * summed)
            write1(out, t, z, fresh)

    def packed(out, slabs):
        parts = [slab[z] for slab in slabs for z in range(part_z)]
        lane = lax.broadcasted_iota(jnp.int32, parts[0].shape, 1)
        values = parts[0]
        for k in range(1, len(parts)):
            values = jnp.where(lane % 4 == k, parts[k], values)
        out[slots[0, 0]] = values

    inside = list(range(1, size_t - 1))
    ends = [0, size_t - 1]

    def first0(ts):
        for t in ts:
            for load in loads[t]:
                load.wait()
            weight = DAMPING / (8.0 + m_ref[t])
            g0[t] = weight
            put(v0a, ys0.at[0], t, weight * s_ref[t])

    first0(ends + inside)
    pl.semaphore_wait(barrier, len(met))
    sides, over_t = exchange(0, v0a, ys0.at[0], y0.at[0])
    for t in range(size_t1):
        m1[PAD_T + t, pl.ds(PAD_Z, pairs1), gy] = to_level1(m_ref[2 * t] + m_ref[2 * t + 1], t)
    mass_copies = spread1(0, m1)

    def sweep0(field, halos, out, faces, ts, also=None):
        for t in ts:
            slab, summed = sum0(field, halos, t)
            fresh = KEEP * slab + g0[t] * (s_ref[t] + summed)
            put(out, faces, t, fresh)
            if also is not None:
                also[t] = fresh

    finish(sides)
    sweep0(v0a, y0.at[0], v0b, ys0.at[1], inside)
    finish(over_t)
    sweep0(v0a, y0.at[0], v0b, ys0.at[1], ends)
    sides, over_t = exchange(1, v0b, ys0.at[1], y0.at[1])
    finish(mass_copies)
    for a, b, count in near1(2):
        write1(g1, a, b, DAMPING / (4.0 + read1(m1, a, b, count)))

    def to_level2(slabs):
        out = []
        for t in range(part_t):
            summed = folded(slabs[2 * t] + slabs[2 * t + 1], t)
            summed = summed + pair_swap(summed, 1, 2)
            out.append((summed + pair_swap(summed, 2, 2)) * 0.0625)
        return out

    packed(m2, to_level2([read1(m1, t, 0, pairs1) for t in range(size_t1)]))
    mass_copies = gather(0, m2)

    def remainder0(ts):
        for t in ts:
            remainder = []
            for odd in range(2):
                slab, summed = sum0(v0b, y0.at[1], 2 * t + odd)
                remainder.append(s_ref[2 * t + odd] + summed - (8.0 + m_ref[2 * t + odd]) * slab)
            s1[PAD_T + t, pl.ds(PAD_Z, pairs1), gy] = to_level1(remainder[0] + remainder[1], t)

    finish(sides)
    remainder0(range(1, size_t1 - 1))
    finish(over_t)
    remainder0((0, size_t1 - 1))
    source_copies = spread1(1, s1)
    finish(mass_copies)
    for cell in stages["source"]:
        g2[slots[cell]] = DAMPING / (2.0 + m2[slots[cell]])
    for cell in stages["coarse"][3]:
        m3[slots[cell]] = DAMPING / (1.0 + coarsened3(m2[slots[cell]]))
    finish(source_copies)

    for a, b, count in near1(2):
        write1(v1a, a, b, read1(g1, a, b, count) * read1(s1, a, b, count))
    sweep1(v1a, v1b, 1)
    remainder = []
    for a, b, count in near1(0):
        slab, summed = sum1(v1b, a, b, count, held1[1])
        write1(v1h, a, b, slab)
        remainder.append(
            read1(s1, a, b, count) + 0.5 * summed - (4.0 + read1(m1, a, b, count)) * slab
        )
    packed(s2, to_level2(remainder))
    source_copies = gather(1, s2)
    wide_copies = widen1(v1h)
    finish(source_copies)

    def around2(cell):
        t, z = cell
        return [((t + dt) % nta, (z + dz) % ngz) for dt, dz in ((-1, 0), (1, 0), (0, -1), (0, 1))]

    def sum2(field, cell):
        slab = field[slots[cell]]
        before_t, after_t, before_z, after_z = [
            slab + field[slots[other]] if other in slots else slab for other in around2(cell)
        ]
        lane = lane_of(slab)
        summed = jnp.where(lane % 4 >= 2, rolled(after_t, 2, 1), rolled(before_t, -2, 1))
        summed = summed + jnp.where(lane % 2 == 1, rolled(after_z, 1, 1), rolled(before_z, -1, 1))
        summed = summed + rolled(slab, 1, 0) + rolled(slab, -1, 0)
        return slab, summed + rolled(slab, 4, 1) + rolled(slab, -4, 1)

    def sweep2(field, out, cells):
        for cell in cells:
            slab, summed = sum2(field, cell)
            at = slots[cell]
            out[at] = KEEP * slab + g2[at] * (s2[at] + 0.25 * summed)

    for cell in stages["source"]:
        at = slots[cell]
        u2[at] = g2[at] * s2[at]
        w2[at] = u2[at]
    sweep2(u2, w2, stages["swept"])
    values = {}
    for cell in stages["coarse"][3]:
        slab, summed = sum2(w2, cell)
        at = slots[cell]
        source = coarsened3(s2[at] + 0.25 * summed - (2.0 + m2[at]) * slab)
        s3[at] = source
        values[cell] = m3[at] * source
    for steps in (2, 1, 0):
        fresh = {}
        for cell in stages["coarse"][steps]:
            slab = values[cell]
            before_t, after_t, before_z, after_z = [values[other] for other in around2(cell)]
            summed = before_t + after_t + before_z + after_z
            summed = summed + rolled(slab, 2, 0) + rolled(slab, -2, 0)
            summed = summed + rolled(slab, 8, 1) + rolled(slab, -8, 1)
            fresh[cell] = KEEP * slab + m3[slots[cell]] * (s3[slots[cell]] + 0.125 * summed)
        values = fresh
    for cell in stages["base"]:
        w2[slots[cell]] = w2[slots[cell]] + refined3(values[cell])
    for cell in stages["base"]:
        u2[slots[cell]] = w2[slots[cell]]
    sweep2(w2, u2, stages["first"])
    sweep2(u2, w2, stages["last"])

    def correct1(t, z):
        piece = piece2(w2[slots[t // 2 % nta, z // 2 % ngz]], t % 2, z % 2)
        e2[t + 2, z + 2, pl.ds(0, full // 2, stride=2), :] = piece
        e2[t + 2, z + 2, pl.ds(1, full // 2, stride=2), :] = piece

    for t in range(-2, part_t + 2):
        for z in range(-2, part_z + 2):
            if max(-t, t - part_t + 1, 0) + max(-z, z - part_z + 1, 0) <= 2:
                correct1(t, z)
    finish(wide_copies)
    for t, z, count in near1(3):
        write1(v1w, t, z, read1(v1h, t, z, count) + e2[t // 2 + 2, pl.ds(z + 2, count)])
    sweep1(v1w, v1x, 2)
    sweep1(v1x, e1, 1)

    under = lax.rem(gy + ngy - 1, ngy)
    over = lax.rem(gy + 1, ngy)

    def split1(slab):
        even = jnp.where(odd_lane(slab), rolled(slab, 1, 2), slab)
        odd = jnp.where(odd_lane(slab), slab, rolled(slab, -1, 2))
        return jnp.stack([even, odd], axis=1).reshape(2 * slab.shape[0], *slab.shape[1:])

    def corrected0(layers):
        for t in layers:
            own = [p for p in (2 * t + 1, 2 * t + 2) if 1 <= p <= size_t]
            if not own:
                p = 0 if t < 0 else size_t + 1
                fine = refined_z(doubled(split1(e1[PAD_T + t, pl.ds(PAD_Z, pairs1), gy]), 0))
                v0w[p, inner_z] = v0b[p, inner_z] + fine
                continue
            fine = split1(e1[PAD_T + t, pl.ds(PAD_Z - 1, pairs1 + 2), gy])
            fine = refined_z(doubled(fine[1:-1], t % 4))
            fine = fine[1:1 + size_z + 2]
            low = refined_z(split1(e1[PAD_T + t, pl.ds(PAD_Z, pairs1), under, pl.ds(rows1 - 1, 1)]))
            high = refined_z(split1(e1[PAD_T + t, pl.ds(PAD_Z, pairs1), over, pl.ds(0, 1)]))
            for p in own:
                v0w[p] = v0b[p] + fine
                y0[2, 0, p - 1] = y0[1, 0, p - 1] + low
                y0[2, 1, p - 1] = y0[1, 1, p - 1] + high

    corrected0(range(-1, size_t1 + 1))
    sweep0(v0w, y0.at[2], v0x, ys0.at[2], range(size_t))
    sides, over_t = exchange(2, v0x, ys0.at[2], y0.at[3])
    finish(sides)
    sweep0(v0x, y0.at[3], v0s, ys0.at[3], inside, sol_ref)
    finish(over_t)
    sweep0(v0x, y0.at[3], v0s, ys0.at[3], ends, sol_ref)
    earlier = len(sent)
    sides, over_t = exchange(3, v0s, ys0.at[3], y0.at[4])
    finish_sends(sent[:earlier])

    def residual(ts):
        for t in ts:
            slab, summed = sum0(v0s, y0.at[4], t)
            res_ref[t] = s_ref[t] + summed - (8.0 + m_ref[t]) * slab

    finish(sides)
    residual(inside)
    finish(over_t)
    residual(ends)
    finish_sends(sent[earlier:])


def lane_of(values):
    return lax.broadcasted_iota(jnp.int32, values.shape, 1)


def coarsened3(values):
    for step in (1, 2, 4):
        values = values + rolled(values, -step, 1)
    return (values + rolled(values, -1, 0)) * 0.0625


def refined3(values):
    row = lax.broadcasted_iota(jnp.int32, values.shape, 0)
    values = jnp.where((lane_of(values) % 8 == 0) & (row % 2 == 0), values, 0.0)
    for step in (1, 2, 4):
        values = values + rolled(values, step, 1)
    return values + rolled(values, 1, 0)


def piece2(values, odd_t, odd_z):
    values = jnp.where(lane_of(values) % 4 == 2 * odd_t + odd_z, values, 0.0)
    values = values + rolled(values, -1 if odd_z else 1, 1)
    return values + rolled(values, -2 if odd_t else 2, 1)


def grown(cells, steps, count_t, count_z):
    for _ in range(steps):
        cells = cells | {
            ((t + dt) % count_t, (z + dz) % count_z)
            for t, z in cells for dt, dz in ((-1, 0), (1, 0), (0, -1), (0, 1))
        }
    return cells


def plan(nta, ngz):
    sites = lambda cells, steps: grown(cells, steps, 2 * nta, 2 * ngz)
    blocks = lambda cells: {(t // 2, z // 2) for t, z in cells}
    inner = lambda cells: {(2 * t + a, 2 * z + b) for t, z in cells for a in (0, 1) for b in (0, 1)}
    last = sites(inner({(0, 0)}), 2)
    first, base = sites(last, 1), sites(last, 2)
    coarse = [grown(blocks(base), steps, nta, ngz) for steps in range(4)]
    swept = sites(inner(coarse[3]), 1) | base
    ordered = lambda cells: sorted(cells, key=lambda c: ((c[0] + nta // 2) % nta, (c[1] + ngz // 2) % ngz))
    return {
        "last": ordered(blocks(last)), "first": ordered(blocks(first)), "base": ordered(blocks(base)),
        "coarse": [ordered(cells) for cells in coarse], "swept": ordered(blocks(swept)),
        "source": ordered(blocks(sites(swept, 1))),
    }


def per_device(sizes, right_side, mass_field):
    nta, ngz, ngy = sizes
    size_t, size_z, rows, lanes = right_side.shape
    size_t1, pairs1, rows1 = size_t // 2, size_z // 4, rows // 2
    part_t, part_z, rows2 = size_t // 4, size_z // 4, rows // 4
    vmem = lambda *shape: pltpu.VMEM(shape, jnp.float32)
    dma = lambda *shape: pltpu.SemaphoreType.DMA(shape)
    padded0 = vmem(size_t + 2, size_z + 2, rows, lanes)
    padded1 = vmem(size_t1 + 2 * PAD_T, pairs1 + 2 * PAD_Z, ngy, rows1, lanes)
    window = len(plan(nta, ngz)["source"])
    packs = vmem(window, rows2 * ngy, lanes)
    spreads = 8 * ngy + ngy - 1
    scratch = [
        vmem(size_t, size_z, rows, lanes), padded0, padded0, padded0, padded0, padded0,
        vmem(5, 2, size_t, size_z, 1, lanes), vmem(4, 2, size_t, size_z, 1, lanes),
        vmem(max(size_t1, part_t + 2), size_z, max(rows, ngy * rows1), lanes),
        *[padded1] * 9, vmem(part_t + 4, part_z + 4, ngy * rows1, lanes),
        *[packs] * 7,
        dma(4, 6), dma(4, 6), dma(2, spreads), dma(2, spreads), dma(8), dma(8),
        dma(2, window), dma(2, window),
        vmem(size_t, size_z, rows, lanes), vmem(size_t, size_z, rows, lanes), dma(2, size_t),
    ]
    block = jax.ShapeDtypeStruct(right_side.shape, jnp.float32)
    return pl.pallas_call(
        functools.partial(kernel, sizes),
        out_shape=(block, block),
        in_specs=[pl.BlockSpec(memory_space=pltpu.HBM)] * 2,
        out_specs=(pl.BlockSpec(memory_space=pltpu.VMEM),) * 2,
        scratch_shapes=scratch,
        compiler_params=pltpu.CompilerParams(
            collective_id=0, has_side_effects=True, vmem_limit_bytes=48 * 1024 * 1024
        ),
    )(*[pltpu.with_memory_space_constraint(values, pltpu.HBM) for values in (right_side, mass_field)])


def solution(mesh):
    sizes = tuple(mesh.shape[axis] for axis in ("ta", "gz", "gy"))
    spec = P("ta", "gz", "gy", None)
    return jax.shard_map(
        functools.partial(per_device, sizes),
        mesh=mesh,
        in_specs=(spec, spec),
        out_specs=(spec, spec),
        check_vma=False,
    )
```

```python
import functools

import jax
import jax.numpy as jnp
from jax import lax
from jax.experimental import pallas as pl
from jax.experimental.pallas import tpu as pltpu
from jax.sharding import PartitionSpec as P

DAMPING = 0.7
KEEP = 1.0 - DAMPING
PAD_T, PAD_Z = 3, 2
MESH = pl.DeviceIdType.MESH


def rolled(values, shift, axis):
    return pltpu.roll(values, shift % values.shape[axis], axis)


def odd_lane(values):
    return lax.broadcasted_iota(jnp.int32, values.shape, values.ndim - 1) % 2 == 1


def pair_swap(values, step, axis):
    index = lax.broadcasted_iota(jnp.int32, values.shape, axis)
    return jnp.where((index // step) % 2 == 0, rolled(values, -step, axis), rolled(values, step, axis))


def z_pairs(summed):
    count, rows, lanes = summed.shape
    summed = summed.reshape(count // 2, 2, rows, lanes)
    return summed[:, 0] + summed[:, 1]


def refined_z(slab):
    return jnp.repeat(slab, 2, axis=0)


def kernel(sizes, s_hbm, m_hbm, sol_ref, res_ref, *scratch):
    nta, ngz, ngy = sizes
    (g0, v0a, v0b, v0w, v0x, v0s, y0, ys0, fold,
     s1, m1, g1, v1a, v1b, v1h, v1w, v1x, e1, e2,
     m2, s2, g2, u2, w2, m3, s3, u3, w3,
     f0s, f0r, f1s, f1r, fxs, fxr, gsend, grecv, s_ref, m_ref, loaded) = scratch
    size_t, size_z, rows, lanes = s_ref.shape
    size_t1, pairs1, rows1 = size_t // 2, size_z // 4, rows // 2
    part_t, part_z, rows2 = size_t // 4, size_z // 4, rows // 4
    stages = plan(nta, ngz)
    slots = {cell: number for number, cell in enumerate(stages["source"])}
    slots3 = {cell: number for number, cell in enumerate(stages["coarse"][3])}
    ta, gz, gy = lax.axis_index("ta"), lax.axis_index("gz"), lax.axis_index("gy")

    places = {}

    def place_of(axis, at, step, count):
        key = axis, step % count
        if key not in places:
            places[key] = at if key[1] == 0 else lax.rem(at + key[1], count)
        return places[key]

    def device(dt, dz, dy):
        return {
            "ta": place_of("ta", ta, dt, nta), "gz": place_of("gz", gz, dz, ngz), "gy": place_of("gy", gy, dy, ngy),
        }

    near = [(dt, dz, dy) for dt in (-1, 0, 1) for dz in (-1, 0, 1) for dy in range(ngy)]
    centred = lambda d, n: (d + n // 2) % n - n // 2
    across = sorted(
        (cell for cell in slots if cell != (0, 0)),
        key=lambda c: -(abs(centred(c[0], nta)) + 2 * abs(centred(c[1], ngz))),
    )
    loads = []
    for t in range(size_t):
        loads.append((
            pltpu.make_async_copy(m_hbm.at[pl.ds(t, 1)], m_ref.at[pl.ds(t, 1)], loaded.at[0, t]),
            pltpu.make_async_copy(s_hbm.at[pl.ds(t, 1)], s_ref.at[pl.ds(t, 1)], loaded.at[1, t]),
        ))
    met = sorted({(dt % nta, dz % ngz, dy % ngy) for dt, dz, dy in near + [(-t, -z, 0) for t, z in across]} - {(0, 0, 0)})
    for t in [0, size_t - 1] + list(range(1, size_t - 1)):
        for load in loads[t]:
            load.start()
    barrier = pltpu.get_barrier_semaphore()
    for offset in met:
        pl.semaphore_signal(barrier, inc=1, device_id=device(*offset), device_id_type=MESH)

    def send(moves, sends, receives):
        copies = [
            pltpu.make_async_remote_copy(
                src_ref=source, dst_ref=target, send_sem=sends(place), recv_sem=receives(place),
                device_id=device(*offset), device_id_type=MESH,
            )
            for place, source, target, offset in moves
        ]
        for copy in copies:
            copy.start()
        sent.extend(copies)
        return copies

    def finish(copies):
        for copy in copies:
            copy.wait_recv()

    sent = []

    def finish_sends(copies):
        for copy in copies:
            copy.wait_send()

    inner_t, inner_z = pl.ds(1, size_t), pl.ds(1, size_z)

    def send0(number, moves):
        return send(moves, lambda place: f0s.at[number, place], lambda place: f0r.at[number, place])

    def exchange(number, field, faces, halos):
        copies = send0(number, [
            (4, faces.at[1], halos.at[0], (0, 0, 1)),
            (5, faces.at[0], halos.at[1], (0, 0, -1)),
            (2, field.at[inner_t, pl.ds(size_z, 1)], field.at[inner_t, pl.ds(0, 1)], (0, 1, 0)),
            (3, field.at[inner_t, pl.ds(1, 1)], field.at[inner_t, pl.ds(size_z + 1, 1)], (0, -1, 0)),
            (1, field.at[pl.ds(size_t, 1), inner_z], field.at[pl.ds(0, 1), inner_z], (1, 0, 0)),
            (0, field.at[pl.ds(1, 1), inner_z], field.at[pl.ds(size_t + 1, 1), inner_z], (-1, 0, 0)),
        ])
        return copies[:4], copies[4:]

    def layers1(deep_t, deep_z, corner_t):
        own_t, own_z = pl.ds(PAD_T, size_t1), pl.ds(PAD_Z, pairs1)

        def span(pad, size, deep, up):
            return pl.ds(pad + (size - deep) * up, deep), pl.ds(pad + size - (size + deep) * up, deep)

        moves = []
        for up in (1, 0):
            for up_z in (1, 0):
                here_t, there_t = span(PAD_T, size_t1, corner_t, up)
                here_z, there_z = span(PAD_Z, pairs1, 1, up_z)
                moves.append((here_t, here_z, there_t, there_z, 2 * up - 1, 2 * up_z - 1))
        for up in (1, 0):
            here, there = span(PAD_T, size_t1, deep_t, up)
            moves.append((here, own_z, there, own_z, 2 * up - 1, 0))
            here, there = span(PAD_Z, pairs1, deep_z, up)
            moves.append((own_t, here, own_t, there, 0, 2 * up - 1))
        return moves

    def spread1(number, field):
        part = pl.ds(gy, 1)
        own = field.at[pl.ds(PAD_T, size_t1), pl.ds(PAD_Z, pairs1), part]
        moves = [(8 * ngy + dy - 1, own, own, (0, 0, dy)) for dy in range(1, ngy)]
        for dy in reversed(range(ngy)):
            for place, (here_t, here_z, there_t, there_z, dt, dz) in enumerate(layers1(2, 1, 1)):
                moves.append((
                    8 * dy + place, field.at[here_t, here_z, part], field.at[there_t, there_z, part], (dt, dz, dy),
                ))
        return send(moves, lambda place: f1s.at[number, place], lambda place: f1r.at[number, place])

    def widen1(field):
        moves = [
            (place, field.at[here_t, here_z], field.at[there_t, there_z], (dt, dz, 0))
            for place, (here_t, here_z, there_t, there_z, dt, dz) in enumerate(layers1(3, 2, 2))
        ]
        return send(moves, lambda place: fxs.at[place], lambda place: fxr.at[place])

    def gather(number, field):
        own = field.at[slots[0, 0]]
        return send(
            [(slots[cell], own, field.at[slots[cell]], (-cell[0], -cell[1], 0)) for cell in across],
            lambda place: gsend.at[number, place], lambda place: grecv.at[number, place],
        )

    def put(field, faces, t, slab):
        field[t + 1, pl.ds(1, size_z)] = slab
        faces[0, t] = slab[:, :1]
        faces[1, t] = slab[:, rows - 1:]

    def sum0(field, halos, t):
        slab = field[t + 1, pl.ds(1, size_z)]
        row = lax.broadcasted_iota(jnp.int32, slab.shape, 1)
        summed = field[t, pl.ds(1, size_z)] + field[t + 2, pl.ds(1, size_z)]
        summed = summed + field[t + 1, pl.ds(0, size_z)] + field[t + 1, pl.ds(2, size_z)]
        summed = summed + jnp.where(row == 0, halos[0, t], rolled(slab, 1, 1))
        summed = summed + jnp.where(row == rows - 1, halos[1, t], rolled(slab, -1, 1))
        return slab, summed + rolled(slab, 1, 2) + rolled(slab, -1, 2)

    def folded(summed, place):
        count, high, _ = summed.shape
        view = fold.at[place, pl.ds(0, count)]
        view[...] = summed
        return view[:, pl.ds(0, high // 2, stride=2), :] + view[:, pl.ds(1, high // 2, stride=2), :]

    def to_level1(summed, place):
        summed = folded(z_pairs(summed), place)
        summed = summed.reshape(summed.shape[0] // 2, 2, *summed.shape[1:])
        even, odd = summed[:, 0], summed[:, 1]
        even, odd = even + rolled(even, -1, 2), odd + rolled(odd, 1, 2)
        return jnp.where(odd_lane(even), odd, even) * 0.0625

    def doubled(slab, place):
        count, high, _ = slab.shape
        view = fold.at[place, pl.ds(0, count)]
        view[:, pl.ds(0, high, stride=2), :] = slab
        view[:, pl.ds(1, high, stride=2), :] = slab
        return view[...]

    full = ngy * rows1

    def near1(radius):
        for t in range(-radius, size_t1 + radius):
            reach = (radius - max(-t, t - size_t1 + 1, 0) + 1) // 2
            yield t, -reach, pairs1 + 2 * reach

    def read1(field, t, z, count):
        return field[PAD_T + t, pl.ds(PAD_Z + z, count)].reshape(count, full, lanes)

    def write1(field, t, z, slab):
        field[PAD_T + t, pl.ds(PAD_Z + z, slab.shape[0])] = slab.reshape(slab.shape[0], ngy, rows1, lanes)

    def sum1(field, t, z, count, held):
        slab = read1(field, t, z, count)
        summed = read1(field, t - 1, z, count) + read1(field, t + 1, z, count)
        if held[t][0] < z:
            before, after = read1(field, t, z - 1, count), read1(field, t, z + 1, count)
        else:
            before = jnp.concatenate([slab[:1], slab[:-1]], axis=0)
            after = jnp.concatenate([slab[1:], slab[-1:]], axis=0)
        summed = summed + jnp.where(odd_lane(slab), rolled(slab + after, 1, 2), rolled(slab + before, -1, 2))
        summed = summed + rolled(slab, 1, 1) + rolled(slab, -1, 1)
        return slab, summed + rolled(slab, 2, 2) + rolled(slab, -2, 2)

    held1 = [{t: (z, count) for t, z, count in near1(radius)} for radius in range(4)]

    def sweep1(field, out, radius):
        for t, z, count in near1(radius):
            slab, summed = sum1(field, t, z, count, held1[radius + 1])
            fresh = KEEP * slab + read1(g1, t, z, count) * (read1(s1, t, z, count) + 0.5 * summed)
            write1(out, t, z, fresh)

    def packed(out, slabs):
        parts = [slab[z] for slab in slabs for z in range(part_z)]
        lane = lax.broadcasted_iota(jnp.int32, parts[0].shape, 1)
        values = parts[0]
        for k in range(1, len(parts)):
            values = jnp.where(lane % 4 == k, parts[k], values)
        out[slots[0, 0]] = values

    inside = list(range(1, size_t - 1))
    ends = [0, size_t - 1]

    def first0(ts):
        for t in ts:
            for load in loads[t]:
                load.wait()
            weight = DAMPING / (8.0 + m_ref[t])
            g0[t] = weight
            put(v0a, ys0.at[0], t, weight * s_ref[t])

    first0(ends + inside)
    pl.semaphore_wait(barrier, len(met))
    sides, over_t = exchange(0, v0a, ys0.at[0], y0.at[0])
    for t in range(size_t1):
        m1[PAD_T + t, pl.ds(PAD_Z, pairs1), gy] = to_level1(m_ref[2 * t] + m_ref[2 * t + 1], t)
    mass_copies = spread1(0, m1)

    def sweep0(field, halos, out, faces, ts, also=None):
        for t in ts:
            slab, summed = sum0(field, halos, t)
            fresh = KEEP * slab + g0[t] * (s_ref[t] + summed)
            put(out, faces, t, fresh)
            if also is not None:
                also[t] = fresh

    finish(sides)
    sweep0(v0a, y0.at[0], v0b, ys0.at[1], inside)
    finish(over_t)
    sweep0(v0a, y0.at[0], v0b, ys0.at[1], ends)
    sides, over_t = exchange(1, v0b, ys0.at[1], y0.at[1])
    finish(mass_copies)
    for a, b, count in near1(2):
        write1(g1, a, b, DAMPING / (4.0 + read1(m1, a, b, count)))

    def to_level2(slabs):
        out = []
        for t in range(part_t):
            summed = folded(slabs[2 * t] + slabs[2 * t + 1], t)
            summed = summed + pair_swap(summed, 1, 2)
            out.append((summed + pair_swap(summed, 2, 2)) * 0.0625)
        return out

    packed(m2, to_level2([read1(m1, t, 0, pairs1) for t in range(size_t1)]))
    mass_copies = gather(0, m2)

    def remainder0(ts):
        for t in ts:
            remainder = []
            for odd in range(2):
                slab, summed = sum0(v0b, y0.at[1], 2 * t + odd)
                remainder.append(s_ref[2 * t + odd] + summed - (8.0 + m_ref[2 * t + odd]) * slab)
            s1[PAD_T + t, pl.ds(PAD_Z, pairs1), gy] = to_level1(remainder[0] + remainder[1], t)

    finish(sides)
    remainder0(range(1, size_t1 - 1))
    finish(over_t)
    remainder0((0, size_t1 - 1))
    source_copies = spread1(1, s1)
    def take(field, places, cells):
        return jnp.stack([field[places[cell]] for cell in cells])

    def put3(field, cells, values):
        field[pl.ds(slots3[cells[0]], len(cells))] = values

    finish(mass_copies)
    for cell in stages["source"]:
        g2[slots[cell]] = DAMPING / (2.0 + m2[slots[cell]])
    for cells in batches(stages["coarse"][3], 24):
        put3(m3, cells, DAMPING / (1.0 + coarsened3(take(m2, slots, cells))))
    finish(source_copies)

    for a, b, count in near1(2):
        write1(v1a, a, b, read1(g1, a, b, count) * read1(s1, a, b, count))
    sweep1(v1a, v1b, 1)
    remainder = []
    for a, b, count in near1(0):
        slab, summed = sum1(v1b, a, b, count, held1[1])
        write1(v1h, a, b, slab)
        remainder.append(
            read1(s1, a, b, count) + 0.5 * summed - (4.0 + read1(m1, a, b, count)) * slab
        )
    packed(s2, to_level2(remainder))
    source_copies = gather(1, s2)
    wide_copies = widen1(v1h)
    finish(source_copies)

    def around2(cell):
        t, z = cell
        return [((t + dt) % nta, (z + dz) % ngz) for dt, dz in ((-1, 0), (1, 0), (0, -1), (0, 1))]

    def sum2(field, cell):
        slab = field[slots[cell]]
        before_t, after_t, before_z, after_z = [
            slab + field[slots[other]] if other in slots else slab for other in around2(cell)
        ]
        lane = place_in(slab, 1)
        summed = jnp.where(lane % 4 >= 2, rolled(after_t, 2, 1), rolled(before_t, -2, 1))
        summed = summed + jnp.where(lane % 2 == 1, rolled(after_z, 1, 1), rolled(before_z, -1, 1))
        summed = summed + rolled(slab, 1, 0) + rolled(slab, -1, 0)
        return slab, summed + rolled(slab, 4, 1) + rolled(slab, -4, 1)

    def sweep2(field, out, cells):
        for cell in cells:
            slab, summed = sum2(field, cell)
            at = slots[cell]
            out[at] = KEEP * slab + g2[at] * (s2[at] + 0.25 * summed)

    for cell in stages["source"]:
        at = slots[cell]
        u2[at] = g2[at] * s2[at]
        w2[at] = u2[at]
    sweep2(u2, w2, stages["swept"])
    for cell in stages["coarse"][3]:
        slab, summed = sum2(w2, cell)
        at = slots[cell]
        s3[slots3[cell]] = s2[at] + 0.25 * summed - (2.0 + m2[at]) * slab
    for cells in batches(stages["coarse"][3], 24):
        source = coarsened3(take(s3, slots3, cells))
        put3(s3, cells, source)
        put3(u3, cells, take(m3, slots3, cells) * source)
    old, new = u3, w3
    for steps in (2, 1, 0):
        for cells in batches(stages["coarse"][steps], 13):
            slab = take(old, slots3, cells)
            near3 = list(zip(*[around2(cell) for cell in cells]))
            summed = take(old, slots3, near3[0]) + take(old, slots3, near3[1])
            summed = summed + take(old, slots3, near3[2]) + take(old, slots3, near3[3])
            summed = summed + rolled(slab, 2, 1) + rolled(slab, -2, 1)
            summed = summed + rolled(slab, 8, 2) + rolled(slab, -8, 2)
            fresh = KEEP * slab + take(m3, slots3, cells) * (take(s3, slots3, cells) + 0.125 * summed)
            for number, cell in enumerate(cells):
                new[slots3[cell]] = fresh[number]
        old, new = new, old
    for cells in batches(stages["base"], 24):
        fine = refined3(take(old, slots3, cells))
        for number, cell in enumerate(cells):
            w2[slots[cell]] = w2[slots[cell]] + fine[number]
    for cell in stages["base"]:
        u2[slots[cell]] = w2[slots[cell]]
    sweep2(w2, u2, stages["first"])
    sweep2(u2, w2, stages["last"])

    def correct1(t, z):
        piece = piece2(w2[slots[t // 2 % nta, z // 2 % ngz]], t % 2, z % 2)
        e2[t + 2, z + 2, pl.ds(0, full // 2, stride=2), :] = piece
        e2[t + 2, z + 2, pl.ds(1, full // 2, stride=2), :] = piece

    for t in range(-2, part_t + 2):
        for z in range(-2, part_z + 2):
            if max(-t, t - part_t + 1, 0) + max(-z, z - part_z + 1, 0) <= 2:
                correct1(t, z)
    finish(wide_copies)
    for t, z, count in near1(3):
        write1(v1w, t, z, read1(v1h, t, z, count) + e2[t // 2 + 2, pl.ds(z + 2, count)])
    sweep1(v1w, v1x, 2)
    sweep1(v1x, e1, 1)

    under = lax.rem(gy + ngy - 1, ngy)
    over = lax.rem(gy + 1, ngy)

    def split1(slab):
        even = jnp.where(odd_lane(slab), rolled(slab, 1, 2), slab)
        odd = jnp.where(odd_lane(slab), slab, rolled(slab, -1, 2))
        return jnp.stack([even, odd], axis=1).reshape(2 * slab.shape[0], *slab.shape[1:])

    def corrected0(layers):
        for t in layers:
            own = [p for p in (2 * t + 1, 2 * t + 2) if 1 <= p <= size_t]
            if not own:
                p = 0 if t < 0 else size_t + 1
                fine = refined_z(doubled(split1(e1[PAD_T + t, pl.ds(PAD_Z, pairs1), gy]), 0))
                v0w[p, inner_z] = v0b[p, inner_z] + fine
                continue
            fine = split1(e1[PAD_T + t, pl.ds(PAD_Z - 1, pairs1 + 2), gy])
            fine = refined_z(doubled(fine[1:-1], t % 4))
            fine = fine[1:1 + size_z + 2]
            low = refined_z(split1(e1[PAD_T + t, pl.ds(PAD_Z, pairs1), under, pl.ds(rows1 - 1, 1)]))
            high = refined_z(split1(e1[PAD_T + t, pl.ds(PAD_Z, pairs1), over, pl.ds(0, 1)]))
            for p in own:
                v0w[p] = v0b[p] + fine
                y0[2, 0, p - 1] = y0[1, 0, p - 1] + low
                y0[2, 1, p - 1] = y0[1, 1, p - 1] + high

    corrected0(range(-1, size_t1 + 1))
    sweep0(v0w, y0.at[2], v0x, ys0.at[2], range(size_t))
    sides, over_t = exchange(2, v0x, ys0.at[2], y0.at[3])
    finish(sides)
    sweep0(v0x, y0.at[3], v0s, ys0.at[3], inside, sol_ref)
    finish(over_t)
    sweep0(v0x, y0.at[3], v0s, ys0.at[3], ends, sol_ref)
    earlier = len(sent)
    sides, over_t = exchange(3, v0s, ys0.at[3], y0.at[4])
    finish_sends(sent[:earlier])

    def residual(ts):
        for t in ts:
            slab, summed = sum0(v0s, y0.at[4], t)
            res_ref[t] = s_ref[t] + summed - (8.0 + m_ref[t]) * slab

    finish(sides)
    residual(inside)
    finish(over_t)
    residual(ends)
    finish_sends(sent[earlier:])


def place_in(values, axis):
    return lax.broadcasted_iota(jnp.int32, values.shape, axis)


def coarsened3(values):
    for step in (1, 2, 4):
        values = values + rolled(values, -step, 2)
    return (values + rolled(values, -1, 1)) * 0.0625


def refined3(values):
    corner = (place_in(values, 2) % 8 == 0) & (place_in(values, 1) % 2 == 0)
    values = jnp.where(corner, values, 0.0)
    values = values + rolled(values, 1, 1)
    for step in (1, 2, 4):
        values = values + rolled(values, step, 2)
    return values


def piece2(values, odd_t, odd_z):
    values = jnp.where(place_in(values, 1) % 4 == 2 * odd_t + odd_z, values, 0.0)
    values = values + rolled(values, -1 if odd_z else 1, 1)
    return values + rolled(values, -2 if odd_t else 2, 1)


def batches(cells, most):
    count = -(-len(cells) // most)
    size = -(-len(cells) // count)
    return [cells[at:at + size] for at in range(0, len(cells), size)]


def grown(cells, steps, count_t, count_z):
    for _ in range(steps):
        cells = cells | {
            ((t + dt) % count_t, (z + dz) % count_z)
            for t, z in cells for dt, dz in ((-1, 0), (1, 0), (0, -1), (0, 1))
        }
    return cells


def plan(nta, ngz):
    sites = lambda cells, steps: grown(cells, steps, 2 * nta, 2 * ngz)
    blocks = lambda cells: {(t // 2, z // 2) for t, z in cells}
    inner = lambda cells: {(2 * t + a, 2 * z + b) for t, z in cells for a in (0, 1) for b in (0, 1)}
    last = sites(inner({(0, 0)}), 2)
    first, base = sites(last, 1), sites(last, 2)
    coarse = [grown(blocks(base), steps, nta, ngz) for steps in range(4)]
    swept = sites(inner(coarse[3]), 1) | base
    ordered = lambda cells: sorted(cells, key=lambda c: ((c[0] + nta // 2) % nta, (c[1] + ngz // 2) % ngz))
    return {
        "last": ordered(blocks(last)), "first": ordered(blocks(first)), "base": ordered(blocks(base)),
        "coarse": [ordered(cells) for cells in coarse], "swept": ordered(blocks(swept)),
        "source": ordered(blocks(sites(swept, 1))),
    }


def per_device(sizes, right_side, mass_field):
    nta, ngz, ngy = sizes
    size_t, size_z, rows, lanes = right_side.shape
    size_t1, pairs1, rows1 = size_t // 2, size_z // 4, rows // 2
    part_t, part_z, rows2 = size_t // 4, size_z // 4, rows // 4
    vmem = lambda *shape: pltpu.VMEM(shape, jnp.float32)
    dma = lambda *shape: pltpu.SemaphoreType.DMA(shape)
    padded0 = vmem(size_t + 2, size_z + 2, rows, lanes)
    padded1 = vmem(size_t1 + 2 * PAD_T, pairs1 + 2 * PAD_Z, ngy, rows1, lanes)
    window = len(plan(nta, ngz)["source"])
    packs = vmem(window, rows2 * ngy, lanes)
    packs3 = vmem(len(plan(nta, ngz)["coarse"][3]), rows2 * ngy, lanes)
    spreads = 8 * ngy + ngy - 1
    scratch = [
        vmem(size_t, size_z, rows, lanes), padded0, padded0, padded0, padded0, padded0,
        vmem(5, 2, size_t, size_z, 1, lanes), vmem(4, 2, size_t, size_z, 1, lanes),
        vmem(max(size_t1, part_t + 2), size_z, max(rows, ngy * rows1), lanes),
        *[padded1] * 9, vmem(part_t + 4, part_z + 4, ngy * rows1, lanes),
        *[packs] * 5, *[packs3] * 4,
        dma(4, 6), dma(4, 6), dma(2, spreads), dma(2, spreads), dma(8), dma(8),
        dma(2, window), dma(2, window),
        vmem(size_t, size_z, rows, lanes), vmem(size_t, size_z, rows, lanes), dma(2, size_t),
    ]
    block = jax.ShapeDtypeStruct(right_side.shape, jnp.float32)
    return pl.pallas_call(
        functools.partial(kernel, sizes),
        out_shape=(block, block),
        in_specs=[pl.BlockSpec(memory_space=pltpu.HBM)] * 2,
        out_specs=(pl.BlockSpec(memory_space=pltpu.VMEM),) * 2,
        scratch_shapes=scratch,
        compiler_params=pltpu.CompilerParams(
            collective_id=0, has_side_effects=True, vmem_limit_bytes=48 * 1024 * 1024
        ),
    )(*[pltpu.with_memory_space_constraint(values, pltpu.HBM) for values in (right_side, mass_field)])


def solution(mesh):
    sizes = tuple(mesh.shape[axis] for axis in ("ta", "gz", "gy"))
    spec = P("ta", "gz", "gy", None)
    return jax.shard_map(
        functools.partial(per_device, sizes),
        mesh=mesh,
        in_specs=(spec, spec),
        out_specs=(spec, spec),
        check_vma=False,
    )
```

```python
import functools

import jax
import jax.numpy as jnp
from jax import lax
from jax.experimental import pallas as pl
from jax.experimental.pallas import tpu as pltpu
from jax.sharding import PartitionSpec as P

DAMPING = 0.7
KEEP = 1.0 - DAMPING
PAD0, PAD_T, PAD_Z = 2, 3, 2
MESH = pl.DeviceIdType.MESH


def rolled(values, shift, axis):
    return pltpu.roll(values, shift % values.shape[axis], axis)


def odd_lane(values):
    return lax.broadcasted_iota(jnp.int32, values.shape, values.ndim - 1) % 2 == 1


def pair_swap(values, step, axis):
    index = lax.broadcasted_iota(jnp.int32, values.shape, axis)
    return jnp.where((index // step) % 2 == 0, rolled(values, -step, axis), rolled(values, step, axis))


def z_pairs(summed):
    count, rows, lanes = summed.shape
    summed = summed.reshape(count // 2, 2, rows, lanes)
    return summed[:, 0] + summed[:, 1]


def refined_z(slab):
    return jnp.repeat(slab, 2, axis=0)


def kernel(sizes, s_hbm, m_hbm, sol_ref, res_ref, *scratch):
    nta, ngz, ngy = sizes
    (g0, v0a, v0b, v0w, v0x, v0s, y0, ys0, y2, ys2, yg, ysg, fold,
     s1, m1, g1, v1a, v1b, v1h, v1w, v1x, e1, e2,
     m2, s2, g2, u2, w2, m3, s3, u3, w3,
     f0s, f0r, fhs, fhr, f1s, f1r, fxs, fxr, gsend, grecv, s_ref, m_ref, loaded) = scratch
    size_t, size_z, rows, lanes = s_ref.shape
    size_t1, pairs1, rows1 = size_t // 2, size_z // 4, rows // 2
    part_t, part_z, rows2 = size_t // 4, size_z // 4, rows // 4
    stages = plan(nta, ngz)
    slots = {cell: number for number, cell in enumerate(stages["source"])}
    slots3 = {cell: number for number, cell in enumerate(stages["coarse"][3])}
    ta, gz, gy = lax.axis_index("ta"), lax.axis_index("gz"), lax.axis_index("gy")

    places = {}

    def place_of(axis, at, step, count):
        key = axis, step % count
        if key not in places:
            places[key] = at if key[1] == 0 else lax.rem(at + key[1], count)
        return places[key]

    def device(dt, dz, dy):
        return {
            "ta": place_of("ta", ta, dt, nta), "gz": place_of("gz", gz, dz, ngz), "gy": place_of("gy", gy, dy, ngy),
        }

    near = [(dt, dz, dy) for dt in (-1, 0, 1) for dz in (-1, 0, 1) for dy in range(ngy)]
    centred = lambda d, n: (d + n // 2) % n - n // 2
    across = sorted(
        (cell for cell in slots if cell != (0, 0)),
        key=lambda c: -(abs(centred(c[0], nta)) + 2 * abs(centred(c[1], ngz))),
    )
    loads = []
    for t in range(size_t):
        loads.append((
            pltpu.make_async_copy(m_hbm.at[pl.ds(t, 1)], m_ref.at[pl.ds(t, 1)], loaded.at[0, t]),
            pltpu.make_async_copy(s_hbm.at[pl.ds(t, 1)], s_ref.at[pl.ds(t, 1)], loaded.at[1, t]),
        ))
    met = sorted({(dt % nta, dz % ngz, dy % ngy) for dt, dz, dy in near + [(-t, -z, 0) for t, z in across]} - {(0, 0, 0)})
    for t in [0, size_t - 1] + list(range(1, size_t - 1)):
        for load in loads[t]:
            load.start()
    barrier = pltpu.get_barrier_semaphore()
    for offset in met:
        pl.semaphore_signal(barrier, inc=1, device_id=device(*offset), device_id_type=MESH)

    def send(moves, sends, receives):
        copies = [
            pltpu.make_async_remote_copy(
                src_ref=source, dst_ref=target, send_sem=sends(place), recv_sem=receives(place),
                device_id=device(*offset), device_id_type=MESH,
            )
            for place, source, target, offset in moves
        ]
        for copy in copies:
            copy.start()
        sent.extend(copies)
        return copies

    def finish(copies):
        for copy in copies:
            copy.wait_recv()

    sent = []

    def finish_sends(copies):
        for copy in copies:
            copy.wait_send()

    inner_t, inner_z = pl.ds(PAD0, size_t), pl.ds(PAD0, size_z)

    def faces0(field, depth):
        one = lambda at: pl.ds(PAD0 + at, 1)
        return [
            (field.at[inner_t, one(size_z - depth)], field.at[inner_t, one(-depth)], (0, 1, 0)),
            (field.at[inner_t, one(depth - 1)], field.at[inner_t, one(size_z - 1 + depth)], (0, -1, 0)),
            (field.at[one(size_t - depth), inner_z], field.at[one(-depth), inner_z], (1, 0, 0)),
            (field.at[one(depth - 1), inner_z], field.at[one(size_t - 1 + depth), inner_z], (-1, 0, 0)),
        ]

    own_t, own_z = pl.ds(1, size_t), pl.ds(1, size_z)

    def exchange(number, field):
        faces, halos = ys0.at[number], y0.at[(0, 1, 4)[number]]
        moves = [
            (faces.at[1], halos.at[0, own_t, own_z], (0, 0, 1)), (faces.at[0], halos.at[1, own_t, own_z], (0, 0, -1)),
        ] + faces0(field, 1)
        copies = send(
            [(place, *move) for place, move in enumerate(moves)],
            lambda place: f0s.at[number, place], lambda place: f0r.at[number, place],
        )
        return copies[:4], copies[4:]

    def behind():
        one = lambda at: pl.ds(at, 1)
        moves = [
            (ys2.at[1], y2.at[0, 0], (0, 0, 1)), (ys2.at[0], y2.at[0, 1], (0, 0, -1)),
            (ysg.at[1], yg.at[0], (0, 0, 1)), (ysg.at[0], yg.at[1], (0, 0, -1)),
        ]
        for up_t in (1, 0):
            for up_z in (1, 0):
                moves.append((
                    v0b.at[one(PAD0 + (size_t - 1) * up_t), one(PAD0 + (size_z - 1) * up_z)],
                    v0b.at[one(PAD0 - 1 + (size_t + 1) * (1 - up_t)), one(PAD0 - 1 + (size_z + 1) * (1 - up_z))],
                    (2 * up_t - 1, 2 * up_z - 1, 0),
                ))
        for up_y in (1, 0):
            faces, halos = ys0.at[1, up_y], y0.at[1, 1 - up_y]
            for up in (1, 0):
                moves.append((
                    faces.at[one((size_t - 1) * up)], halos.at[one((size_t + 1) * (1 - up)), own_z],
                    (2 * up - 1, 0, 2 * up_y - 1),
                ))
                moves.append((
                    faces.at[:, one((size_z - 1) * up)], halos.at[own_t, one((size_z + 1) * (1 - up))],
                    (0, 2 * up - 1, 2 * up_y - 1),
                ))
        moves += faces0(v0b, 2) + faces0(g0, 1)
        return send(
            [(place, *move) for place, move in enumerate(moves)],
            lambda place: fhs.at[place], lambda place: fhr.at[place],
        )

    def layers1(deep_t, deep_z, corner_t):
        own_t, own_z = pl.ds(PAD_T, size_t1), pl.ds(PAD_Z, pairs1)

        def span(pad, size, deep, up):
            return pl.ds(pad + (size - deep) * up, deep), pl.ds(pad + size - (size + deep) * up, deep)

        moves = []
        for up in (1, 0):
            for up_z in (1, 0):
                here_t, there_t = span(PAD_T, size_t1, corner_t, up)
                here_z, there_z = span(PAD_Z, pairs1, 1, up_z)
                moves.append((here_t, here_z, there_t, there_z, 2 * up - 1, 2 * up_z - 1))
        for up in (1, 0):
            here, there = span(PAD_T, size_t1, deep_t, up)
            moves.append((here, own_z, there, own_z, 2 * up - 1, 0))
            here, there = span(PAD_Z, pairs1, deep_z, up)
            moves.append((own_t, here, own_t, there, 0, 2 * up - 1))
        return moves

    def spread1(number, field):
        part = pl.ds(gy, 1)
        own = field.at[pl.ds(PAD_T, size_t1), pl.ds(PAD_Z, pairs1), part]
        moves = [(8 * ngy + dy - 1, own, own, (0, 0, dy)) for dy in range(1, ngy)]
        for dy in reversed(range(ngy)):
            for place, (here_t, here_z, there_t, there_z, dt, dz) in enumerate(layers1(2, 1, 2)):
                moves.append((
                    8 * dy + place, field.at[here_t, here_z, part], field.at[there_t, there_z, part], (dt, dz, dy),
                ))
        return send(moves, lambda place: f1s.at[number, place], lambda place: f1r.at[number, place])

    def widen1(field):
        moves = [
            (place, field.at[here_t, here_z], field.at[there_t, there_z], (dt, dz, 0))
            for place, (here_t, here_z, there_t, there_z, dt, dz) in enumerate(layers1(3, 2, 3))
        ]
        one = lambda at: pl.ds(at, 1)
        for up in (1, 0):
            for up_z in (1, 0):
                moves.append((
                    len(moves),
                    field.at[one(PAD_T + (size_t1 - 1) * up), one(PAD_Z + 1 + (pairs1 - 3) * up_z)],
                    field.at[one(PAD_T - 1 + (size_t1 + 1) * (1 - up)), one(PAD_Z - 2 + (pairs1 + 3) * (1 - up_z))],
                    (2 * up - 1, 2 * up_z - 1, 0),
                ))
        return send(moves, lambda place: fxs.at[place], lambda place: fxr.at[place])

    def gather(number, field):
        own = field.at[slots[0, 0]]
        return send(
            [(slots[cell], own, field.at[slots[cell]], (-cell[0], -cell[1], 0)) for cell in across],
            lambda place: gsend.at[number, place], lambda place: grecv.at[number, place],
        )

    def put(field, faces, t, slab):
        field[PAD0 + t, inner_z] = slab
        faces[0, t] = slab[:, :1]
        faces[1, t] = slab[:, rows - 1:]

    def sum0(field, halos, t, reach=0):
        count = size_z + 2 * reach
        at = lambda dt, dz: field[PAD0 + t + dt, pl.ds(PAD0 - reach + dz, count)]
        slab, out = at(0, 0), pl.ds(1 - reach, count)
        row = lax.broadcasted_iota(jnp.int32, slab.shape, 1)
        summed = at(-1, 0) + at(1, 0) + at(0, -1) + at(0, 1)
        summed = summed + jnp.where(row == 0, halos[0, 1 + t, out], rolled(slab, 1, 1))
        summed = summed + jnp.where(row == rows - 1, halos[1, 1 + t, out], rolled(slab, -1, 1))
        return slab, summed + rolled(slab, 1, 2) + rolled(slab, -1, 2)

    def folded(summed, place):
        count, high, _ = summed.shape
        view = fold.at[place, pl.ds(0, count)]
        view[...] = summed
        return view[:, pl.ds(0, high // 2, stride=2), :] + view[:, pl.ds(1, high // 2, stride=2), :]

    def to_level1(summed, place):
        summed = folded(z_pairs(summed), place)
        summed = summed.reshape(summed.shape[0] // 2, 2, *summed.shape[1:])
        even, odd = summed[:, 0], summed[:, 1]
        even, odd = even + rolled(even, -1, 2), odd + rolled(odd, 1, 2)
        return jnp.where(odd_lane(even), odd, even) * 0.0625

    def doubled(slab, place):
        count, high, _ = slab.shape
        view = fold.at[place, pl.ds(0, count)]
        view[:, pl.ds(0, high, stride=2), :] = slab
        view[:, pl.ds(1, high, stride=2), :] = slab
        return view[...]

    full = ngy * rows1

    def area1(*reaches):
        far = len(reaches) - 1
        for t in range(-far, size_t1 + far):
            reach = reaches[max(-t, t - size_t1 + 1, 0)]
            yield t, -reach, pairs1 + 2 * reach

    def read1(field, t, z, count):
        return field[PAD_T + t, pl.ds(PAD_Z + z, count)].reshape(count, full, lanes)

    def write1(field, t, z, slab):
        field[PAD_T + t, pl.ds(PAD_Z + z, slab.shape[0])] = slab.reshape(slab.shape[0], ngy, rows1, lanes)

    def sum1(field, t, z, count, held):
        slab = read1(field, t, z, count)
        summed = read1(field, t - 1, z, count) + read1(field, t + 1, z, count)
        if held[t][0] < z:
            before, after = read1(field, t, z - 1, count), read1(field, t, z + 1, count)
        else:
            before = jnp.concatenate([slab[:1], slab[:-1]], axis=0)
            after = jnp.concatenate([slab[1:], slab[-1:]], axis=0)
        summed = summed + jnp.where(odd_lane(slab), rolled(slab + after, 1, 2), rolled(slab + before, -1, 2))
        summed = summed + rolled(slab, 1, 1) + rolled(slab, -1, 1)
        return slab, summed + rolled(slab, 2, 2) + rolled(slab, -2, 2)

    def sweep1(field, out, area, held):
        held = {t: (z, count) for t, z, count in area1(*held)}
        for t, z, count in area1(*area):
            slab, summed = sum1(field, t, z, count, held)
            fresh = KEEP * slab + read1(g1, t, z, count) * (read1(s1, t, z, count) + 0.5 * summed)
            write1(out, t, z, fresh)

    def packed(out, slabs):
        parts = [slab[z] for slab in slabs for z in range(part_z)]
        lane = lax.broadcasted_iota(jnp.int32, parts[0].shape, 1)
        values = parts[0]
        for k in range(1, len(parts)):
            values = jnp.where(lane % 4 == k, parts[k], values)
        out[slots[0, 0]] = values

    inside = list(range(1, size_t - 1))
    ends = [0, size_t - 1]

    def first0(ts):
        for t in ts:
            for load in loads[t]:
                load.wait()
            weight = DAMPING / (8.0 + m_ref[t])
            put(g0, ysg, t, weight)
            put(v0a, ys0.at[0], t, weight * s_ref[t])

    first0(ends + inside)
    pl.semaphore_wait(barrier, len(met))
    sides, over_t = exchange(0, v0a)
    for t in range(size_t1):
        m1[PAD_T + t, pl.ds(PAD_Z, pairs1), gy] = to_level1(m_ref[2 * t] + m_ref[2 * t + 1], t)
    mass_copies = spread1(0, m1)

    def sweep0(field, halos, out, faces, ts, also=None):
        for t in ts:
            slab, summed = sum0(field, halos, t)
            fresh = KEEP * slab + g0[PAD0 + t, inner_z] * (s_ref[t] + summed)
            put(out, faces, t, fresh)
            if also is not None:
                also[t] = fresh

    finish(sides)
    sweep0(v0a, y0.at[0], v0b, ys0.at[1], inside)
    finish(over_t)
    sweep0(v0a, y0.at[0], v0b, ys0.at[1], ends)
    for t in range(size_t):
        ys2[0, t] = v0b[PAD0 + t, inner_z, pl.ds(1, 1)]
        ys2[1, t] = v0b[PAD0 + t, inner_z, pl.ds(rows - 2, 1)]
    sides, over_t = exchange(1, v0b)
    finish(mass_copies)
    for a, b, count in area1(1, 1, 1):
        write1(g1, a, b, DAMPING / (4.0 + read1(m1, a, b, count)))

    def to_level2(slabs):
        out = []
        for t in range(part_t):
            summed = folded(slabs[2 * t] + slabs[2 * t + 1], t)
            summed = summed + pair_swap(summed, 1, 2)
            out.append((summed + pair_swap(summed, 2, 2)) * 0.0625)
        return out

    packed(m2, to_level2([read1(m1, t, 0, pairs1) for t in range(size_t1)]))
    mass_copies = gather(0, m2)

    def remainder0(ts):
        for t in ts:
            remainder = []
            for odd in range(2):
                slab, summed = sum0(v0b, y0.at[1], 2 * t + odd)
                remainder.append(s_ref[2 * t + odd] + summed - (8.0 + m_ref[2 * t + odd]) * slab)
            s1[PAD_T + t, pl.ds(PAD_Z, pairs1), gy] = to_level1(remainder[0] + remainder[1], t)

    finish(sides)
    remainder0(range(1, size_t1 - 1))
    finish(over_t)
    remainder0((0, size_t1 - 1))
    source_copies = spread1(1, s1)
    behind_copies = behind()
    def take(field, places, cells):
        return jnp.stack([field[places[cell]] for cell in cells])

    def put3(field, cells, values):
        field[pl.ds(slots3[cells[0]], len(cells))] = values

    finish(mass_copies)
    for cell in stages["source"]:
        g2[slots[cell]] = DAMPING / (2.0 + m2[slots[cell]])
    for cells in batches(stages["coarse"][3], 24):
        put3(m3, cells, DAMPING / (1.0 + coarsened3(take(m2, slots, cells))))
    finish(source_copies)

    for a, b, count in area1(1, 1, 0):
        write1(v1a, a, b, read1(g1, a, b, count) * read1(s1, a, b, count))
    sweep1(v1a, v1b, (1, 0), (1, 1, 0))
    remainder = []
    held = {t: (z, count) for t, z, count in area1(1, 0)}
    for a, b, count in area1(0):
        slab, summed = sum1(v1b, a, b, count, held)
        write1(v1h, a, b, slab)
        remainder.append(
            read1(s1, a, b, count) + 0.5 * summed - (4.0 + read1(m1, a, b, count)) * slab
        )
    packed(s2, to_level2(remainder))
    source_copies = gather(1, s2)
    wide_copies = widen1(v1h)
    finish(source_copies)

    def around2(cell):
        t, z = cell
        return [((t + dt) % nta, (z + dz) % ngz) for dt, dz in ((-1, 0), (1, 0), (0, -1), (0, 1))]

    def sum2(field, cell):
        slab = field[slots[cell]]
        before_t, after_t, before_z, after_z = [
            slab + field[slots[other]] if other in slots else slab for other in around2(cell)
        ]
        lane = place_in(slab, 1)
        summed = jnp.where(lane % 4 >= 2, rolled(after_t, 2, 1), rolled(before_t, -2, 1))
        summed = summed + jnp.where(lane % 2 == 1, rolled(after_z, 1, 1), rolled(before_z, -1, 1))
        summed = summed + rolled(slab, 1, 0) + rolled(slab, -1, 0)
        return slab, summed + rolled(slab, 4, 1) + rolled(slab, -4, 1)

    def sweep2(field, out, cells):
        for cell in cells:
            slab, summed = sum2(field, cell)
            at = slots[cell]
            out[at] = KEEP * slab + g2[at] * (s2[at] + 0.25 * summed)

    for cell in stages["source"]:
        at = slots[cell]
        u2[at] = g2[at] * s2[at]
        w2[at] = u2[at]
    sweep2(u2, w2, stages["swept"])
    for cell in stages["coarse"][3]:
        slab, summed = sum2(w2, cell)
        at = slots[cell]
        s3[slots3[cell]] = s2[at] + 0.25 * summed - (2.0 + m2[at]) * slab
    for cells in batches(stages["coarse"][3], 24):
        source = coarsened3(take(s3, slots3, cells))
        put3(s3, cells, source)
        put3(u3, cells, take(m3, slots3, cells) * source)
    old, new = u3, w3
    for steps in (2, 1, 0):
        for cells in batches(stages["coarse"][steps], 13):
            slab = take(old, slots3, cells)
            near3 = list(zip(*[around2(cell) for cell in cells]))
            summed = take(old, slots3, near3[0]) + take(old, slots3, near3[1])
            summed = summed + take(old, slots3, near3[2]) + take(old, slots3, near3[3])
            summed = summed + rolled(slab, 2, 1) + rolled(slab, -2, 1)
            summed = summed + rolled(slab, 8, 2) + rolled(slab, -8, 2)
            fresh = KEEP * slab + take(m3, slots3, cells) * (take(s3, slots3, cells) + 0.125 * summed)
            for number, cell in enumerate(cells):
                new[slots3[cell]] = fresh[number]
        old, new = new, old
    for cells in batches(stages["base"], 24):
        fine = refined3(take(old, slots3, cells))
        for number, cell in enumerate(cells):
            w2[slots[cell]] = w2[slots[cell]] + fine[number]
    for cell in stages["base"]:
        u2[slots[cell]] = w2[slots[cell]]
    sweep2(w2, u2, stages["first"])
    sweep2(u2, w2, stages["last"])

    def correct1(t, z):
        piece = piece2(w2[slots[t // 2 % nta, z // 2 % ngz]], t % 2, z % 2)
        e2[t + 2, z + 2, pl.ds(0, full // 2, stride=2), :] = piece
        e2[t + 2, z + 2, pl.ds(1, full // 2, stride=2), :] = piece

    for t in range(-2, part_t + 2):
        for z in range(-2, part_z + 2):
            if max(-t, t - part_t + 1, 0) + max(-z, z - part_z + 1, 0) <= 3:
                correct1(t, z)
    finish(wide_copies)
    for t, z, count in area1(2, 2, 1, 1):
        write1(v1w, t, z, read1(v1h, t, z, count) + e2[t // 2 + 2, pl.ds(z + 2, count)])
    sweep1(v1w, v1x, (1, 1, 1), (2, 2, 1, 1))
    sweep1(v1x, e1, (1, 1), (1, 1, 1))

    under = lax.rem(gy + ngy - 1, ngy)
    over = lax.rem(gy + 1, ngy)

    def split1(slab):
        even = jnp.where(odd_lane(slab), rolled(slab, 1, 2), slab)
        odd = jnp.where(odd_lane(slab), slab, rolled(slab, -1, 2))
        return jnp.stack([even, odd], axis=1).reshape(2 * slab.shape[0], *slab.shape[1:])

    def corrected0(level):
        fine = split1(e1[PAD_T + level, pl.ds(PAD_Z - 1, pairs1 + 2), gy])[1:-1]
        fine = refined_z(doubled(fine, level % 4))
        beyond = [
            refined_z(split1(e1[PAD_T + level, pl.ds(PAD_Z - 1, pairs1 + 2), side, pl.ds(row, 1)])[1:-1])
            for side, row in ((under, rows1 - 1), (over, 0))
        ]
        for t in (2 * level, 2 * level + 1):
            reach = 2 - max(-t, t - size_t + 1, 0)
            out = pl.ds(PAD0 - reach, size_z + 2 * reach)
            v0w[PAD0 + t, out] = v0b[PAD0 + t, out] + fine[2 - reach:size_z + 2 + reach]
            reach -= 1
            if reach < 0:
                continue
            out = pl.ds(1 - reach, size_z + 2 * reach)
            for side in range(2):
                shifted = beyond[side][2 - reach:size_z + 2 + reach]
                y0[2, side, 1 + t, out] = y0[1, side, 1 + t, out] + shifted
                if reach == 1:
                    y2[1, side, t] = y2[0, side, t] + beyond[side][2:size_z + 2]

    finish(behind_copies)
    for level in range(-1, size_t1 + 1):
        corrected0(level)
    for t in range(-1, size_t + 1):
        reach = 1 if 0 <= t < size_t else 0
        out = pl.ds(PAD0 - reach, size_z + 2 * reach)
        slab, summed = sum0(v0w, y0.at[2], t, reach)
        v0x[PAD0 + t, out] = KEEP * slab + v0a[PAD0 + t, out] + g0[PAD0 + t, out] * summed
    for t in range(size_t):
        for side, row in ((0, 0), (1, rows - 1)):
            at = lambda dt, dz: y0[2, side, 1 + t + dt, pl.ds(1 + dz, size_z)]
            slab = at(0, 0)
            summed = at(-1, 0) + at(1, 0) + at(0, -1) + at(0, 1)
            summed = summed + y2[1, side, t] + v0w[PAD0 + t, inner_z, pl.ds(row, 1)]
            summed = summed + rolled(slab, 1, 2) + rolled(slab, -1, 2)
            y0[3, side, 1 + t, own_z] = KEEP * slab + y0[0, side, 1 + t, own_z] + yg[side, t] * summed
    sweep0(v0x, y0.at[3], v0s, ys0.at[2], range(size_t), sol_ref)
    earlier = len(sent)
    sides, over_t = exchange(2, v0s)
    finish_sends(sent[:earlier])

    def residual(ts):
        for t in ts:
            slab, summed = sum0(v0s, y0.at[4], t)
            res_ref[t] = s_ref[t] + summed - (8.0 + m_ref[t]) * slab

    finish(sides)
    residual(inside)
    finish(over_t)
    residual(ends)
    finish_sends(sent[earlier:])


def place_in(values, axis):
    return lax.broadcasted_iota(jnp.int32, values.shape, axis)


def coarsened3(values):
    for step in (1, 2, 4):
        values = values + rolled(values, -step, 2)
    return (values + rolled(values, -1, 1)) * 0.0625


def refined3(values):
    corner = (place_in(values, 2) % 8 == 0) & (place_in(values, 1) % 2 == 0)
    values = jnp.where(corner, values, 0.0)
    values = values + rolled(values, 1, 1)
    for step in (1, 2, 4):
        values = values + rolled(values, step, 2)
    return values


def piece2(values, odd_t, odd_z):
    values = jnp.where(place_in(values, 1) % 4 == 2 * odd_t + odd_z, values, 0.0)
    values = values + rolled(values, -1 if odd_z else 1, 1)
    return values + rolled(values, -2 if odd_t else 2, 1)


def batches(cells, most):
    count = -(-len(cells) // most)
    size = -(-len(cells) // count)
    return [cells[at:at + size] for at in range(0, len(cells), size)]


def grown(cells, steps, count_t, count_z):
    for _ in range(steps):
        cells = cells | {
            ((t + dt) % count_t, (z + dz) % count_z)
            for t, z in cells for dt, dz in ((-1, 0), (1, 0), (0, -1), (0, 1))
        }
    return cells


def plan(nta, ngz):
    sites = lambda cells, steps: grown(cells, steps, 2 * nta, 2 * ngz)
    blocks = lambda cells: {(t // 2, z // 2) for t, z in cells}
    inner = lambda cells: {(2 * t + a, 2 * z + b) for t, z in cells for a in (0, 1) for b in (0, 1)}
    box = {(t % (2 * nta), z % (2 * ngz)) for t in range(-2, 4) for z in range(-2, 4)}
    last = sites(inner({(0, 0)}), 3) & box
    first, base = sites(last, 1), sites(last, 2)
    coarse = [grown(blocks(base), steps, nta, ngz) for steps in range(4)]
    swept = sites(inner(coarse[3]), 1) | base
    ordered = lambda cells: sorted(cells, key=lambda c: ((c[0] + nta // 2) % nta, (c[1] + ngz // 2) % ngz))
    return {
        "last": ordered(blocks(last)), "first": ordered(blocks(first)), "base": ordered(blocks(base)),
        "coarse": [ordered(cells) for cells in coarse], "swept": ordered(blocks(swept)),
        "source": ordered(blocks(sites(swept, 1))),
    }


def per_device(sizes, right_side, mass_field):
    nta, ngz, ngy = sizes
    size_t, size_z, rows, lanes = right_side.shape
    size_t1, pairs1, rows1 = size_t // 2, size_z // 4, rows // 2
    part_t, part_z, rows2 = size_t // 4, size_z // 4, rows // 4
    vmem = lambda *shape: pltpu.VMEM(shape, jnp.float32)
    dma = lambda *shape: pltpu.SemaphoreType.DMA(shape)
    padded0 = vmem(size_t + 2 * PAD0, size_z + 2 * PAD0, rows, lanes)
    faces = vmem(2, size_t, size_z, 1, lanes)
    padded1 = vmem(size_t1 + 2 * PAD_T, pairs1 + 2 * PAD_Z, ngy, rows1, lanes)
    window = len(plan(nta, ngz)["source"])
    packs = vmem(window, rows2 * ngy, lanes)
    packs3 = vmem(len(plan(nta, ngz)["coarse"][3]), rows2 * ngy, lanes)
    spreads = 8 * ngy + ngy - 1
    scratch = [
        *[padded0] * 6,
        vmem(5, 2, size_t + 2, size_z + 2, 1, lanes), vmem(3, 2, size_t, size_z, 1, lanes),
        vmem(2, 2, size_t, size_z, 1, lanes), faces, faces, faces,
        vmem(max(size_t1, part_t + 2), size_z, max(rows, ngy * rows1), lanes),
        *[padded1] * 9, vmem(part_t + 4, part_z + 4, ngy * rows1, lanes),
        *[packs] * 5, *[packs3] * 4,
        dma(3, 6), dma(3, 6), dma(24), dma(24), dma(2, spreads), dma(2, spreads), dma(12), dma(12),
        dma(2, window), dma(2, window),
        vmem(size_t, size_z, rows, lanes), vmem(size_t, size_z, rows, lanes), dma(2, size_t),
    ]
    block = jax.ShapeDtypeStruct(right_side.shape, jnp.float32)
    return pl.pallas_call(
        functools.partial(kernel, sizes),
        out_shape=(block, block),
        in_specs=[pl.BlockSpec(memory_space=pltpu.HBM)] * 2,
        out_specs=(pl.BlockSpec(memory_space=pltpu.VMEM),) * 2,
        scratch_shapes=scratch,
        compiler_params=pltpu.CompilerParams(
            collective_id=0, has_side_effects=True, vmem_limit_bytes=48 * 1024 * 1024
        ),
    )(*[pltpu.with_memory_space_constraint(values, pltpu.HBM) for values in (right_side, mass_field)])


def solution(mesh):
    sizes = tuple(mesh.shape[axis] for axis in ("ta", "gz", "gy"))
    spec = P("ta", "gz", "gy", None)
    return jax.shard_map(
        functools.partial(per_device, sizes),
        mesh=mesh,
        in_specs=(spec, spec),
        out_specs=(spec, spec),
        check_vma=False,
    )
```

```python
import functools

import jax
import jax.numpy as jnp
from jax import lax
from jax.experimental import pallas as pl
from jax.experimental.pallas import tpu as pltpu
from jax.sharding import PartitionSpec as P

DAMPING = 0.7
KEEP = 1.0 - DAMPING
PAD0, PAD_T, PAD_Z = 2, 3, 2
MESH = pl.DeviceIdType.MESH


def rolled(values, shift, axis):
    return pltpu.roll(values, shift % values.shape[axis], axis)


def odd_lane(values):
    return lax.broadcasted_iota(jnp.int32, values.shape, values.ndim - 1) % 2 == 1


def pair_swap(values, step, axis):
    index = lax.broadcasted_iota(jnp.int32, values.shape, axis)
    return jnp.where((index // step) % 2 == 0, rolled(values, -step, axis), rolled(values, step, axis))


def z_pairs(summed):
    count, rows, lanes = summed.shape
    summed = summed.reshape(count // 2, 2, rows, lanes)
    return summed[:, 0] + summed[:, 1]


def refined_z(slab):
    return jnp.repeat(slab, 2, axis=0)


def kernel(sizes, s_hbm, m_hbm, sol_ref, res_ref, *scratch):
    nta, ngz, ngy = sizes
    (g0, v0a, v0b, v0w, v0x, v0s, y0, ys0, y2, ys2, yg, ysg, fold,
     s1, m1, g1, v1a, v1b, v1h, v1w, v1x, e1, e2,
     m2, s2, g2, u2, w2, m3, s3, u3, w3,
     s_ref, m_ref, tally, departed, arrived, loaded) = scratch
    size_t, size_z, rows, lanes = s_ref.shape
    size_t1, pairs1, rows1 = size_t // 2, size_z // 4, rows // 2
    part_t, part_z, rows2 = size_t // 4, size_z // 4, rows // 4
    stages = plan(nta, ngz)
    slots = {cell: number for number, cell in enumerate(stages["source"])}
    slots3 = {cell: number for number, cell in enumerate(stages["coarse"][3])}
    ta, gz, gy = lax.axis_index("ta"), lax.axis_index("gz"), lax.axis_index("gy")

    places = {}

    def place_of(axis, at, step, count):
        key = axis, step % count
        if key not in places:
            places[key] = at if key[1] == 0 else lax.rem(at + key[1], count)
        return places[key]

    def device(dt, dz, dy):
        return {
            "ta": place_of("ta", ta, dt, nta), "gz": place_of("gz", gz, dz, ngz), "gy": place_of("gy", gy, dy, ngy),
        }

    near = [(dt, dz, dy) for dt in (-1, 0, 1) for dz in (-1, 0, 1) for dy in range(ngy)]
    centred = lambda d, n: (d + n // 2) % n - n // 2
    across = sorted(
        (cell for cell in slots if cell != (0, 0)),
        key=lambda c: -(abs(centred(c[0], nta)) + 2 * abs(centred(c[1], ngz))),
    )
    half = size_t // 2
    loads = [
        [
            pltpu.make_async_copy(source.at[pl.ds(part * half, half)], target.at[pl.ds(part * half, half)], loaded.at[part, place])
            for place, (source, target) in enumerate(((m_hbm, m_ref), (s_hbm, s_ref)))
        ]
        for part in range(2)
    ]
    met = sorted({(dt % nta, dz % ngz, dy % ngy) for dt, dz, dy in near + [(-t, -z, 0) for t, z in across]} - {(0, 0, 0)})
    for load in loads[0] + loads[1]:
        load.start()
    barrier = pltpu.get_barrier_semaphore()
    for offset in met:
        pl.semaphore_signal(barrier, inc=1, device_id=device(*offset), device_id_type=MESH)

    rows_of, all_rows = {}, []

    def send(group, moves):
        for source, target, offset in moves:
            pltpu.make_async_remote_copy(
                src_ref=source, dst_ref=target, send_sem=departed, recv_sem=arrived.at[group],
                device_id=device(*offset), device_id_type=MESH,
            ).start()
            count = 1
            for extent in source.shape[:-1]:
                count *= extent
            rows_of[group] = rows_of.get(group, 0) + count
            all_rows.append(count)
        return group

    def whole(group, count):
        view = tally.at[pl.ds(0, count)]
        return pltpu.make_async_remote_copy(
            src_ref=view, dst_ref=view, send_sem=departed, recv_sem=arrived.at[group],
            device_id=device(1, 0, 0), device_id_type=MESH,
        )

    def finish(group):
        whole(group, rows_of[group]).wait_recv()

    inner_t, inner_z = pl.ds(PAD0, size_t), pl.ds(PAD0, size_z)

    def faces0(field, depth):
        one = lambda at: pl.ds(PAD0 + at, 1)
        return [
            (field.at[inner_t, one(size_z - depth)], field.at[inner_t, one(-depth)], (0, 1, 0)),
            (field.at[inner_t, one(depth - 1)], field.at[inner_t, one(size_z - 1 + depth)], (0, -1, 0)),
            (field.at[one(size_t - depth), inner_z], field.at[one(-depth), inner_z], (1, 0, 0)),
            (field.at[one(depth - 1), inner_z], field.at[one(size_t - 1 + depth), inner_z], (-1, 0, 0)),
        ]

    own_t, own_z = pl.ds(1, size_t), pl.ds(1, size_z)

    def exchange(number, field):
        faces, halos = ys0.at[number], y0.at[(0, 1, 4)[number]]
        moves = [
            (faces.at[1], halos.at[0, own_t, own_z], (0, 0, 1)), (faces.at[0], halos.at[1, own_t, own_z], (0, 0, -1)),
        ] + faces0(field, 1)
        return send(2 * number, moves[:4]), send(2 * number + 1, moves[4:])

    def weights_behind():
        moves = [(ysg.at[1], yg.at[0], (0, 0, 1)), (ysg.at[0], yg.at[1], (0, 0, -1))]
        return send(6, moves + faces0(g0, 1))

    def second_behind():
        one = lambda at: pl.ds(at, 1)
        moves = [(ys2.at[1], y2.at[0, 0], (0, 0, 1)), (ys2.at[0], y2.at[0, 1], (0, 0, -1))]
        for up_t in (1, 0):
            for up_z in (1, 0):
                moves.append((
                    v0b.at[one(PAD0 + (size_t - 1) * up_t), one(PAD0 + (size_z - 1) * up_z)],
                    v0b.at[one(PAD0 - 1 + (size_t + 1) * (1 - up_t)), one(PAD0 - 1 + (size_z + 1) * (1 - up_z))],
                    (2 * up_t - 1, 2 * up_z - 1, 0),
                ))
        for up_y in (1, 0):
            faces, halos = ys0.at[1, up_y], y0.at[1, 1 - up_y]
            for up in (1, 0):
                moves.append((
                    faces.at[one((size_t - 1) * up)], halos.at[one((size_t + 1) * (1 - up)), own_z],
                    (2 * up - 1, 0, 2 * up_y - 1),
                ))
                moves.append((
                    faces.at[:, one((size_z - 1) * up)], halos.at[own_t, one((size_z + 1) * (1 - up))],
                    (0, 2 * up - 1, 2 * up_y - 1),
                ))
        return send(7, moves + faces0(v0b, 2))

    def layers1(deep_t, deep_z, corner_t):
        own_t, own_z = pl.ds(PAD_T, size_t1), pl.ds(PAD_Z, pairs1)

        def span(pad, size, deep, up):
            return pl.ds(pad + (size - deep) * up, deep), pl.ds(pad + size - (size + deep) * up, deep)

        moves = []
        for up in (1, 0):
            for up_z in (1, 0):
                here_t, there_t = span(PAD_T, size_t1, corner_t, up)
                here_z, there_z = span(PAD_Z, pairs1, 1, up_z)
                moves.append((here_t, here_z, there_t, there_z, 2 * up - 1, 2 * up_z - 1))
        for up in (1, 0):
            here, there = span(PAD_T, size_t1, deep_t, up)
            moves.append((here, own_z, there, own_z, 2 * up - 1, 0))
            here, there = span(PAD_Z, pairs1, deep_z, up)
            moves.append((own_t, here, own_t, there, 0, 2 * up - 1))
        return moves

    def spread1(number, field):
        part = pl.ds(gy, 1)
        own = field.at[pl.ds(PAD_T, size_t1), pl.ds(PAD_Z, pairs1), part]
        moves = [(own, own, (0, 0, dy)) for dy in range(1, ngy)]
        for dy in reversed(range(ngy)):
            for here_t, here_z, there_t, there_z, dt, dz in layers1(2, 1, 2):
                moves.append((field.at[here_t, here_z, part], field.at[there_t, there_z, part], (dt, dz, dy)))
        return send(8 + number, moves)

    def widen1(field):
        moves = [
            (field.at[here_t, here_z], field.at[there_t, there_z], (dt, dz, 0))
            for here_t, here_z, there_t, there_z, dt, dz in layers1(3, 2, 3)
        ]
        one = lambda at: pl.ds(at, 1)
        for up in (1, 0):
            for up_z in (1, 0):
                moves.append((
                    field.at[one(PAD_T + (size_t1 - 1) * up), one(PAD_Z + 1 + (pairs1 - 3) * up_z)],
                    field.at[one(PAD_T - 1 + (size_t1 + 1) * (1 - up)), one(PAD_Z - 2 + (pairs1 + 3) * (1 - up_z))],
                    (2 * up - 1, 2 * up_z - 1, 0),
                ))
        return send(10, moves)

    def gather(number, field):
        own = field.at[slots[0, 0]]
        return send(11 + number, [
            (own, field.at[slots[cell]], (-cell[0], -cell[1], 0)) for cell in across
        ])

    def put(field, faces, t, slab):
        field[PAD0 + t, inner_z] = slab
        faces[0, t] = slab[:, :1]
        faces[1, t] = slab[:, rows - 1:]

    def sum0(field, halos, t, reach=0):
        count = size_z + 2 * reach
        at = lambda dt, dz: field[PAD0 + t + dt, pl.ds(PAD0 - reach + dz, count)]
        slab, out = at(0, 0), pl.ds(1 - reach, count)
        row = lax.broadcasted_iota(jnp.int32, slab.shape, 1)
        summed = at(-1, 0) + at(1, 0) + at(0, -1) + at(0, 1)
        summed = summed + jnp.where(row == 0, halos[0, 1 + t, out], rolled(slab, 1, 1))
        summed = summed + jnp.where(row == rows - 1, halos[1, 1 + t, out], rolled(slab, -1, 1))
        return slab, summed + rolled(slab, 1, 2) + rolled(slab, -1, 2)

    def folded(summed, place):
        count, high, _ = summed.shape
        view = fold.at[place, pl.ds(0, count)]
        view[...] = summed
        return view[:, pl.ds(0, high // 2, stride=2), :] + view[:, pl.ds(1, high // 2, stride=2), :]

    def to_level1(summed, place):
        summed = folded(z_pairs(summed), place)
        summed = summed.reshape(summed.shape[0] // 2, 2, *summed.shape[1:])
        even, odd = summed[:, 0], summed[:, 1]
        even, odd = even + rolled(even, -1, 2), odd + rolled(odd, 1, 2)
        return jnp.where(odd_lane(even), odd, even) * 0.0625

    def doubled(slab, place):
        count, high, _ = slab.shape
        view = fold.at[place, pl.ds(0, count)]
        view[:, pl.ds(0, high, stride=2), :] = slab
        view[:, pl.ds(1, high, stride=2), :] = slab
        return view[...]

    full = ngy * rows1

    def area1(*reaches):
        far = len(reaches) - 1
        for t in range(-far, size_t1 + far):
            reach = reaches[max(-t, t - size_t1 + 1, 0)]
            yield t, -reach, pairs1 + 2 * reach

    def read1(field, t, z, count):
        return field[PAD_T + t, pl.ds(PAD_Z + z, count)].reshape(count, full, lanes)

    def write1(field, t, z, slab):
        field[PAD_T + t, pl.ds(PAD_Z + z, slab.shape[0])] = slab.reshape(slab.shape[0], ngy, rows1, lanes)

    def sum1(field, t, z, count, held):
        slab = read1(field, t, z, count)
        summed = read1(field, t - 1, z, count) + read1(field, t + 1, z, count)
        if held[t][0] < z:
            before, after = read1(field, t, z - 1, count), read1(field, t, z + 1, count)
        else:
            before = jnp.concatenate([slab[:1], slab[:-1]], axis=0)
            after = jnp.concatenate([slab[1:], slab[-1:]], axis=0)
        summed = summed + jnp.where(odd_lane(slab), rolled(slab + after, 1, 2), rolled(slab + before, -1, 2))
        summed = summed + rolled(slab, 1, 1) + rolled(slab, -1, 1)
        return slab, summed + rolled(slab, 2, 2) + rolled(slab, -2, 2)

    def sweep1(field, out, area, held):
        held = {t: (z, count) for t, z, count in area1(*held)}
        for t, z, count in area1(*area):
            slab, summed = sum1(field, t, z, count, held)
            fresh = KEEP * slab + read1(g1, t, z, count) * (read1(s1, t, z, count) + 0.5 * summed)
            write1(out, t, z, fresh)

    def packed(out, slabs):
        parts = [slab[z] for slab in slabs for z in range(part_z)]
        lane = lax.broadcasted_iota(jnp.int32, parts[0].shape, 1)
        values = parts[0]
        for k in range(1, len(parts)):
            values = jnp.where(lane % 4 == k, parts[k], values)
        out[slots[0, 0]] = values

    inside = list(range(1, size_t - 1))
    ends = [0, size_t - 1]

    for part in range(2):
        for load in loads[part]:
            load.wait()
        for t in range(part * half, (part + 1) * half):
            weight = DAMPING / (8.0 + m_ref[t])
            put(g0, ysg, t, weight)
            put(v0a, ys0.at[0], t, weight * s_ref[t])

    pl.semaphore_wait(barrier, len(met))
    sides, over_t = exchange(0, v0a)
    for t in range(size_t1):
        m1[PAD_T + t, pl.ds(PAD_Z, pairs1), gy] = to_level1(m_ref[2 * t] + m_ref[2 * t + 1], t)
    mass_copies = spread1(0, m1)
    weight_copies = weights_behind()

    def sweep0(field, halos, out, faces, ts, also=None):
        for t in ts:
            slab, summed = sum0(field, halos, t)
            fresh = KEEP * slab + g0[PAD0 + t, inner_z] * (s_ref[t] + summed)
            put(out, faces, t, fresh)
            if also is not None:
                also[t] = fresh

    finish(sides)
    sweep0(v0a, y0.at[0], v0b, ys0.at[1], inside)
    finish(over_t)
    sweep0(v0a, y0.at[0], v0b, ys0.at[1], ends)
    for t in range(size_t):
        ys2[0, t] = v0b[PAD0 + t, inner_z, pl.ds(1, 1)]
        ys2[1, t] = v0b[PAD0 + t, inner_z, pl.ds(rows - 2, 1)]
    sides, over_t = exchange(1, v0b)
    finish(mass_copies)
    for a, b, count in area1(1, 1, 1):
        write1(g1, a, b, DAMPING / (4.0 + read1(m1, a, b, count)))

    def to_level2(slabs):
        out = []
        for t in range(part_t):
            summed = folded(slabs[2 * t] + slabs[2 * t + 1], t)
            summed = summed + pair_swap(summed, 1, 2)
            out.append((summed + pair_swap(summed, 2, 2)) * 0.0625)
        return out

    packed(m2, to_level2([read1(m1, t, 0, pairs1) for t in range(size_t1)]))
    mass_copies = gather(0, m2)

    def remainder0(ts):
        for t in ts:
            remainder = []
            for odd in range(2):
                slab, summed = sum0(v0b, y0.at[1], 2 * t + odd)
                remainder.append(s_ref[2 * t + odd] + summed - (8.0 + m_ref[2 * t + odd]) * slab)
            s1[PAD_T + t, pl.ds(PAD_Z, pairs1), gy] = to_level1(remainder[0] + remainder[1], t)

    finish(sides)
    remainder0(range(1, size_t1 - 1))
    finish(over_t)
    remainder0((0, size_t1 - 1))
    source_copies = spread1(1, s1)
    def take(field, places, cells):
        return jnp.stack([field[places[cell]] for cell in cells])

    def put3(field, cells, values):
        field[pl.ds(slots3[cells[0]], len(cells))] = values

    finish(source_copies)

    for a, b, count in area1(1, 1, 0):
        write1(v1a, a, b, read1(g1, a, b, count) * read1(s1, a, b, count))
    sweep1(v1a, v1b, (1, 0), (1, 1, 0))
    remainder = []
    held = {t: (z, count) for t, z, count in area1(1, 0)}
    for a, b, count in area1(0):
        slab, summed = sum1(v1b, a, b, count, held)
        write1(v1h, a, b, slab)
        remainder.append(
            read1(s1, a, b, count) + 0.5 * summed - (4.0 + read1(m1, a, b, count)) * slab
        )
    packed(s2, to_level2(remainder))
    source_copies = gather(1, s2)
    wide_copies = widen1(v1h)
    behind_copies = second_behind()
    finish(mass_copies)
    for cell in stages["source"]:
        g2[slots[cell]] = DAMPING / (2.0 + m2[slots[cell]])
    for cells in batches(stages["coarse"][3], 24):
        put3(m3, cells, DAMPING / (1.0 + coarsened3(take(m2, slots, cells))))
    finish(source_copies)

    def around2(cell):
        t, z = cell
        return [((t + dt) % nta, (z + dz) % ngz) for dt, dz in ((-1, 0), (1, 0), (0, -1), (0, 1))]

    def sum2(field, cell):
        slab = field[slots[cell]]
        before_t, after_t, before_z, after_z = [
            slab + field[slots[other]] if other in slots else slab for other in around2(cell)
        ]
        lane = place_in(slab, 1)
        summed = jnp.where(lane % 4 >= 2, rolled(after_t, 2, 1), rolled(before_t, -2, 1))
        summed = summed + jnp.where(lane % 2 == 1, rolled(after_z, 1, 1), rolled(before_z, -1, 1))
        summed = summed + rolled(slab, 1, 0) + rolled(slab, -1, 0)
        return slab, summed + rolled(slab, 4, 1) + rolled(slab, -4, 1)

    def sweep2(field, out, cells):
        for cell in cells:
            slab, summed = sum2(field, cell)
            at = slots[cell]
            out[at] = KEEP * slab + g2[at] * (s2[at] + 0.25 * summed)

    for cell in stages["source"]:
        at = slots[cell]
        u2[at] = g2[at] * s2[at]
        w2[at] = u2[at]
    sweep2(u2, w2, stages["swept"])
    for cell in stages["coarse"][3]:
        slab, summed = sum2(w2, cell)
        at = slots[cell]
        s3[slots3[cell]] = s2[at] + 0.25 * summed - (2.0 + m2[at]) * slab
    for cells in batches(stages["coarse"][3], 24):
        source = coarsened3(take(s3, slots3, cells))
        put3(s3, cells, source)
        put3(u3, cells, take(m3, slots3, cells) * source)
    old, new = u3, w3
    for steps in (2, 1, 0):
        for cells in batches(stages["coarse"][steps], 13):
            slab = take(old, slots3, cells)
            near3 = list(zip(*[around2(cell) for cell in cells]))
            summed = take(old, slots3, near3[0]) + take(old, slots3, near3[1])
            summed = summed + take(old, slots3, near3[2]) + take(old, slots3, near3[3])
            summed = summed + rolled(slab, 2, 1) + rolled(slab, -2, 1)
            summed = summed + rolled(slab, 8, 2) + rolled(slab, -8, 2)
            fresh = KEEP * slab + take(m3, slots3, cells) * (take(s3, slots3, cells) + 0.125 * summed)
            for number, cell in enumerate(cells):
                new[slots3[cell]] = fresh[number]
        old, new = new, old
    for cells in batches(stages["base"], 24):
        fine = refined3(take(old, slots3, cells))
        for number, cell in enumerate(cells):
            w2[slots[cell]] = w2[slots[cell]] + fine[number]
    for cell in stages["base"]:
        u2[slots[cell]] = w2[slots[cell]]
    sweep2(w2, u2, stages["first"])
    sweep2(u2, w2, stages["last"])

    def correct1(t, z):
        piece = piece2(w2[slots[t // 2 % nta, z // 2 % ngz]], t % 2, z % 2)
        e2[t + 2, z + 2, pl.ds(0, full // 2, stride=2), :] = piece
        e2[t + 2, z + 2, pl.ds(1, full // 2, stride=2), :] = piece

    for t in range(-2, part_t + 2):
        for z in range(-2, part_z + 2):
            if max(-t, t - part_t + 1, 0) + max(-z, z - part_z + 1, 0) <= 3:
                correct1(t, z)
    finish(wide_copies)
    for t, z, count in area1(2, 2, 1, 1):
        write1(v1w, t, z, read1(v1h, t, z, count) + e2[t // 2 + 2, pl.ds(z + 2, count)])
    sweep1(v1w, v1x, (1, 1, 1), (2, 2, 1, 1))
    sweep1(v1x, e1, (1, 1), (1, 1, 1))

    under = lax.rem(gy + ngy - 1, ngy)
    over = lax.rem(gy + 1, ngy)

    def split1(slab):
        even = jnp.where(odd_lane(slab), rolled(slab, 1, 2), slab)
        odd = jnp.where(odd_lane(slab), slab, rolled(slab, -1, 2))
        return jnp.stack([even, odd], axis=1).reshape(2 * slab.shape[0], *slab.shape[1:])

    def corrected0(level):
        fine = split1(e1[PAD_T + level, pl.ds(PAD_Z - 1, pairs1 + 2), gy])[1:-1]
        fine = refined_z(doubled(fine, level % 4))
        beyond = [
            refined_z(split1(e1[PAD_T + level, pl.ds(PAD_Z - 1, pairs1 + 2), side, pl.ds(row, 1)])[1:-1])
            for side, row in ((under, rows1 - 1), (over, 0))
        ]
        for t in (2 * level, 2 * level + 1):
            reach = 2 - max(-t, t - size_t + 1, 0)
            out = pl.ds(PAD0 - reach, size_z + 2 * reach)
            v0w[PAD0 + t, out] = v0b[PAD0 + t, out] + fine[2 - reach:size_z + 2 + reach]
            reach -= 1
            if reach < 0:
                continue
            out = pl.ds(1 - reach, size_z + 2 * reach)
            for side in range(2):
                shifted = beyond[side][2 - reach:size_z + 2 + reach]
                y0[2, side, 1 + t, out] = y0[1, side, 1 + t, out] + shifted
                if reach == 1:
                    y2[1, side, t] = y2[0, side, t] + beyond[side][2:size_z + 2]

    finish(weight_copies)
    finish(behind_copies)
    for level in range(-1, size_t1 + 1):
        corrected0(level)
    for t in range(-1, size_t + 1):
        reach = 1 if 0 <= t < size_t else 0
        out = pl.ds(PAD0 - reach, size_z + 2 * reach)
        slab, summed = sum0(v0w, y0.at[2], t, reach)
        v0x[PAD0 + t, out] = KEEP * slab + v0a[PAD0 + t, out] + g0[PAD0 + t, out] * summed
    for t in range(size_t):
        for side, row in ((0, 0), (1, rows - 1)):
            at = lambda dt, dz: y0[2, side, 1 + t + dt, pl.ds(1 + dz, size_z)]
            slab = at(0, 0)
            summed = at(-1, 0) + at(1, 0) + at(0, -1) + at(0, 1)
            summed = summed + y2[1, side, t] + v0w[PAD0 + t, inner_z, pl.ds(row, 1)]
            summed = summed + rolled(slab, 1, 2) + rolled(slab, -1, 2)
            y0[3, side, 1 + t, own_z] = KEEP * slab + y0[0, side, 1 + t, own_z] + yg[side, t] * summed
    sweep0(v0x, y0.at[3], v0s, ys0.at[2], range(size_t), sol_ref)
    sides, over_t = exchange(2, v0s)

    def residual(ts):
        for t in ts:
            slab, summed = sum0(v0s, y0.at[4], t)
            res_ref[t] = s_ref[t] + summed - (8.0 + m_ref[t]) * slab

    finish(sides)
    residual(inside)
    finish(over_t)
    residual(ends)
    whole(0, sum(all_rows)).wait_send()


def place_in(values, axis):
    return lax.broadcasted_iota(jnp.int32, values.shape, axis)


def coarsened3(values):
    for step in (1, 2, 4):
        values = values + rolled(values, -step, 2)
    return (values + rolled(values, -1, 1)) * 0.0625


def refined3(values):
    corner = (place_in(values, 2) % 8 == 0) & (place_in(values, 1) % 2 == 0)
    values = jnp.where(corner, values, 0.0)
    values = values + rolled(values, 1, 1)
    for step in (1, 2, 4):
        values = values + rolled(values, step, 2)
    return values


def piece2(values, odd_t, odd_z):
    values = jnp.where(place_in(values, 1) % 4 == 2 * odd_t + odd_z, values, 0.0)
    values = values + rolled(values, -1 if odd_z else 1, 1)
    return values + rolled(values, -2 if odd_t else 2, 1)


def batches(cells, most):
    count = -(-len(cells) // most)
    size = -(-len(cells) // count)
    return [cells[at:at + size] for at in range(0, len(cells), size)]


def grown(cells, steps, count_t, count_z):
    for _ in range(steps):
        cells = cells | {
            ((t + dt) % count_t, (z + dz) % count_z)
            for t, z in cells for dt, dz in ((-1, 0), (1, 0), (0, -1), (0, 1))
        }
    return cells


def plan(nta, ngz):
    sites = lambda cells, steps: grown(cells, steps, 2 * nta, 2 * ngz)
    blocks = lambda cells: {(t // 2, z // 2) for t, z in cells}
    inner = lambda cells: {(2 * t + a, 2 * z + b) for t, z in cells for a in (0, 1) for b in (0, 1)}
    box = {(t % (2 * nta), z % (2 * ngz)) for t in range(-2, 4) for z in range(-2, 4)}
    last = sites(inner({(0, 0)}), 3) & box
    first, base = sites(last, 1), sites(last, 2)
    coarse = [grown(blocks(base), steps, nta, ngz) for steps in range(4)]
    swept = sites(inner(coarse[3]), 1) | base
    ordered = lambda cells: sorted(cells, key=lambda c: ((c[0] + nta // 2) % nta, (c[1] + ngz // 2) % ngz))
    return {
        "last": ordered(blocks(last)), "first": ordered(blocks(first)), "base": ordered(blocks(base)),
        "coarse": [ordered(cells) for cells in coarse], "swept": ordered(blocks(swept)),
        "source": ordered(blocks(sites(swept, 1))),
    }


def per_device(sizes, right_side, mass_field):
    nta, ngz, ngy = sizes
    size_t, size_z, rows, lanes = right_side.shape
    size_t1, pairs1, rows1 = size_t // 2, size_z // 4, rows // 2
    part_t, part_z, rows2 = size_t // 4, size_z // 4, rows // 4
    vmem = lambda *shape: pltpu.VMEM(shape, jnp.float32)
    dma = lambda *shape: pltpu.SemaphoreType.DMA(shape)
    padded0 = vmem(size_t + 2 * PAD0, size_z + 2 * PAD0, rows, lanes)
    faces = vmem(2, size_t, size_z, 1, lanes)
    padded1 = vmem(size_t1 + 2 * PAD_T, pairs1 + 2 * PAD_Z, ngy, rows1, lanes)
    window = len(plan(nta, ngz)["source"])
    packs = vmem(window, rows2 * ngy, lanes)
    packs3 = vmem(len(plan(nta, ngz)["coarse"][3]), rows2 * ngy, lanes)
    scratch = [
        *[padded0] * 6,
        vmem(5, 2, size_t + 2, size_z + 2, 1, lanes), vmem(3, 2, size_t, size_z, 1, lanes),
        vmem(2, 2, size_t, size_z, 1, lanes), faces, faces, faces,
        vmem(max(size_t1, part_t + 2), size_z, max(rows, ngy * rows1), lanes),
        *[padded1] * 9, vmem(part_t + 4, part_z + 4, ngy * rows1, lanes),
        *[packs] * 5, *[packs3] * 4,
        vmem(size_t, size_z, rows, lanes), vmem(size_t, size_z, rows, lanes),
        vmem(8192, 1, lanes), pltpu.SemaphoreType.DMA, dma(13), dma(2, 2),
    ]
    block = jax.ShapeDtypeStruct(right_side.shape, jnp.float32)
    return pl.pallas_call(
        functools.partial(kernel, sizes),
        out_shape=(block, block),
        in_specs=[pl.BlockSpec(memory_space=pltpu.HBM)] * 2,
        out_specs=(pl.BlockSpec(memory_space=pltpu.VMEM),) * 2,
        scratch_shapes=scratch,
        compiler_params=pltpu.CompilerParams(
            collective_id=0, has_side_effects=True, vmem_limit_bytes=48 * 1024 * 1024
        ),
    )(*[pltpu.with_memory_space_constraint(values, pltpu.HBM) for values in (right_side, mass_field)])


def solution(mesh):
    sizes = tuple(mesh.shape[axis] for axis in ("ta", "gz", "gy"))
    spec = P("ta", "gz", "gy", None)
    return jax.shard_map(
        functools.partial(per_device, sizes),
        mesh=mesh,
        in_specs=(spec, spec),
        out_specs=(spec, spec),
        check_vma=False,
    )
```

```python
import functools

import jax
import jax.numpy as jnp
from jax import lax
from jax.experimental import pallas as pl
from jax.experimental.pallas import tpu as pltpu
from jax.sharding import PartitionSpec as P

DAMPING = 0.7
KEEP = 1.0 - DAMPING
PAD0, PAD_T, PAD_Z = 2, 3, 2
MESH = pl.DeviceIdType.MESH


def rolled(values, shift, axis):
    return pltpu.roll(values, shift % values.shape[axis], axis)


def odd_lane(values):
    return lax.broadcasted_iota(jnp.int32, values.shape, values.ndim - 1) % 2 == 1


def pair_swap(values, step, axis):
    index = lax.broadcasted_iota(jnp.int32, values.shape, axis)
    return jnp.where((index // step) % 2 == 0, rolled(values, -step, axis), rolled(values, step, axis))


def z_pairs(summed):
    count, rows, lanes = summed.shape
    summed = summed.reshape(count // 2, 2, rows, lanes)
    return summed[:, 0] + summed[:, 1]


def refined_z(slab):
    return jnp.repeat(slab, 2, axis=0)


def kernel(sizes, s_hbm, m_hbm, sol_ref, res_ref, *scratch):
    nta, ngz, ngy = sizes
    (g0, v0a, v0b, v0w, v0x, v0s, y0, ys0, y2, ys2, yg, ysg, fold,
     s1, m1, g1, v1a, v1b, v1h, v1w, v1x, e1, e2,
     m2, s2, g2, u2, w2, m3, s3, u3, w3,
     s_ref, m_ref, tally, departed, arrived, loaded) = scratch
    size_t, size_z, rows, lanes = s_ref.shape
    size_t1, pairs1, rows1 = size_t // 2, size_z // 4, rows // 2
    part_t, part_z, rows2 = size_t // 4, size_z // 4, rows // 4
    stages = plan(nta, ngz)
    slots = {cell: number for number, cell in enumerate(stages["source"])}
    slots3 = {cell: number for number, cell in enumerate(stages["coarse"][3])}
    ta, gz, gy = lax.axis_index("ta"), lax.axis_index("gz"), lax.axis_index("gy")

    places = {}

    def place_of(axis, at, step, count):
        key = axis, step % count
        if key not in places:
            places[key] = at if key[1] == 0 else lax.rem(at + key[1], count)
        return places[key]

    def device(dt, dz, dy):
        return {
            "ta": place_of("ta", ta, dt, nta), "gz": place_of("gz", gz, dz, ngz), "gy": place_of("gy", gy, dy, ngy),
        }

    near = [(dt, dz, dy) for dt in (-1, 0, 1) for dz in (-1, 0, 1) for dy in range(ngy)]
    centred = lambda d, n: (d + n // 2) % n - n // 2
    across = sorted(
        (cell for cell in slots if cell != (0, 0)),
        key=lambda c: -(abs(centred(c[0], nta)) + 2 * abs(centred(c[1], ngz))),
    )
    half = size_t // 2
    loads = [
        [
            pltpu.make_async_copy(source.at[pl.ds(part * half, half)], target.at[pl.ds(part * half, half)], loaded.at[part, place])
            for place, (source, target) in enumerate(((m_hbm, m_ref), (s_hbm, s_ref)))
        ]
        for part in range(2)
    ]
    met = {(dt % nta, dz % ngz, dy % ngy) for dt, dz, dy in near + [(-t, -z, 0) for t, z in across]} - {(0, 0, 0)}
    met = sorted(met, key=lambda d: (-abs(centred(d[0], nta)) - 2 * abs(centred(d[1], ngz)) - 2 * d[2], d))
    barrier = pltpu.get_barrier_semaphore()
    for offset in met:
        pl.semaphore_signal(barrier, inc=1, device_id=device(*offset), device_id_type=MESH)
    for load in loads[0] + loads[1]:
        load.start()

    rows_of, all_rows = {}, []

    def send(group, moves):
        for source, target, offset in moves:
            pltpu.make_async_remote_copy(
                src_ref=source, dst_ref=target, send_sem=departed, recv_sem=arrived.at[group],
                device_id=device(*offset), device_id_type=MESH,
            ).start()
            count = 1
            for extent in source.shape[:-1]:
                count *= extent
            rows_of[group] = rows_of.get(group, 0) + count
            all_rows.append(count)
        return group

    def whole(group, count):
        view = tally.at[pl.ds(0, count)]
        return pltpu.make_async_remote_copy(
            src_ref=view, dst_ref=view, send_sem=departed, recv_sem=arrived.at[group],
            device_id=device(1, 0, 0), device_id_type=MESH,
        )

    def finish(group):
        whole(group, rows_of[group]).wait_recv()

    inner_t, inner_z = pl.ds(PAD0, size_t), pl.ds(PAD0, size_z)

    def faces0(field, depth):
        one = lambda at: pl.ds(PAD0 + at, 1)
        return [
            (field.at[inner_t, one(size_z - depth)], field.at[inner_t, one(-depth)], (0, 1, 0)),
            (field.at[inner_t, one(depth - 1)], field.at[inner_t, one(size_z - 1 + depth)], (0, -1, 0)),
            (field.at[one(size_t - depth), inner_z], field.at[one(-depth), inner_z], (1, 0, 0)),
            (field.at[one(depth - 1), inner_z], field.at[one(size_t - 1 + depth), inner_z], (-1, 0, 0)),
        ]

    own_t, own_z = pl.ds(1, size_t), pl.ds(1, size_z)

    def exchange(number, field):
        faces, halos = ys0.at[number], y0.at[(0, 1, 4)[number]]
        moves = [
            (faces.at[1], halos.at[0, own_t, own_z], (0, 0, 1)), (faces.at[0], halos.at[1, own_t, own_z], (0, 0, -1)),
        ] + faces0(field, 1)
        return send(2 * number, moves[:4]), send(2 * number + 1, moves[4:])

    def weights_behind():
        moves = [(ysg.at[1], yg.at[0], (0, 0, 1)), (ysg.at[0], yg.at[1], (0, 0, -1))]
        return send(6, moves + faces0(g0, 1))

    def second_behind():
        one = lambda at: pl.ds(at, 1)
        moves = [(ys2.at[1], y2.at[0, 0], (0, 0, 1)), (ys2.at[0], y2.at[0, 1], (0, 0, -1))]
        for up_t in (1, 0):
            for up_z in (1, 0):
                moves.append((
                    v0b.at[one(PAD0 + (size_t - 1) * up_t), one(PAD0 + (size_z - 1) * up_z)],
                    v0b.at[one(PAD0 - 1 + (size_t + 1) * (1 - up_t)), one(PAD0 - 1 + (size_z + 1) * (1 - up_z))],
                    (2 * up_t - 1, 2 * up_z - 1, 0),
                ))
        for up_y in (1, 0):
            faces, halos = ys0.at[1, up_y], y0.at[1, 1 - up_y]
            for up in (1, 0):
                moves.append((
                    faces.at[one((size_t - 1) * up)], halos.at[one((size_t + 1) * (1 - up)), own_z],
                    (2 * up - 1, 0, 2 * up_y - 1),
                ))
                moves.append((
                    faces.at[:, one((size_z - 1) * up)], halos.at[own_t, one((size_z + 1) * (1 - up))],
                    (0, 2 * up - 1, 2 * up_y - 1),
                ))
        return send(7, moves + faces0(v0b, 2))

    def layers1(deep_t, deep_z, corner_t):
        own_t, own_z = pl.ds(PAD_T, size_t1), pl.ds(PAD_Z, pairs1)

        def span(pad, size, deep, up):
            return pl.ds(pad + (size - deep) * up, deep), pl.ds(pad + size - (size + deep) * up, deep)

        moves = []
        for up in (1, 0):
            for up_z in (1, 0):
                here_t, there_t = span(PAD_T, size_t1, corner_t, up)
                here_z, there_z = span(PAD_Z, pairs1, 1, up_z)
                moves.append((here_t, here_z, there_t, there_z, 2 * up - 1, 2 * up_z - 1))
        for up in (1, 0):
            here, there = span(PAD_T, size_t1, deep_t, up)
            moves.append((here, own_z, there, own_z, 2 * up - 1, 0))
            here, there = span(PAD_Z, pairs1, deep_z, up)
            moves.append((own_t, here, own_t, there, 0, 2 * up - 1))
        return moves

    def spread1(number, field):
        part = pl.ds(gy, 1)
        own = field.at[pl.ds(PAD_T, size_t1), pl.ds(PAD_Z, pairs1), part]
        moves = [(own, own, (0, 0, dy)) for dy in range(1, ngy)]
        for dy in reversed(range(ngy)):
            for here_t, here_z, there_t, there_z, dt, dz in layers1(2, 1, 2):
                moves.append((field.at[here_t, here_z, part], field.at[there_t, there_z, part], (dt, dz, dy)))
        return send(8 + number, moves)

    def widen1(field):
        moves = [
            (field.at[here_t, here_z], field.at[there_t, there_z], (dt, dz, 0))
            for here_t, here_z, there_t, there_z, dt, dz in layers1(3, 2, 3)
        ]
        one = lambda at: pl.ds(at, 1)
        for up in (1, 0):
            for up_z in (1, 0):
                moves.append((
                    field.at[one(PAD_T + (size_t1 - 1) * up), one(PAD_Z + 1 + (pairs1 - 3) * up_z)],
                    field.at[one(PAD_T - 1 + (size_t1 + 1) * (1 - up)), one(PAD_Z - 2 + (pairs1 + 3) * (1 - up_z))],
                    (2 * up - 1, 2 * up_z - 1, 0),
                ))
        return send(10, moves)

    def gather(number, field):
        own = field.at[slots[0, 0]]
        return send(11 + number, [
            (own, field.at[slots[cell]], (-cell[0], -cell[1], 0)) for cell in across
        ])

    def put(field, faces, t, slab):
        field[PAD0 + t, inner_z] = slab
        faces[0, t] = slab[:, :1]
        faces[1, t] = slab[:, rows - 1:]

    def sum0(field, halos, t, reach=0):
        count = size_z + 2 * reach
        at = lambda dt, dz: field[PAD0 + t + dt, pl.ds(PAD0 - reach + dz, count)]
        slab, out = at(0, 0), pl.ds(1 - reach, count)
        row = lax.broadcasted_iota(jnp.int32, slab.shape, 1)
        summed = at(-1, 0) + at(1, 0) + at(0, -1) + at(0, 1)
        summed = summed + jnp.where(row == 0, halos[0, 1 + t, out], rolled(slab, 1, 1))
        summed = summed + jnp.where(row == rows - 1, halos[1, 1 + t, out], rolled(slab, -1, 1))
        return slab, summed + rolled(slab, 1, 2) + rolled(slab, -1, 2)

    def folded(summed, place):
        count, high, _ = summed.shape
        view = fold.at[place, pl.ds(0, count)]
        view[...] = summed
        return view[:, pl.ds(0, high // 2, stride=2), :] + view[:, pl.ds(1, high // 2, stride=2), :]

    def to_level1(summed, place):
        summed = folded(z_pairs(summed), place)
        summed = summed.reshape(summed.shape[0] // 2, 2, *summed.shape[1:])
        even, odd = summed[:, 0], summed[:, 1]
        even, odd = even + rolled(even, -1, 2), odd + rolled(odd, 1, 2)
        return jnp.where(odd_lane(even), odd, even) * 0.0625

    def doubled(slab, place):
        count, high, _ = slab.shape
        view = fold.at[place, pl.ds(0, count)]
        view[:, pl.ds(0, high, stride=2), :] = slab
        view[:, pl.ds(1, high, stride=2), :] = slab
        return view[...]

    full = ngy * rows1

    def area1(*reaches):
        far = len(reaches) - 1
        for t in range(-far, size_t1 + far):
            reach = reaches[max(-t, t - size_t1 + 1, 0)]
            yield t, -reach, pairs1 + 2 * reach

    def read1(field, t, z, count):
        return field[PAD_T + t, pl.ds(PAD_Z + z, count)].reshape(count, full, lanes)

    def write1(field, t, z, slab):
        field[PAD_T + t, pl.ds(PAD_Z + z, slab.shape[0])] = slab.reshape(slab.shape[0], ngy, rows1, lanes)

    def sum1(field, t, z, count, held):
        slab = read1(field, t, z, count)
        summed = read1(field, t - 1, z, count) + read1(field, t + 1, z, count)
        if held[t][0] < z:
            before, after = read1(field, t, z - 1, count), read1(field, t, z + 1, count)
        else:
            before = jnp.concatenate([slab[:1], slab[:-1]], axis=0)
            after = jnp.concatenate([slab[1:], slab[-1:]], axis=0)
        summed = summed + jnp.where(odd_lane(slab), rolled(slab + after, 1, 2), rolled(slab + before, -1, 2))
        summed = summed + rolled(slab, 1, 1) + rolled(slab, -1, 1)
        return slab, summed + rolled(slab, 2, 2) + rolled(slab, -2, 2)

    def sweep1(field, out, area, held):
        held = {t: (z, count) for t, z, count in area1(*held)}
        for t, z, count in area1(*area):
            slab, summed = sum1(field, t, z, count, held)
            fresh = KEEP * slab + read1(g1, t, z, count) * (read1(s1, t, z, count) + 0.5 * summed)
            write1(out, t, z, fresh)

    def packed(out, slabs):
        parts = [slab[z] for slab in slabs for z in range(part_z)]
        lane = lax.broadcasted_iota(jnp.int32, parts[0].shape, 1)
        values = parts[0]
        for k in range(1, len(parts)):
            values = jnp.where(lane % 4 == k, parts[k], values)
        out[slots[0, 0]] = values

    inside = list(range(1, size_t - 1))
    ends = [0, size_t - 1]

    for part in range(2):
        for load in loads[part]:
            load.wait()
        for t in range(part * half, (part + 1) * half):
            weight = DAMPING / (8.0 + m_ref[t])
            put(g0, ysg, t, weight)
            put(v0a, ys0.at[0], t, weight * s_ref[t])

    pl.semaphore_wait(barrier, len(met))
    sides, over_t = exchange(0, v0a)
    for t in range(size_t1):
        m1[PAD_T + t, pl.ds(PAD_Z, pairs1), gy] = to_level1(m_ref[2 * t] + m_ref[2 * t + 1], t)
    mass_copies = spread1(0, m1)

    def sweep0(field, halos, out, faces, ts, also=None):
        for t in ts:
            slab, summed = sum0(field, halos, t)
            fresh = KEEP * slab + g0[PAD0 + t, inner_z] * (s_ref[t] + summed)
            put(out, faces, t, fresh)
            if also is not None:
                also[t] = fresh

    finish(sides)
    sweep0(v0a, y0.at[0], v0b, ys0.at[1], inside)
    finish(over_t)
    sweep0(v0a, y0.at[0], v0b, ys0.at[1], ends)
    for t in range(size_t):
        ys2[0, t] = v0b[PAD0 + t, inner_z, pl.ds(1, 1)]
        ys2[1, t] = v0b[PAD0 + t, inner_z, pl.ds(rows - 2, 1)]
    sides, over_t = exchange(1, v0b)
    finish(mass_copies)
    for a, b, count in area1(1, 1, 1):
        write1(g1, a, b, DAMPING / (4.0 + read1(m1, a, b, count)))

    def to_level2(slabs):
        out = []
        for t in range(part_t):
            summed = folded(slabs[2 * t] + slabs[2 * t + 1], t)
            summed = summed + pair_swap(summed, 1, 2)
            out.append((summed + pair_swap(summed, 2, 2)) * 0.0625)
        return out

    weight_copies = weights_behind()

    def remainder0(ts):
        for t in ts:
            remainder = []
            for odd in range(2):
                slab, summed = sum0(v0b, y0.at[1], 2 * t + odd)
                remainder.append(s_ref[2 * t + odd] + summed - (8.0 + m_ref[2 * t + odd]) * slab)
            s1[PAD_T + t, pl.ds(PAD_Z, pairs1), gy] = to_level1(remainder[0] + remainder[1], t)

    finish(sides)
    remainder0(range(1, size_t1 - 1))
    finish(over_t)
    remainder0((0, size_t1 - 1))
    source_copies = spread1(1, s1)
    packed(m2, to_level2([read1(m1, t, 0, pairs1) for t in range(size_t1)]))
    mass_copies = gather(0, m2)
    def take(field, places, cells):
        return jnp.stack([field[places[cell]] for cell in cells])

    def put3(field, cells, values):
        field[pl.ds(slots3[cells[0]], len(cells))] = values

    finish(source_copies)

    for a, b, count in area1(1, 1, 0):
        write1(v1a, a, b, read1(g1, a, b, count) * read1(s1, a, b, count))
    sweep1(v1a, v1b, (1, 0), (1, 1, 0))
    remainder = []
    held = {t: (z, count) for t, z, count in area1(1, 0)}
    for a, b, count in area1(0):
        slab, summed = sum1(v1b, a, b, count, held)
        write1(v1h, a, b, slab)
        remainder.append(
            read1(s1, a, b, count) + 0.5 * summed - (4.0 + read1(m1, a, b, count)) * slab
        )
    packed(s2, to_level2(remainder))
    source_copies = gather(1, s2)
    wide_copies = widen1(v1h)
    behind_copies = second_behind()
    finish(mass_copies)
    for cell in stages["source"]:
        g2[slots[cell]] = DAMPING / (2.0 + m2[slots[cell]])
    for cells in batches(stages["coarse"][3], 24):
        put3(m3, cells, DAMPING / (1.0 + coarsened3(take(m2, slots, cells))))
    finish(source_copies)

    def around2(cell):
        t, z = cell
        return [((t + dt) % nta, (z + dz) % ngz) for dt, dz in ((-1, 0), (1, 0), (0, -1), (0, 1))]

    def sum2(field, cell):
        slab = field[slots[cell]]
        before_t, after_t, before_z, after_z = [
            slab + field[slots[other]] if other in slots else slab for other in around2(cell)
        ]
        lane = place_in(slab, 1)
        summed = jnp.where(lane % 4 >= 2, rolled(after_t, 2, 1), rolled(before_t, -2, 1))
        summed = summed + jnp.where(lane % 2 == 1, rolled(after_z, 1, 1), rolled(before_z, -1, 1))
        summed = summed + rolled(slab, 1, 0) + rolled(slab, -1, 0)
        return slab, summed + rolled(slab, 4, 1) + rolled(slab, -4, 1)

    def sweep2(field, out, cells):
        for cell in cells:
            slab, summed = sum2(field, cell)
            at = slots[cell]
            out[at] = KEEP * slab + g2[at] * (s2[at] + 0.25 * summed)

    for cell in stages["source"]:
        at = slots[cell]
        u2[at] = g2[at] * s2[at]
        w2[at] = u2[at]
    sweep2(u2, w2, stages["swept"])
    for cell in stages["coarse"][3]:
        slab, summed = sum2(w2, cell)
        at = slots[cell]
        s3[slots3[cell]] = s2[at] + 0.25 * summed - (2.0 + m2[at]) * slab
    for cells in batches(stages["coarse"][3], 24):
        source = coarsened3(take(s3, slots3, cells))
        put3(s3, cells, source)
        put3(u3, cells, take(m3, slots3, cells) * source)
    old, new = u3, w3
    for steps in (2, 1, 0):
        for cells in batches(stages["coarse"][steps], 13):
            slab = take(old, slots3, cells)
            near3 = list(zip(*[around2(cell) for cell in cells]))
            summed = take(old, slots3, near3[0]) + take(old, slots3, near3[1])
            summed = summed + take(old, slots3, near3[2]) + take(old, slots3, near3[3])
            summed = summed + rolled(slab, 2, 1) + rolled(slab, -2, 1)
            summed = summed + rolled(slab, 8, 2) + rolled(slab, -8, 2)
            fresh = KEEP * slab + take(m3, slots3, cells) * (take(s3, slots3, cells) + 0.125 * summed)
            for number, cell in enumerate(cells):
                new[slots3[cell]] = fresh[number]
        old, new = new, old
    for cells in batches(stages["base"], 24):
        fine = refined3(take(old, slots3, cells))
        for number, cell in enumerate(cells):
            w2[slots[cell]] = w2[slots[cell]] + fine[number]
    for cell in stages["base"]:
        u2[slots[cell]] = w2[slots[cell]]
    sweep2(w2, u2, stages["first"])
    sweep2(u2, w2, stages["last"])

    def correct1(t, z):
        piece = piece2(w2[slots[t // 2 % nta, z // 2 % ngz]], t % 2, z % 2)
        e2[t + 2, z + 2, pl.ds(0, full // 2, stride=2), :] = piece
        e2[t + 2, z + 2, pl.ds(1, full // 2, stride=2), :] = piece

    for t in range(-2, part_t + 2):
        for z in range(-2, part_z + 2):
            if max(-t, t - part_t + 1, 0) + max(-z, z - part_z + 1, 0) <= 3:
                correct1(t, z)
    finish(wide_copies)
    for t, z, count in area1(2, 2, 1, 1):
        write1(v1w, t, z, read1(v1h, t, z, count) + e2[t // 2 + 2, pl.ds(z + 2, count)])
    sweep1(v1w, v1x, (1, 1, 1), (2, 2, 1, 1))
    sweep1(v1x, e1, (1, 1), (1, 1, 1))

    under = lax.rem(gy + ngy - 1, ngy)
    over = lax.rem(gy + 1, ngy)

    def split1(slab):
        even = jnp.where(odd_lane(slab), rolled(slab, 1, 2), slab)
        odd = jnp.where(odd_lane(slab), slab, rolled(slab, -1, 2))
        return jnp.stack([even, odd], axis=1).reshape(2 * slab.shape[0], *slab.shape[1:])

    def corrected0(level):
        fine = split1(e1[PAD_T + level, pl.ds(PAD_Z - 1, pairs1 + 2), gy])[1:-1]
        fine = refined_z(doubled(fine, level % 4))
        beyond = [
            refined_z(split1(e1[PAD_T + level, pl.ds(PAD_Z - 1, pairs1 + 2), side, pl.ds(row, 1)])[1:-1])
            for side, row in ((under, rows1 - 1), (over, 0))
        ]
        for t in (2 * level, 2 * level + 1):
            reach = 2 - max(-t, t - size_t + 1, 0)
            out = pl.ds(PAD0 - reach, size_z + 2 * reach)
            v0w[PAD0 + t, out] = v0b[PAD0 + t, out] + fine[2 - reach:size_z + 2 + reach]
            reach -= 1
            if reach < 0:
                continue
            out = pl.ds(1 - reach, size_z + 2 * reach)
            for side in range(2):
                shifted = beyond[side][2 - reach:size_z + 2 + reach]
                y0[2, side, 1 + t, out] = y0[1, side, 1 + t, out] + shifted
                if reach == 1:
                    y2[1, side, t] = y2[0, side, t] + beyond[side][2:size_z + 2]

    finish(weight_copies)
    finish(behind_copies)
    for level in range(-1, size_t1 + 1):
        corrected0(level)
    for t in range(-1, size_t + 1):
        reach = 1 if 0 <= t < size_t else 0
        out = pl.ds(PAD0 - reach, size_z + 2 * reach)
        slab, summed = sum0(v0w, y0.at[2], t, reach)
        v0x[PAD0 + t, out] = KEEP * slab + v0a[PAD0 + t, out] + g0[PAD0 + t, out] * summed
    for t in range(size_t):
        for side, row in ((0, 0), (1, rows - 1)):
            at = lambda dt, dz: y0[2, side, 1 + t + dt, pl.ds(1 + dz, size_z)]
            slab = at(0, 0)
            summed = at(-1, 0) + at(1, 0) + at(0, -1) + at(0, 1)
            summed = summed + y2[1, side, t] + v0w[PAD0 + t, inner_z, pl.ds(row, 1)]
            summed = summed + rolled(slab, 1, 2) + rolled(slab, -1, 2)
            y0[3, side, 1 + t, own_z] = KEEP * slab + y0[0, side, 1 + t, own_z] + yg[side, t] * summed
    sweep0(v0x, y0.at[3], v0s, ys0.at[2], range(size_t), sol_ref)
    sides, over_t = exchange(2, v0s)

    def residual(ts):
        for t in ts:
            slab, summed = sum0(v0s, y0.at[4], t)
            res_ref[t] = s_ref[t] + summed - (8.0 + m_ref[t]) * slab

    finish(sides)
    residual(inside)
    finish(over_t)
    residual(ends)
    whole(0, sum(all_rows)).wait_send()


def place_in(values, axis):
    return lax.broadcasted_iota(jnp.int32, values.shape, axis)


def coarsened3(values):
    for step in (1, 2, 4):
        values = values + rolled(values, -step, 2)
    return (values + rolled(values, -1, 1)) * 0.0625


def refined3(values):
    corner = (place_in(values, 2) % 8 == 0) & (place_in(values, 1) % 2 == 0)
    values = jnp.where(corner, values, 0.0)
    values = values + rolled(values, 1, 1)
    for step in (1, 2, 4):
        values = values + rolled(values, step, 2)
    return values


def piece2(values, odd_t, odd_z):
    values = jnp.where(place_in(values, 1) % 4 == 2 * odd_t + odd_z, values, 0.0)
    values = values + rolled(values, -1 if odd_z else 1, 1)
    return values + rolled(values, -2 if odd_t else 2, 1)


def batches(cells, most):
    count = -(-len(cells) // most)
    size = -(-len(cells) // count)
    return [cells[at:at + size] for at in range(0, len(cells), size)]


def grown(cells, steps, count_t, count_z):
    for _ in range(steps):
        cells = cells | {
            ((t + dt) % count_t, (z + dz) % count_z)
            for t, z in cells for dt, dz in ((-1, 0), (1, 0), (0, -1), (0, 1))
        }
    return cells


def plan(nta, ngz):
    sites = lambda cells, steps: grown(cells, steps, 2 * nta, 2 * ngz)
    blocks = lambda cells: {(t // 2, z // 2) for t, z in cells}
    inner = lambda cells: {(2 * t + a, 2 * z + b) for t, z in cells for a in (0, 1) for b in (0, 1)}
    box = {(t % (2 * nta), z % (2 * ngz)) for t in range(-2, 4) for z in range(-2, 4)}
    last = sites(inner({(0, 0)}), 3) & box
    first, base = sites(last, 1), sites(last, 2)
    coarse = [grown(blocks(base), steps, nta, ngz) for steps in range(4)]
    swept = sites(inner(coarse[3]), 1) | base
    ordered = lambda cells: sorted(cells, key=lambda c: ((c[0] + nta // 2) % nta, (c[1] + ngz // 2) % ngz))
    return {
        "last": ordered(blocks(last)), "first": ordered(blocks(first)), "base": ordered(blocks(base)),
        "coarse": [ordered(cells) for cells in coarse], "swept": ordered(blocks(swept)),
        "source": ordered(blocks(sites(swept, 1))),
    }


def per_device(sizes, right_side, mass_field):
    nta, ngz, ngy = sizes
    size_t, size_z, rows, lanes = right_side.shape
    size_t1, pairs1, rows1 = size_t // 2, size_z // 4, rows // 2
    part_t, part_z, rows2 = size_t // 4, size_z // 4, rows // 4
    vmem = lambda *shape: pltpu.VMEM(shape, jnp.float32)
    dma = lambda *shape: pltpu.SemaphoreType.DMA(shape)
    padded0 = vmem(size_t + 2 * PAD0, size_z + 2 * PAD0, rows, lanes)
    faces = vmem(2, size_t, size_z, 1, lanes)
    padded1 = vmem(size_t1 + 2 * PAD_T, pairs1 + 2 * PAD_Z, ngy, rows1, lanes)
    window = len(plan(nta, ngz)["source"])
    packs = vmem(window, rows2 * ngy, lanes)
    packs3 = vmem(len(plan(nta, ngz)["coarse"][3]), rows2 * ngy, lanes)
    scratch = [
        *[padded0] * 6,
        vmem(5, 2, size_t + 2, size_z + 2, 1, lanes), vmem(3, 2, size_t, size_z, 1, lanes),
        vmem(2, 2, size_t, size_z, 1, lanes), faces, faces, faces,
        vmem(max(size_t1, part_t + 2), size_z, max(rows, ngy * rows1), lanes),
        *[padded1] * 9, vmem(part_t + 4, part_z + 4, ngy * rows1, lanes),
        *[packs] * 5, *[packs3] * 4,
        vmem(size_t, size_z, rows, lanes), vmem(size_t, size_z, rows, lanes),
        vmem(8192, 1, lanes), pltpu.SemaphoreType.DMA, dma(13), dma(2, 2),
    ]
    block = jax.ShapeDtypeStruct(right_side.shape, jnp.float32)
    return pl.pallas_call(
        functools.partial(kernel, sizes),
        out_shape=(block, block),
        in_specs=[pl.BlockSpec(memory_space=pltpu.HBM)] * 2,
        out_specs=(pl.BlockSpec(memory_space=pltpu.VMEM),) * 2,
        scratch_shapes=scratch,
        compiler_params=pltpu.CompilerParams(
            collective_id=0, has_side_effects=True, vmem_limit_bytes=48 * 1024 * 1024
        ),
    )(*[pltpu.with_memory_space_constraint(values, pltpu.HBM) for values in (right_side, mass_field)])


def solution(mesh):
    sizes = tuple(mesh.shape[axis] for axis in ("ta", "gz", "gy"))
    spec = P("ta", "gz", "gy", None)
    return jax.shard_map(
        functools.partial(per_device, sizes),
        mesh=mesh,
        in_specs=(spec, spec),
        out_specs=(spec, spec),
        check_vma=False,
    )
```

```python
import functools

import jax
import jax.numpy as jnp
from jax import lax
from jax.experimental import pallas as pl
from jax.experimental.pallas import tpu as pltpu
from jax.sharding import PartitionSpec as P

DAMPING = 0.7
KEEP = 1.0 - DAMPING
PAD0, PAD_T, PAD_Z = 2, 3, 2
MESH = pl.DeviceIdType.MESH


def rolled(values, shift, axis):
    return pltpu.roll(values, shift % values.shape[axis], axis)


def odd_lane(values):
    return lax.broadcasted_iota(jnp.int32, values.shape, values.ndim - 1) % 2 == 1


def pair_swap(values, step, axis):
    index = lax.broadcasted_iota(jnp.int32, values.shape, axis)
    return jnp.where((index // step) % 2 == 0, rolled(values, -step, axis), rolled(values, step, axis))


def z_pairs(summed):
    count, rows, lanes = summed.shape
    summed = summed.reshape(count // 2, 2, rows, lanes)
    return summed[:, 0] + summed[:, 1]


def refined_z(slab):
    return jnp.repeat(slab, 2, axis=0)


def neighbours0(field, low, high, t, start=0, count=None):
    count = count or field.shape[1] - 2 * PAD0
    at = lambda dt, dz: field[PAD0 + t + dt, pl.ds(PAD0 + start + dz, count)]
    slab = at(0, 0)
    row = lax.broadcasted_iota(jnp.int32, slab.shape, 1)
    summed = at(-1, 0) + at(1, 0) + at(0, -1) + at(0, 1)
    summed = summed + jnp.where(row == 0, low, rolled(slab, 1, 1))
    summed = summed + jnp.where(row == slab.shape[1] - 1, high, rolled(slab, -1, 1))
    return slab, summed + rolled(slab, 1, 2) + rolled(slab, -1, 2)


def last_kernel(v0s, yl, base, sol_hbm, res_hbm, res, written):
    size_t, size_z = base.shape[:2]
    copies = [pltpu.make_async_copy(v0s.at[pl.ds(PAD0, size_t), pl.ds(PAD0, size_z)], sol_hbm, written.at[0])]
    copies[0].start()
    for part in range(2):
        own = pl.ds(part * (size_t // 2), size_t // 2)
        for t in range(part * (size_t // 2), (part + 1) * (size_t // 2)):
            _, summed = neighbours0(v0s, yl[0, t], yl[1, t], t)
            res[t] = base[t] + summed
        copies.append(pltpu.make_async_copy(res.at[own], res_hbm.at[own], written.at[1 + part]))
        copies[-1].start()
    for copy in copies:
        copy.wait()


def kernel(sizes, s_hbm, m_hbm, v0s, yl, base, *scratch):
    nta, ngz, ngy = sizes
    (g0, v0a, v0b, v0w, v0x, y0, ys0, y2, ys2, yg, ysg, fold,
     s1, m1, g1, v1a, v1b, v1h, v1w, v1x, e1, e2,
     m2, s2, g2, u2, w2, m3, s3, u3, w3,
     s_ref, m_ref, tally, departed, arrived, loaded) = scratch
    size_t, size_z, rows, lanes = s_ref.shape
    size_t1, pairs1, rows1 = size_t // 2, size_z // 4, rows // 2
    part_t, part_z, rows2 = size_t // 4, size_z // 4, rows // 4
    stages = plan(nta, ngz)
    slots = {cell: number for number, cell in enumerate(stages["source"])}
    slots3 = {cell: number for number, cell in enumerate(stages["coarse"][3])}
    ta, gz, gy = lax.axis_index("ta"), lax.axis_index("gz"), lax.axis_index("gy")

    places = {}

    def place_of(axis, at, step, count):
        key = axis, step % count
        if key not in places:
            places[key] = at if key[1] == 0 else lax.rem(at + key[1], count)
        return places[key]

    def device(dt, dz, dy):
        return {
            "ta": place_of("ta", ta, dt, nta), "gz": place_of("gz", gz, dz, ngz), "gy": place_of("gy", gy, dy, ngy),
        }

    near = [(dt, dz, dy) for dt in (-1, 0, 1) for dz in (-1, 0, 1) for dy in range(ngy)]
    centred = lambda d, n: (d + n // 2) % n - n // 2
    across = sorted(
        (cell for cell in slots if cell != (0, 0)),
        key=lambda c: -(abs(centred(c[0], nta)) + 2 * abs(centred(c[1], ngz))),
    )
    half = size_t // 2
    loads = [
        [
            pltpu.make_async_copy(source.at[pl.ds(part * half, half)], target.at[pl.ds(part * half, half)], loaded.at[part, place])
            for place, (source, target) in enumerate(((m_hbm, m_ref), (s_hbm, s_ref)))
        ]
        for part in range(2)
    ]
    met = {(dt % nta, dz % ngz, dy % ngy) for dt, dz, dy in near + [(-t, -z, 0) for t, z in across]} - {(0, 0, 0)}
    met = sorted(met, key=lambda d: (-abs(centred(d[0], nta)) - 2 * abs(centred(d[1], ngz)) - 2 * d[2], d))
    barrier = pltpu.get_barrier_semaphore()
    for offset in met:
        pl.semaphore_signal(barrier, inc=1, device_id=device(*offset), device_id_type=MESH)
    for load in loads[0] + loads[1]:
        load.start()

    rows_of, all_rows = {}, []

    def send(group, moves):
        for source, target, offset in moves:
            pltpu.make_async_remote_copy(
                src_ref=source, dst_ref=target, send_sem=departed, recv_sem=arrived.at[group],
                device_id=device(*offset), device_id_type=MESH,
            ).start()
            count = 1
            for extent in source.shape[:-1]:
                count *= extent
            rows_of[group] = rows_of.get(group, 0) + count
            all_rows.append(count)
        return group

    def whole(group, count):
        view = tally.at[pl.ds(0, count)]
        return pltpu.make_async_remote_copy(
            src_ref=view, dst_ref=view, send_sem=departed, recv_sem=arrived.at[group],
            device_id=device(1, 0, 0), device_id_type=MESH,
        )

    def finish(group):
        whole(group, rows_of[group]).wait_recv()

    inner_t, inner_z = pl.ds(PAD0, size_t), pl.ds(PAD0, size_z)

    def faces0(field, depth):
        one = lambda at: pl.ds(PAD0 + at, 1)
        return [
            (field.at[inner_t, one(size_z - depth)], field.at[inner_t, one(-depth)], (0, 1, 0)),
            (field.at[inner_t, one(depth - 1)], field.at[inner_t, one(size_z - 1 + depth)], (0, -1, 0)),
            (field.at[one(size_t - depth), inner_z], field.at[one(-depth), inner_z], (1, 0, 0)),
            (field.at[one(depth - 1), inner_z], field.at[one(size_t - 1 + depth), inner_z], (-1, 0, 0)),
        ]

    own_t, own_z = pl.ds(1, size_t), pl.ds(1, size_z)

    def exchange(number, field):
        faces = ys0.at[number]
        low, high = [y0.at[number, side, own_t, own_z] if number < 2 else yl.at[side] for side in range(2)]
        moves = [(faces.at[1], low, (0, 0, 1)), (faces.at[0], high, (0, 0, -1))] + faces0(field, 1)
        return send(2 * number, moves[:4]), send(2 * number + 1, moves[4:])

    def weights_behind():
        moves = [(ysg.at[1], yg.at[0], (0, 0, 1)), (ysg.at[0], yg.at[1], (0, 0, -1))]
        return send(6, moves + faces0(g0, 1))

    def second_behind():
        one = lambda at: pl.ds(at, 1)
        moves = [(ys2.at[1], y2.at[0, 0], (0, 0, 1)), (ys2.at[0], y2.at[0, 1], (0, 0, -1))]
        for up_t in (1, 0):
            for up_z in (1, 0):
                moves.append((
                    v0b.at[one(PAD0 + (size_t - 1) * up_t), one(PAD0 + (size_z - 1) * up_z)],
                    v0b.at[one(PAD0 - 1 + (size_t + 1) * (1 - up_t)), one(PAD0 - 1 + (size_z + 1) * (1 - up_z))],
                    (2 * up_t - 1, 2 * up_z - 1, 0),
                ))
        for up_y in (1, 0):
            faces, halos = ys0.at[1, up_y], y0.at[1, 1 - up_y]
            for up in (1, 0):
                moves.append((
                    faces.at[one((size_t - 1) * up)], halos.at[one((size_t + 1) * (1 - up)), own_z],
                    (2 * up - 1, 0, 2 * up_y - 1),
                ))
                moves.append((
                    faces.at[:, one((size_z - 1) * up)], halos.at[own_t, one((size_z + 1) * (1 - up))],
                    (0, 2 * up - 1, 2 * up_y - 1),
                ))
        return send(7, moves + faces0(v0b, 2))

    def layers1(deep_t, deep_z, corner_t):
        own_t, own_z = pl.ds(PAD_T, size_t1), pl.ds(PAD_Z, pairs1)

        def span(pad, size, deep, up):
            return pl.ds(pad + (size - deep) * up, deep), pl.ds(pad + size - (size + deep) * up, deep)

        moves = []
        for up in (1, 0):
            for up_z in (1, 0):
                here_t, there_t = span(PAD_T, size_t1, corner_t, up)
                here_z, there_z = span(PAD_Z, pairs1, 1, up_z)
                moves.append((here_t, here_z, there_t, there_z, 2 * up - 1, 2 * up_z - 1))
        for up in (1, 0):
            here, there = span(PAD_T, size_t1, deep_t, up)
            moves.append((here, own_z, there, own_z, 2 * up - 1, 0))
            here, there = span(PAD_Z, pairs1, deep_z, up)
            moves.append((own_t, here, own_t, there, 0, 2 * up - 1))
        return moves

    def spread1(number, field):
        part = pl.ds(gy, 1)
        own = field.at[pl.ds(PAD_T, size_t1), pl.ds(PAD_Z, pairs1), part]
        moves = [(own, own, (0, 0, dy)) for dy in range(1, ngy)]
        for dy in reversed(range(ngy)):
            for here_t, here_z, there_t, there_z, dt, dz in layers1(2, 1, 2):
                moves.append((field.at[here_t, here_z, part], field.at[there_t, there_z, part], (dt, dz, dy)))
        return send(8 + number, moves)

    def widen1(field):
        moves = [
            (field.at[here_t, here_z], field.at[there_t, there_z], (dt, dz, 0))
            for here_t, here_z, there_t, there_z, dt, dz in layers1(3, 2, 3)
        ]
        one = lambda at: pl.ds(at, 1)
        for up in (1, 0):
            for up_z in (1, 0):
                moves.append((
                    field.at[one(PAD_T + (size_t1 - 1) * up), one(PAD_Z + 1 + (pairs1 - 3) * up_z)],
                    field.at[one(PAD_T - 1 + (size_t1 + 1) * (1 - up)), one(PAD_Z - 2 + (pairs1 + 3) * (1 - up_z))],
                    (2 * up - 1, 2 * up_z - 1, 0),
                ))
        return send(10, moves)

    def gather(number, field):
        own = field.at[slots[0, 0]]
        return send(11 + number, [
            (own, field.at[slots[cell]], (-cell[0], -cell[1], 0)) for cell in across
        ])

    def put(field, faces, t, slab):
        field[PAD0 + t, inner_z] = slab
        faces[0, t] = slab[:, :1]
        faces[1, t] = slab[:, rows - 1:]

    def sum0(field, halos, t, reach=0):
        count = size_z + 2 * reach
        out = pl.ds(1 - reach, count)
        return neighbours0(field, halos[0, 1 + t, out], halos[1, 1 + t, out], t, -reach, count)

    def folded(summed, place):
        count, high, _ = summed.shape
        view = fold.at[place, pl.ds(0, count)]
        view[...] = summed
        return view[:, pl.ds(0, high // 2, stride=2), :] + view[:, pl.ds(1, high // 2, stride=2), :]

    def to_level1(summed, place):
        summed = folded(z_pairs(summed), place)
        summed = summed.reshape(summed.shape[0] // 2, 2, *summed.shape[1:])
        even, odd = summed[:, 0], summed[:, 1]
        even, odd = even + rolled(even, -1, 2), odd + rolled(odd, 1, 2)
        return jnp.where(odd_lane(even), odd, even) * 0.0625

    def doubled(slab, place):
        count, high, _ = slab.shape
        view = fold.at[place, pl.ds(0, count)]
        view[:, pl.ds(0, high, stride=2), :] = slab
        view[:, pl.ds(1, high, stride=2), :] = slab
        return view[...]

    full = ngy * rows1

    def area1(*reaches):
        far = len(reaches) - 1
        for t in range(-far, size_t1 + far):
            reach = reaches[max(-t, t - size_t1 + 1, 0)]
            yield t, -reach, pairs1 + 2 * reach

    def read1(field, t, z, count):
        return field[PAD_T + t, pl.ds(PAD_Z + z, count)].reshape(count, full, lanes)

    def write1(field, t, z, slab):
        field[PAD_T + t, pl.ds(PAD_Z + z, slab.shape[0])] = slab.reshape(slab.shape[0], ngy, rows1, lanes)

    def sum1(field, t, z, count, held):
        slab = read1(field, t, z, count)
        summed = read1(field, t - 1, z, count) + read1(field, t + 1, z, count)
        if held[t][0] < z:
            before, after = read1(field, t, z - 1, count), read1(field, t, z + 1, count)
        else:
            before = jnp.concatenate([slab[:1], slab[:-1]], axis=0)
            after = jnp.concatenate([slab[1:], slab[-1:]], axis=0)
        summed = summed + jnp.where(odd_lane(slab), rolled(slab + after, 1, 2), rolled(slab + before, -1, 2))
        summed = summed + rolled(slab, 1, 1) + rolled(slab, -1, 1)
        return slab, summed + rolled(slab, 2, 2) + rolled(slab, -2, 2)

    def sweep1(field, out, area, held):
        held = {t: (z, count) for t, z, count in area1(*held)}
        for t, z, count in area1(*area):
            slab, summed = sum1(field, t, z, count, held)
            fresh = KEEP * slab + read1(g1, t, z, count) * (read1(s1, t, z, count) + 0.5 * summed)
            write1(out, t, z, fresh)

    def packed(out, slabs):
        parts = [slab[z] for slab in slabs for z in range(part_z)]
        lane = lax.broadcasted_iota(jnp.int32, parts[0].shape, 1)
        values = parts[0]
        for k in range(1, len(parts)):
            values = jnp.where(lane % 4 == k, parts[k], values)
        out[slots[0, 0]] = values

    inside = list(range(1, size_t - 1))
    ends = [0, size_t - 1]

    for part in range(2):
        for load in loads[part]:
            load.wait()
        for t in range(part * half, (part + 1) * half):
            weight = DAMPING / (8.0 + m_ref[t])
            put(g0, ysg, t, weight)
            put(v0a, ys0.at[0], t, weight * s_ref[t])

    pl.semaphore_wait(barrier, len(met))
    sides, over_t = exchange(0, v0a)
    for t in range(size_t1):
        m1[PAD_T + t, pl.ds(PAD_Z, pairs1), gy] = to_level1(m_ref[2 * t] + m_ref[2 * t + 1], t)
    mass_copies = spread1(0, m1)

    def sweep0(field, halos, out, faces, ts):
        for t in ts:
            slab, summed = sum0(field, halos, t)
            fresh = KEEP * slab + g0[PAD0 + t, inner_z] * (s_ref[t] + summed)
            put(out, faces, t, fresh)

    finish(sides)
    sweep0(v0a, y0.at[0], v0b, ys0.at[1], inside)
    finish(over_t)
    sweep0(v0a, y0.at[0], v0b, ys0.at[1], ends)
    for t in range(size_t):
        ys2[0, t] = v0b[PAD0 + t, inner_z, pl.ds(1, 1)]
        ys2[1, t] = v0b[PAD0 + t, inner_z, pl.ds(rows - 2, 1)]
    sides, over_t = exchange(1, v0b)
    finish(mass_copies)
    for a, b, count in area1(1, 1, 1):
        write1(g1, a, b, DAMPING / (4.0 + read1(m1, a, b, count)))

    def to_level2(slabs):
        out = []
        for t in range(part_t):
            summed = folded(slabs[2 * t] + slabs[2 * t + 1], t)
            summed = summed + pair_swap(summed, 1, 2)
            out.append((summed + pair_swap(summed, 2, 2)) * 0.0625)
        return out

    weight_copies = weights_behind()

    def remainder0(ts):
        for t in ts:
            remainder = []
            for odd in range(2):
                slab, summed = sum0(v0b, y0.at[1], 2 * t + odd)
                remainder.append(s_ref[2 * t + odd] + summed - (8.0 + m_ref[2 * t + odd]) * slab)
            s1[PAD_T + t, pl.ds(PAD_Z, pairs1), gy] = to_level1(remainder[0] + remainder[1], t)

    finish(sides)
    remainder0(range(1, size_t1 - 1))
    finish(over_t)
    remainder0((0, size_t1 - 1))
    source_copies = spread1(1, s1)
    packed(m2, to_level2([read1(m1, t, 0, pairs1) for t in range(size_t1)]))
    mass_copies = gather(0, m2)
    def take(field, places, cells):
        return jnp.stack([field[places[cell]] for cell in cells])

    def put3(field, cells, values):
        field[pl.ds(slots3[cells[0]], len(cells))] = values

    finish(source_copies)

    for a, b, count in area1(1, 1, 0):
        write1(v1a, a, b, read1(g1, a, b, count) * read1(s1, a, b, count))
    sweep1(v1a, v1b, (1, 0), (1, 1, 0))
    remainder = []
    held = {t: (z, count) for t, z, count in area1(1, 0)}
    for a, b, count in area1(0):
        slab, summed = sum1(v1b, a, b, count, held)
        write1(v1h, a, b, slab)
        remainder.append(
            read1(s1, a, b, count) + 0.5 * summed - (4.0 + read1(m1, a, b, count)) * slab
        )
    packed(s2, to_level2(remainder))
    source_copies = gather(1, s2)
    wide_copies = widen1(v1h)
    behind_copies = second_behind()
    finish(mass_copies)
    for cell in stages["source"]:
        g2[slots[cell]] = DAMPING / (2.0 + m2[slots[cell]])
    for cells in batches(stages["coarse"][3], 24):
        put3(m3, cells, DAMPING / (1.0 + coarsened3(take(m2, slots, cells))))
    finish(source_copies)

    def around2(cell):
        t, z = cell
        return [((t + dt) % nta, (z + dz) % ngz) for dt, dz in ((-1, 0), (1, 0), (0, -1), (0, 1))]

    def sum2(field, cell):
        slab = field[slots[cell]]
        before_t, after_t, before_z, after_z = [
            slab + field[slots[other]] if other in slots else slab for other in around2(cell)
        ]
        lane = place_in(slab, 1)
        summed = jnp.where(lane % 4 >= 2, rolled(after_t, 2, 1), rolled(before_t, -2, 1))
        summed = summed + jnp.where(lane % 2 == 1, rolled(after_z, 1, 1), rolled(before_z, -1, 1))
        summed = summed + rolled(slab, 1, 0) + rolled(slab, -1, 0)
        return slab, summed + rolled(slab, 4, 1) + rolled(slab, -4, 1)

    def sweep2(field, out, cells):
        for cell in cells:
            slab, summed = sum2(field, cell)
            at = slots[cell]
            out[at] = KEEP * slab + g2[at] * (s2[at] + 0.25 * summed)

    for cell in stages["source"]:
        at = slots[cell]
        u2[at] = g2[at] * s2[at]
        w2[at] = u2[at]
    sweep2(u2, w2, stages["swept"])
    for cell in stages["coarse"][3]:
        slab, summed = sum2(w2, cell)
        at = slots[cell]
        s3[slots3[cell]] = s2[at] + 0.25 * summed - (2.0 + m2[at]) * slab
    for cells in batches(stages["coarse"][3], 24):
        source = coarsened3(take(s3, slots3, cells))
        put3(s3, cells, source)
        put3(u3, cells, take(m3, slots3, cells) * source)
    old, new = u3, w3
    for steps in (2, 1, 0):
        for cells in batches(stages["coarse"][steps], 13):
            slab = take(old, slots3, cells)
            near3 = list(zip(*[around2(cell) for cell in cells]))
            summed = take(old, slots3, near3[0]) + take(old, slots3, near3[1])
            summed = summed + take(old, slots3, near3[2]) + take(old, slots3, near3[3])
            summed = summed + rolled(slab, 2, 1) + rolled(slab, -2, 1)
            summed = summed + rolled(slab, 8, 2) + rolled(slab, -8, 2)
            fresh = KEEP * slab + take(m3, slots3, cells) * (take(s3, slots3, cells) + 0.125 * summed)
            for number, cell in enumerate(cells):
                new[slots3[cell]] = fresh[number]
        old, new = new, old
    for cells in batches(stages["base"], 24):
        fine = refined3(take(old, slots3, cells))
        for number, cell in enumerate(cells):
            w2[slots[cell]] = w2[slots[cell]] + fine[number]
    for cell in stages["base"]:
        u2[slots[cell]] = w2[slots[cell]]
    sweep2(w2, u2, stages["first"])
    sweep2(u2, w2, stages["last"])

    def correct1(t, z):
        piece = piece2(w2[slots[t // 2 % nta, z // 2 % ngz]], t % 2, z % 2)
        e2[t + 2, z + 2, pl.ds(0, full // 2, stride=2), :] = piece
        e2[t + 2, z + 2, pl.ds(1, full // 2, stride=2), :] = piece

    for t in range(-2, part_t + 2):
        for z in range(-2, part_z + 2):
            if max(-t, t - part_t + 1, 0) + max(-z, z - part_z + 1, 0) <= 3:
                correct1(t, z)
    finish(wide_copies)
    for t, z, count in area1(2, 2, 1, 1):
        write1(v1w, t, z, read1(v1h, t, z, count) + e2[t // 2 + 2, pl.ds(z + 2, count)])
    sweep1(v1w, v1x, (1, 1, 1), (2, 2, 1, 1))
    sweep1(v1x, e1, (1, 1), (1, 1, 1))

    under = lax.rem(gy + ngy - 1, ngy)
    over = lax.rem(gy + 1, ngy)

    def split1(slab):
        even = jnp.where(odd_lane(slab), rolled(slab, 1, 2), slab)
        odd = jnp.where(odd_lane(slab), slab, rolled(slab, -1, 2))
        return jnp.stack([even, odd], axis=1).reshape(2 * slab.shape[0], *slab.shape[1:])

    def corrected0(level):
        fine = split1(e1[PAD_T + level, pl.ds(PAD_Z - 1, pairs1 + 2), gy])[1:-1]
        fine = refined_z(doubled(fine, level % 4))
        beyond = [
            refined_z(split1(e1[PAD_T + level, pl.ds(PAD_Z - 1, pairs1 + 2), side, pl.ds(row, 1)])[1:-1])
            for side, row in ((under, rows1 - 1), (over, 0))
        ]
        for t in (2 * level, 2 * level + 1):
            reach = 2 - max(-t, t - size_t + 1, 0)
            out = pl.ds(PAD0 - reach, size_z + 2 * reach)
            v0w[PAD0 + t, out] = v0b[PAD0 + t, out] + fine[2 - reach:size_z + 2 + reach]
            reach -= 1
            if reach < 0:
                continue
            out = pl.ds(1 - reach, size_z + 2 * reach)
            for side in range(2):
                shifted = beyond[side][2 - reach:size_z + 2 + reach]
                y0[2, side, 1 + t, out] = y0[1, side, 1 + t, out] + shifted
                if reach == 1:
                    y2[1, side, t] = y2[0, side, t] + beyond[side][2:size_z + 2]

    finish(weight_copies)
    finish(behind_copies)
    for level in range(-1, size_t1 + 1):
        corrected0(level)
    for t in range(-1, size_t + 1):
        reach = 1 if 0 <= t < size_t else 0
        out = pl.ds(PAD0 - reach, size_z + 2 * reach)
        slab, summed = sum0(v0w, y0.at[2], t, reach)
        v0x[PAD0 + t, out] = KEEP * slab + v0a[PAD0 + t, out] + g0[PAD0 + t, out] * summed
    for t in range(size_t):
        for side, row in ((0, 0), (1, rows - 1)):
            at = lambda dt, dz: y0[2, side, 1 + t + dt, pl.ds(1 + dz, size_z)]
            slab = at(0, 0)
            summed = at(-1, 0) + at(1, 0) + at(0, -1) + at(0, 1)
            summed = summed + y2[1, side, t] + v0w[PAD0 + t, inner_z, pl.ds(row, 1)]
            summed = summed + rolled(slab, 1, 2) + rolled(slab, -1, 2)
            y0[3, side, 1 + t, own_z] = KEEP * slab + y0[0, side, 1 + t, own_z] + yg[side, t] * summed
    sweep0(v0x, y0.at[3], v0s, ys0.at[2], range(size_t))
    sides, over_t = exchange(2, v0s)

    for t in range(size_t):
        base[t] = s_ref[t] - (8.0 + m_ref[t]) * v0s[PAD0 + t, inner_z]
    finish(sides)
    finish(over_t)
    whole(0, sum(all_rows)).wait_send()


def place_in(values, axis):
    return lax.broadcasted_iota(jnp.int32, values.shape, axis)


def coarsened3(values):
    for step in (1, 2, 4):
        values = values + rolled(values, -step, 2)
    return (values + rolled(values, -1, 1)) * 0.0625


def refined3(values):
    corner = (place_in(values, 2) % 8 == 0) & (place_in(values, 1) % 2 == 0)
    values = jnp.where(corner, values, 0.0)
    values = values + rolled(values, 1, 1)
    for step in (1, 2, 4):
        values = values + rolled(values, step, 2)
    return values


def piece2(values, odd_t, odd_z):
    values = jnp.where(place_in(values, 1) % 4 == 2 * odd_t + odd_z, values, 0.0)
    values = values + rolled(values, -1 if odd_z else 1, 1)
    return values + rolled(values, -2 if odd_t else 2, 1)


def batches(cells, most):
    count = -(-len(cells) // most)
    size = -(-len(cells) // count)
    return [cells[at:at + size] for at in range(0, len(cells), size)]


def grown(cells, steps, count_t, count_z):
    for _ in range(steps):
        cells = cells | {
            ((t + dt) % count_t, (z + dz) % count_z)
            for t, z in cells for dt, dz in ((-1, 0), (1, 0), (0, -1), (0, 1))
        }
    return cells


def plan(nta, ngz):
    sites = lambda cells, steps: grown(cells, steps, 2 * nta, 2 * ngz)
    blocks = lambda cells: {(t // 2, z // 2) for t, z in cells}
    inner = lambda cells: {(2 * t + a, 2 * z + b) for t, z in cells for a in (0, 1) for b in (0, 1)}
    box = {(t % (2 * nta), z % (2 * ngz)) for t in range(-2, 4) for z in range(-2, 4)}
    last = sites(inner({(0, 0)}), 3) & box
    first, base = sites(last, 1), sites(last, 2)
    coarse = [grown(blocks(base), steps, nta, ngz) for steps in range(4)]
    swept = sites(inner(coarse[3]), 1) | base
    ordered = lambda cells: sorted(cells, key=lambda c: ((c[0] + nta // 2) % nta, (c[1] + ngz // 2) % ngz))
    return {
        "last": ordered(blocks(last)), "first": ordered(blocks(first)), "base": ordered(blocks(base)),
        "coarse": [ordered(cells) for cells in coarse], "swept": ordered(blocks(swept)),
        "source": ordered(blocks(sites(swept, 1))),
    }


def per_device(sizes, right_side, mass_field):
    nta, ngz, ngy = sizes
    size_t, size_z, rows, lanes = right_side.shape
    size_t1, pairs1, rows1 = size_t // 2, size_z // 4, rows // 2
    part_t, part_z, rows2 = size_t // 4, size_z // 4, rows // 4
    vmem = lambda *shape: pltpu.VMEM(shape, jnp.float32)
    dma = lambda *shape: pltpu.SemaphoreType.DMA(shape)
    padded0 = vmem(size_t + 2 * PAD0, size_z + 2 * PAD0, rows, lanes)
    faces = vmem(2, size_t, size_z, 1, lanes)
    padded1 = vmem(size_t1 + 2 * PAD_T, pairs1 + 2 * PAD_Z, ngy, rows1, lanes)
    window = len(plan(nta, ngz)["source"])
    packs = vmem(window, rows2 * ngy, lanes)
    packs3 = vmem(len(plan(nta, ngz)["coarse"][3]), rows2 * ngy, lanes)
    scratch = [
        *[padded0] * 5,
        vmem(4, 2, size_t + 2, size_z + 2, 1, lanes), vmem(3, 2, size_t, size_z, 1, lanes),
        vmem(2, 2, size_t, size_z, 1, lanes), faces, faces, faces,
        vmem(max(size_t1, part_t + 2), size_z, max(rows, ngy * rows1), lanes),
        *[padded1] * 9, vmem(part_t + 4, part_z + 4, ngy * rows1, lanes),
        *[packs] * 5, *[packs3] * 4,
        vmem(size_t, size_z, rows, lanes), vmem(size_t, size_z, rows, lanes),
        vmem(8192, 1, lanes), pltpu.SemaphoreType.DMA, dma(13), dma(2, 2),
    ]
    array = lambda *shape: jax.ShapeDtypeStruct(shape, jnp.float32)
    block, place = array(*right_side.shape), pl.BlockSpec(memory_space=pltpu.VMEM)
    kept = pl.pallas_call(
        functools.partial(kernel, sizes),
        out_shape=(
            array(size_t + 2 * PAD0, size_z + 2 * PAD0, rows, lanes), array(2, size_t, size_z, 1, lanes), block,
        ),
        in_specs=[pl.BlockSpec(memory_space=pltpu.HBM)] * 2,
        out_specs=(place,) * 3,
        scratch_shapes=scratch,
        compiler_params=pltpu.CompilerParams(
            collective_id=0, has_side_effects=True, vmem_limit_bytes=48 * 1024 * 1024
        ),
    )(*[pltpu.with_memory_space_constraint(values, pltpu.HBM) for values in (right_side, mass_field)])
    return pl.pallas_call(
        last_kernel,
        out_shape=(block, block),
        in_specs=[place] * 3,
        out_specs=(pl.BlockSpec(memory_space=pltpu.HBM),) * 2,
        scratch_shapes=[vmem(size_t, size_z, rows, lanes), dma(3)],
        compiler_params=pltpu.CompilerParams(vmem_limit_bytes=8 * 1024 * 1024),
    )(*kept)


def solution(mesh):
    sizes = tuple(mesh.shape[axis] for axis in ("ta", "gz", "gy"))
    spec = P("ta", "gz", "gy", None)
    return jax.shard_map(
        functools.partial(per_device, sizes),
        mesh=mesh,
        in_specs=(spec, spec),
        out_specs=(spec, spec),
        check_vma=False,
    )
```

```python
import functools

import jax
import jax.numpy as jnp
from jax import lax
from jax.experimental import pallas as pl
from jax.experimental.pallas import tpu as pltpu
from jax.sharding import PartitionSpec as P

DAMPING = 0.7
KEEP = 1.0 - DAMPING
PAD0, PAD_T, PAD_Z = 2, 3, 2
MESH = pl.DeviceIdType.MESH


def rolled(values, shift, axis):
    return pltpu.roll(values, shift % values.shape[axis], axis)


def odd_lane(values):
    return lax.broadcasted_iota(jnp.int32, values.shape, values.ndim - 1) % 2 == 1


def pair_swap(values, step, axis):
    index = lax.broadcasted_iota(jnp.int32, values.shape, axis)
    return jnp.where((index // step) % 2 == 0, rolled(values, -step, axis), rolled(values, step, axis))


def z_pairs(summed):
    count, rows, lanes = summed.shape
    summed = summed.reshape(count // 2, 2, rows, lanes)
    return summed[:, 0] + summed[:, 1]


def refined_z(slab):
    return jnp.repeat(slab, 2, axis=0)


def neighbours0(field, low, high, t, start=0, count=None):
    count = count or field.shape[1] - 2 * PAD0
    at = lambda dt, dz: field[PAD0 + t + dt, pl.ds(PAD0 + start + dz, count)]
    slab = at(0, 0)
    row = lax.broadcasted_iota(jnp.int32, slab.shape, 1)
    summed = at(-1, 0) + at(1, 0) + at(0, -1) + at(0, 1)
    summed = summed + jnp.where(row == 0, low, rolled(slab, 1, 1))
    summed = summed + jnp.where(row == slab.shape[1] - 1, high, rolled(slab, -1, 1))
    return slab, summed + rolled(slab, 1, 2) + rolled(slab, -1, 2)


def last_kernel(v0s, yl, base, sol_hbm, res_hbm, res, written):
    size_t, size_z = base.shape[:2]
    copies = [pltpu.make_async_copy(v0s.at[pl.ds(PAD0, size_t), pl.ds(PAD0, size_z)], sol_hbm, written.at[0])]
    copies[0].start()
    for part in range(2):
        own = pl.ds(part * (size_t // 2), size_t // 2)
        for t in range(part * (size_t // 2), (part + 1) * (size_t // 2)):
            _, summed = neighbours0(v0s, yl[0, t], yl[1, t], t)
            res[t] = base[t] + summed
        copies.append(pltpu.make_async_copy(res.at[own], res_hbm.at[own], written.at[1 + part]))
        copies[-1].start()
    for copy in copies:
        copy.wait()


def kernel(sizes, s_hbm, m_hbm, v0s, yl, base, *scratch):
    nta, ngz, ngy = sizes
    (g0, v0a, v0b, v0w, v0x, y0, ys0, y2, ys2, yg, ysg, fold,
     s1, m1, g1, v1a, v1b, v1h, v1w, v1x, e1, e2,
     m2, s2, g2, u2, w2, m3, s3, u3, w3,
     s_ref, m_ref, tally, departed, arrived, loaded) = scratch
    size_t, size_z, rows, lanes = s_ref.shape
    size_t1, pairs1, rows1 = size_t // 2, size_z // 4, rows // 2
    part_t, part_z, rows2 = size_t // 4, size_z // 4, rows // 4
    stages = plan(nta, ngz)
    slots = {cell: number for number, cell in enumerate(stages["source"])}
    slots3 = {cell: number for number, cell in enumerate(stages["coarse"][3])}
    ta, gz, gy = lax.axis_index("ta"), lax.axis_index("gz"), lax.axis_index("gy")

    places = {}

    def place_of(axis, at, step, count):
        key = axis, step % count
        if key not in places:
            places[key] = at if key[1] == 0 else lax.rem(at + key[1], count)
        return places[key]

    def device(dt, dz, dy):
        return {
            "ta": place_of("ta", ta, dt, nta), "gz": place_of("gz", gz, dz, ngz), "gy": place_of("gy", gy, dy, ngy),
        }

    near = [(dt, dz, dy) for dt in (-1, 0, 1) for dz in (-1, 0, 1) for dy in range(ngy)]
    centred = lambda d, n: (d + n // 2) % n - n // 2
    across = sorted(
        (cell for cell in slots if cell != (0, 0)),
        key=lambda c: -(abs(centred(c[0], nta)) + 2 * abs(centred(c[1], ngz))),
    )
    half = size_t // 2
    loads = [
        [
            pltpu.make_async_copy(source.at[pl.ds(part * half, half)], target.at[pl.ds(part * half, half)], loaded.at[part, place])
            for place, (source, target) in enumerate(((m_hbm, m_ref), (s_hbm, s_ref)))
        ]
        for part in range(2)
    ]
    met = {(dt % nta, dz % ngz, dy % ngy) for dt, dz, dy in near + [(-t, -z, 0) for t, z in across]} - {(0, 0, 0)}
    met = sorted(met, key=lambda d: (-abs(centred(d[0], nta)) - 2 * abs(centred(d[1], ngz)) - 2 * d[2], d))
    barrier = pltpu.get_barrier_semaphore()
    for offset in met:
        pl.semaphore_signal(barrier, inc=1, device_id=device(*offset), device_id_type=MESH)
    for load in loads[0] + loads[1]:
        load.start()

    rows_of, all_rows = {}, []

    def send(group, moves):
        for source, target, offset in moves:
            pltpu.make_async_remote_copy(
                src_ref=source, dst_ref=target, send_sem=departed, recv_sem=arrived.at[group],
                device_id=offset if isinstance(offset, dict) else device(*offset), device_id_type=MESH,
            ).start()
            count = 1
            for extent in source.shape[:-1]:
                count *= extent
            rows_of[group] = rows_of.get(group, 0) + count
            all_rows.append(count)
        return group

    def whole(group, count):
        view = tally.at[pl.ds(0, count)]
        return pltpu.make_async_remote_copy(
            src_ref=view, dst_ref=view, send_sem=departed, recv_sem=arrived.at[group],
            device_id=device(1, 0, 0), device_id_type=MESH,
        )

    def finish(group):
        whole(group, rows_of[group]).wait_recv()

    inner_t, inner_z = pl.ds(PAD0, size_t), pl.ds(PAD0, size_z)

    def faces0(field, depth):
        one = lambda at: pl.ds(PAD0 + at, 1)
        return [
            (field.at[inner_t, one(size_z - depth)], field.at[inner_t, one(-depth)], (0, 1, 0)),
            (field.at[inner_t, one(depth - 1)], field.at[inner_t, one(size_z - 1 + depth)], (0, -1, 0)),
            (field.at[one(size_t - depth), inner_z], field.at[one(-depth), inner_z], (1, 0, 0)),
            (field.at[one(depth - 1), inner_z], field.at[one(size_t - 1 + depth), inner_z], (-1, 0, 0)),
        ]

    own_t, own_z = pl.ds(1, size_t), pl.ds(1, size_z)

    def exchange(number, field):
        faces = ys0.at[number]
        low, high = [y0.at[number, side, own_t, own_z] if number < 2 else yl.at[side] for side in range(2)]
        moves = [(faces.at[1], low, (0, 0, 1)), (faces.at[0], high, (0, 0, -1))] + faces0(field, 1)
        return send(2 * number, moves[:4]), send(2 * number + 1, moves[4:])

    def weights_behind():
        moves = [(ysg.at[1], yg.at[0], (0, 0, 1)), (ysg.at[0], yg.at[1], (0, 0, -1))]
        return send(6, moves + faces0(g0, 1))

    def second_behind():
        one = lambda at: pl.ds(at, 1)
        moves = [(ys2.at[1], y2.at[0, 0], (0, 0, 1)), (ys2.at[0], y2.at[0, 1], (0, 0, -1))]
        for up_t in (1, 0):
            for up_z in (1, 0):
                moves.append((
                    v0b.at[one(PAD0 + (size_t - 1) * up_t), one(PAD0 + (size_z - 1) * up_z)],
                    v0b.at[one(PAD0 - 1 + (size_t + 1) * (1 - up_t)), one(PAD0 - 1 + (size_z + 1) * (1 - up_z))],
                    (2 * up_t - 1, 2 * up_z - 1, 0),
                ))
        for up_y in (1, 0):
            faces, halos = ys0.at[1, up_y], y0.at[1, 1 - up_y]
            for up in (1, 0):
                moves.append((
                    faces.at[one((size_t - 1) * up)], halos.at[one((size_t + 1) * (1 - up)), own_z],
                    (2 * up - 1, 0, 2 * up_y - 1),
                ))
                moves.append((
                    faces.at[:, one((size_z - 1) * up)], halos.at[own_t, one((size_z + 1) * (1 - up))],
                    (0, 2 * up - 1, 2 * up_y - 1),
                ))
        return send(7, moves + faces0(v0b, 2))

    def layers1(deep_t, deep_z, corner_t):
        own_t, own_z = pl.ds(PAD_T, size_t1), pl.ds(PAD_Z, pairs1)

        def span(pad, size, deep, up):
            return pl.ds(pad + (size - deep) * up, deep), pl.ds(pad + size - (size + deep) * up, deep)

        moves = []
        for up in (1, 0):
            for up_z in (1, 0):
                here_t, there_t = span(PAD_T, size_t1, corner_t, up)
                here_z, there_z = span(PAD_Z, pairs1, 1, up_z)
                moves.append((here_t, here_z, there_t, there_z, 2 * up - 1, 2 * up_z - 1))
        for up in (1, 0):
            here, there = span(PAD_T, size_t1, deep_t, up)
            moves.append((here, own_z, there, own_z, 2 * up - 1, 0))
            here, there = span(PAD_Z, pairs1, deep_z, up)
            moves.append((own_t, here, own_t, there, 0, 2 * up - 1))
        return moves

    def spread1(number, field):
        part = pl.ds(gy, 1)
        own = field.at[pl.ds(PAD_T, size_t1), pl.ds(PAD_Z, pairs1), part]
        moves = [(own, own, (0, 0, dy)) for dy in range(1, ngy)]
        for dy in reversed(range(ngy)):
            for here_t, here_z, there_t, there_z, dt, dz in layers1(2, 1, 2):
                moves.append((field.at[here_t, here_z, part], field.at[there_t, there_z, part], (dt, dz, dy)))
        return send(8 + number, moves)

    def widen1(field):
        moves = [
            (field.at[here_t, here_z], field.at[there_t, there_z], (dt, dz, 0))
            for here_t, here_z, there_t, there_z, dt, dz in layers1(3, 2, 3)
        ]
        one = lambda at: pl.ds(at, 1)
        for up in (1, 0):
            for up_z in (1, 0):
                moves.append((
                    field.at[one(PAD_T + (size_t1 - 1) * up), one(PAD_Z + 1 + (pairs1 - 3) * up_z)],
                    field.at[one(PAD_T - 1 + (size_t1 + 1) * (1 - up)), one(PAD_Z - 2 + (pairs1 + 3) * (1 - up_z))],
                    (2 * up - 1, 2 * up_z - 1, 0),
                ))
        return send(10, moves)

    def gather(number, field, cells):
        own = field.at[slots[0, 0]]
        return send(11 + number, [(own, field.at[slots[cell]], (-cell[0], -cell[1], 0)) for cell in cells])

    core = lax.rem(ta, 2)
    even = [cell for cell in across if cell[0] % 2 == 0]

    def relay(field):
        sibling = {"ta": ta + 1 - 2 * core, "gz": gz, "gy": gy}
        count = len(slots) // ngz // 2
        return send(13, [
            (
                field.at[pl.ds((2 * number + 2 - 2 * core) * ngz, ngz)],
                field.at[pl.ds((2 * number + 1) * ngz, ngz)], sibling,
            )
            for number in range(count)
        ])

    def put(field, faces, t, slab):
        field[PAD0 + t, inner_z] = slab
        faces[0, t] = slab[:, :1]
        faces[1, t] = slab[:, rows - 1:]

    def sum0(field, halos, t, reach=0):
        count = size_z + 2 * reach
        out = pl.ds(1 - reach, count)
        return neighbours0(field, halos[0, 1 + t, out], halos[1, 1 + t, out], t, -reach, count)

    def folded(summed, place):
        count, high, _ = summed.shape
        view = fold.at[place, pl.ds(0, count)]
        view[...] = summed
        return view[:, pl.ds(0, high // 2, stride=2), :] + view[:, pl.ds(1, high // 2, stride=2), :]

    def to_level1(summed, place):
        summed = folded(z_pairs(summed), place)
        summed = summed.reshape(summed.shape[0] // 2, 2, *summed.shape[1:])
        even, odd = summed[:, 0], summed[:, 1]
        even, odd = even + rolled(even, -1, 2), odd + rolled(odd, 1, 2)
        return jnp.where(odd_lane(even), odd, even) * 0.0625

    def doubled(slab, place):
        count, high, _ = slab.shape
        view = fold.at[place, pl.ds(0, count)]
        view[:, pl.ds(0, high, stride=2), :] = slab
        view[:, pl.ds(1, high, stride=2), :] = slab
        return view[...]

    full = ngy * rows1

    def area1(*reaches):
        far = len(reaches) - 1
        for t in range(-far, size_t1 + far):
            reach = reaches[max(-t, t - size_t1 + 1, 0)]
            yield t, -reach, pairs1 + 2 * reach

    def read1(field, t, z, count):
        return field[PAD_T + t, pl.ds(PAD_Z + z, count)].reshape(count, full, lanes)

    def write1(field, t, z, slab):
        field[PAD_T + t, pl.ds(PAD_Z + z, slab.shape[0])] = slab.reshape(slab.shape[0], ngy, rows1, lanes)

    def sum1(field, t, z, count, held):
        slab = read1(field, t, z, count)
        summed = read1(field, t - 1, z, count) + read1(field, t + 1, z, count)
        if held[t][0] < z:
            before, after = read1(field, t, z - 1, count), read1(field, t, z + 1, count)
        else:
            before = jnp.concatenate([slab[:1], slab[:-1]], axis=0)
            after = jnp.concatenate([slab[1:], slab[-1:]], axis=0)
        summed = summed + jnp.where(odd_lane(slab), rolled(slab + after, 1, 2), rolled(slab + before, -1, 2))
        summed = summed + rolled(slab, 1, 1) + rolled(slab, -1, 1)
        return slab, summed + rolled(slab, 2, 2) + rolled(slab, -2, 2)

    def sweep1(field, out, area, held):
        held = {t: (z, count) for t, z, count in area1(*held)}
        for t, z, count in area1(*area):
            slab, summed = sum1(field, t, z, count, held)
            fresh = KEEP * slab + read1(g1, t, z, count) * (read1(s1, t, z, count) + 0.5 * summed)
            write1(out, t, z, fresh)

    def packed(out, slabs):
        parts = [slab[z] for slab in slabs for z in range(part_z)]
        lane = lax.broadcasted_iota(jnp.int32, parts[0].shape, 1)
        values = parts[0]
        for k in range(1, len(parts)):
            values = jnp.where(lane % 4 == k, parts[k], values)
        out[slots[0, 0]] = values

    inside = list(range(1, size_t - 1))
    ends = [0, size_t - 1]

    for part in range(2):
        for load in loads[part]:
            load.wait()
        for t in range(part * half, (part + 1) * half):
            weight = DAMPING / (8.0 + m_ref[t])
            put(g0, ysg, t, weight)
            put(v0a, ys0.at[0], t, weight * s_ref[t])

    pl.semaphore_wait(barrier, len(met))
    sides, over_t = exchange(0, v0a)
    for t in range(size_t1):
        m1[PAD_T + t, pl.ds(PAD_Z, pairs1), gy] = to_level1(m_ref[2 * t] + m_ref[2 * t + 1], t)
    mass_copies = spread1(0, m1)

    def sweep0(field, halos, out, faces, ts):
        for t in ts:
            slab, summed = sum0(field, halos, t)
            fresh = KEEP * slab + g0[PAD0 + t, inner_z] * (s_ref[t] + summed)
            put(out, faces, t, fresh)

    finish(sides)
    sweep0(v0a, y0.at[0], v0b, ys0.at[1], inside)
    finish(over_t)
    sweep0(v0a, y0.at[0], v0b, ys0.at[1], ends)
    for t in range(size_t):
        ys2[0, t] = v0b[PAD0 + t, inner_z, pl.ds(1, 1)]
        ys2[1, t] = v0b[PAD0 + t, inner_z, pl.ds(rows - 2, 1)]
    sides, over_t = exchange(1, v0b)
    finish(mass_copies)
    for a, b, count in area1(1, 1, 1):
        write1(g1, a, b, DAMPING / (4.0 + read1(m1, a, b, count)))

    def to_level2(slabs):
        out = []
        for t in range(part_t):
            summed = folded(slabs[2 * t] + slabs[2 * t + 1], t)
            summed = summed + pair_swap(summed, 1, 2)
            out.append((summed + pair_swap(summed, 2, 2)) * 0.0625)
        return out

    weight_copies = weights_behind()

    def remainder0(ts):
        for t in ts:
            remainder = []
            for odd in range(2):
                slab, summed = sum0(v0b, y0.at[1], 2 * t + odd)
                remainder.append(s_ref[2 * t + odd] + summed - (8.0 + m_ref[2 * t + odd]) * slab)
            s1[PAD_T + t, pl.ds(PAD_Z, pairs1), gy] = to_level1(remainder[0] + remainder[1], t)

    finish(sides)
    remainder0(range(1, size_t1 - 1))
    finish(over_t)
    remainder0((0, size_t1 - 1))
    source_copies = spread1(1, s1)
    packed(m2, to_level2([read1(m1, t, 0, pairs1) for t in range(size_t1)]))
    mass_copies = gather(0, m2, even)
    def take(field, places, cells):
        return jnp.stack([field[places[cell]] for cell in cells])

    def put3(field, cells, values):
        field[pl.ds(slots3[cells[0]], len(cells))] = values

    finish(source_copies)

    for a, b, count in area1(1, 1, 0):
        write1(v1a, a, b, read1(g1, a, b, count) * read1(s1, a, b, count))
    sweep1(v1a, v1b, (1, 0), (1, 1, 0))
    remainder = []
    held = {t: (z, count) for t, z, count in area1(1, 0)}
    for a, b, count in area1(0):
        slab, summed = sum1(v1b, a, b, count, held)
        write1(v1h, a, b, slab)
        remainder.append(
            read1(s1, a, b, count) + 0.5 * summed - (4.0 + read1(m1, a, b, count)) * slab
        )
    packed(s2, to_level2(remainder))
    source_copies = gather(1, s2, across)
    wide_copies = widen1(v1h)
    finish(mass_copies)
    mass_copies = relay(m2)
    behind_copies = second_behind()
    finish(mass_copies)
    for cell in stages["source"]:
        g2[slots[cell]] = DAMPING / (2.0 + m2[slots[cell]])
    for cells in batches(stages["coarse"][3], 24):
        put3(m3, cells, DAMPING / (1.0 + coarsened3(take(m2, slots, cells))))
    finish(source_copies)

    def around2(cell):
        t, z = cell
        return [((t + dt) % nta, (z + dz) % ngz) for dt, dz in ((-1, 0), (1, 0), (0, -1), (0, 1))]

    def sum2(field, cell):
        slab = field[slots[cell]]
        before_t, after_t, before_z, after_z = [
            slab + field[slots[other]] if other in slots else slab for other in around2(cell)
        ]
        lane = place_in(slab, 1)
        summed = jnp.where(lane % 4 >= 2, rolled(after_t, 2, 1), rolled(before_t, -2, 1))
        summed = summed + jnp.where(lane % 2 == 1, rolled(after_z, 1, 1), rolled(before_z, -1, 1))
        summed = summed + rolled(slab, 1, 0) + rolled(slab, -1, 0)
        return slab, summed + rolled(slab, 4, 1) + rolled(slab, -4, 1)

    def sweep2(field, out, cells):
        for cell in cells:
            slab, summed = sum2(field, cell)
            at = slots[cell]
            out[at] = KEEP * slab + g2[at] * (s2[at] + 0.25 * summed)

    for cell in stages["source"]:
        at = slots[cell]
        u2[at] = g2[at] * s2[at]
        w2[at] = u2[at]
    sweep2(u2, w2, stages["swept"])
    for cell in stages["coarse"][3]:
        slab, summed = sum2(w2, cell)
        at = slots[cell]
        s3[slots3[cell]] = s2[at] + 0.25 * summed - (2.0 + m2[at]) * slab
    for cells in batches(stages["coarse"][3], 24):
        source = coarsened3(take(s3, slots3, cells))
        put3(s3, cells, source)
        put3(u3, cells, take(m3, slots3, cells) * source)
    old, new = u3, w3
    for steps in (2, 1, 0):
        for cells in batches(stages["coarse"][steps], 13):
            slab = take(old, slots3, cells)
            near3 = list(zip(*[around2(cell) for cell in cells]))
            summed = take(old, slots3, near3[0]) + take(old, slots3, near3[1])
            summed = summed + take(old, slots3, near3[2]) + take(old, slots3, near3[3])
            summed = summed + rolled(slab, 2, 1) + rolled(slab, -2, 1)
            summed = summed + rolled(slab, 8, 2) + rolled(slab, -8, 2)
            fresh = KEEP * slab + take(m3, slots3, cells) * (take(s3, slots3, cells) + 0.125 * summed)
            for number, cell in enumerate(cells):
                new[slots3[cell]] = fresh[number]
        old, new = new, old
    for cells in batches(stages["base"], 24):
        fine = refined3(take(old, slots3, cells))
        for number, cell in enumerate(cells):
            w2[slots[cell]] = w2[slots[cell]] + fine[number]
    for cell in stages["base"]:
        u2[slots[cell]] = w2[slots[cell]]
    sweep2(w2, u2, stages["first"])
    sweep2(u2, w2, stages["last"])

    def correct1(t, z):
        piece = piece2(w2[slots[t // 2 % nta, z // 2 % ngz]], t % 2, z % 2)
        e2[t + 2, z + 2, pl.ds(0, full // 2, stride=2), :] = piece
        e2[t + 2, z + 2, pl.ds(1, full // 2, stride=2), :] = piece

    for t in range(-2, part_t + 2):
        for z in range(-2, part_z + 2):
            if max(-t, t - part_t + 1, 0) + max(-z, z - part_z + 1, 0) <= 3:
                correct1(t, z)
    finish(wide_copies)
    for t, z, count in area1(2, 2, 1, 1):
        write1(v1w, t, z, read1(v1h, t, z, count) + e2[t // 2 + 2, pl.ds(z + 2, count)])
    sweep1(v1w, v1x, (1, 1, 1), (2, 2, 1, 1))
    sweep1(v1x, e1, (1, 1), (1, 1, 1))

    under = lax.rem(gy + ngy - 1, ngy)
    over = lax.rem(gy + 1, ngy)

    def split1(slab):
        even = jnp.where(odd_lane(slab), rolled(slab, 1, 2), slab)
        odd = jnp.where(odd_lane(slab), slab, rolled(slab, -1, 2))
        return jnp.stack([even, odd], axis=1).reshape(2 * slab.shape[0], *slab.shape[1:])

    def corrected0(level):
        fine = split1(e1[PAD_T + level, pl.ds(PAD_Z - 1, pairs1 + 2), gy])[1:-1]
        fine = refined_z(doubled(fine, level % 4))
        beyond = [
            refined_z(split1(e1[PAD_T + level, pl.ds(PAD_Z - 1, pairs1 + 2), side, pl.ds(row, 1)])[1:-1])
            for side, row in ((under, rows1 - 1), (over, 0))
        ]
        for t in (2 * level, 2 * level + 1):
            reach = 2 - max(-t, t - size_t + 1, 0)
            out = pl.ds(PAD0 - reach, size_z + 2 * reach)
            v0w[PAD0 + t, out] = v0b[PAD0 + t, out] + fine[2 - reach:size_z + 2 + reach]
            reach -= 1
            if reach < 0:
                continue
            out = pl.ds(1 - reach, size_z + 2 * reach)
            for side in range(2):
                shifted = beyond[side][2 - reach:size_z + 2 + reach]
                y0[2, side, 1 + t, out] = y0[1, side, 1 + t, out] + shifted
                if reach == 1:
                    y2[1, side, t] = y2[0, side, t] + beyond[side][2:size_z + 2]

    finish(weight_copies)
    finish(behind_copies)
    for level in range(-1, size_t1 + 1):
        corrected0(level)
    for t in range(-1, size_t + 1):
        reach = 1 if 0 <= t < size_t else 0
        out = pl.ds(PAD0 - reach, size_z + 2 * reach)
        slab, summed = sum0(v0w, y0.at[2], t, reach)
        v0x[PAD0 + t, out] = KEEP * slab + v0a[PAD0 + t, out] + g0[PAD0 + t, out] * summed
    for t in range(size_t):
        for side, row in ((0, 0), (1, rows - 1)):
            at = lambda dt, dz: y0[2, side, 1 + t + dt, pl.ds(1 + dz, size_z)]
            slab = at(0, 0)
            summed = at(-1, 0) + at(1, 0) + at(0, -1) + at(0, 1)
            summed = summed + y2[1, side, t] + v0w[PAD0 + t, inner_z, pl.ds(row, 1)]
            summed = summed + rolled(slab, 1, 2) + rolled(slab, -1, 2)
            y0[3, side, 1 + t, own_z] = KEEP * slab + y0[0, side, 1 + t, own_z] + yg[side, t] * summed
    sweep0(v0x, y0.at[3], v0s, ys0.at[2], range(size_t))
    sides, over_t = exchange(2, v0s)

    for t in range(size_t):
        base[t] = s_ref[t] - (8.0 + m_ref[t]) * v0s[PAD0 + t, inner_z]
    finish(sides)
    finish(over_t)
    whole(0, sum(all_rows)).wait_send()


def place_in(values, axis):
    return lax.broadcasted_iota(jnp.int32, values.shape, axis)


def coarsened3(values):
    for step in (1, 2, 4):
        values = values + rolled(values, -step, 2)
    return (values + rolled(values, -1, 1)) * 0.0625


def refined3(values):
    corner = (place_in(values, 2) % 8 == 0) & (place_in(values, 1) % 2 == 0)
    values = jnp.where(corner, values, 0.0)
    values = values + rolled(values, 1, 1)
    for step in (1, 2, 4):
        values = values + rolled(values, step, 2)
    return values


def piece2(values, odd_t, odd_z):
    values = jnp.where(place_in(values, 1) % 4 == 2 * odd_t + odd_z, values, 0.0)
    values = values + rolled(values, -1 if odd_z else 1, 1)
    return values + rolled(values, -2 if odd_t else 2, 1)


def batches(cells, most):
    count = -(-len(cells) // most)
    size = -(-len(cells) // count)
    return [cells[at:at + size] for at in range(0, len(cells), size)]


def grown(cells, steps, count_t, count_z):
    for _ in range(steps):
        cells = cells | {
            ((t + dt) % count_t, (z + dz) % count_z)
            for t, z in cells for dt, dz in ((-1, 0), (1, 0), (0, -1), (0, 1))
        }
    return cells


def plan(nta, ngz):
    sites = lambda cells, steps: grown(cells, steps, 2 * nta, 2 * ngz)
    blocks = lambda cells: {(t // 2, z // 2) for t, z in cells}
    inner = lambda cells: {(2 * t + a, 2 * z + b) for t, z in cells for a in (0, 1) for b in (0, 1)}
    box = {(t % (2 * nta), z % (2 * ngz)) for t in range(-2, 4) for z in range(-2, 4)}
    last = sites(inner({(0, 0)}), 3) & box
    first, base = sites(last, 1), sites(last, 2)
    coarse = [grown(blocks(base), steps, nta, ngz) for steps in range(4)]
    swept = sites(inner(coarse[3]), 1) | base
    ordered = lambda cells: sorted(cells, key=lambda c: ((c[0] + nta // 2) % nta, (c[1] + ngz // 2) % ngz))
    return {
        "last": ordered(blocks(last)), "first": ordered(blocks(first)), "base": ordered(blocks(base)),
        "coarse": [ordered(cells) for cells in coarse], "swept": ordered(blocks(swept)),
        "source": ordered(blocks(sites(swept, 1))),
    }


def per_device(sizes, right_side, mass_field):
    nta, ngz, ngy = sizes
    size_t, size_z, rows, lanes = right_side.shape
    size_t1, pairs1, rows1 = size_t // 2, size_z // 4, rows // 2
    part_t, part_z, rows2 = size_t // 4, size_z // 4, rows // 4
    vmem = lambda *shape: pltpu.VMEM(shape, jnp.float32)
    dma = lambda *shape: pltpu.SemaphoreType.DMA(shape)
    padded0 = vmem(size_t + 2 * PAD0, size_z + 2 * PAD0, rows, lanes)
    faces = vmem(2, size_t, size_z, 1, lanes)
    padded1 = vmem(size_t1 + 2 * PAD_T, pairs1 + 2 * PAD_Z, ngy, rows1, lanes)
    window = len(plan(nta, ngz)["source"])
    packs = vmem(window, rows2 * ngy, lanes)
    packs3 = vmem(len(plan(nta, ngz)["coarse"][3]), rows2 * ngy, lanes)
    scratch = [
        *[padded0] * 5,
        vmem(4, 2, size_t + 2, size_z + 2, 1, lanes), vmem(3, 2, size_t, size_z, 1, lanes),
        vmem(2, 2, size_t, size_z, 1, lanes), faces, faces, faces,
        vmem(max(size_t1, part_t + 2), size_z, max(rows, ngy * rows1), lanes),
        *[padded1] * 9, vmem(part_t + 4, part_z + 4, ngy * rows1, lanes),
        *[packs] * 5, *[packs3] * 4,
        vmem(size_t, size_z, rows, lanes), vmem(size_t, size_z, rows, lanes),
        vmem(8192, 1, lanes), pltpu.SemaphoreType.DMA, dma(15), dma(2, 2),
    ]
    array = lambda *shape: jax.ShapeDtypeStruct(shape, jnp.float32)
    block, place = array(*right_side.shape), pl.BlockSpec(memory_space=pltpu.VMEM)
    kept = pl.pallas_call(
        functools.partial(kernel, sizes),
        out_shape=(
            array(size_t + 2 * PAD0, size_z + 2 * PAD0, rows, lanes), array(2, size_t, size_z, 1, lanes), block,
        ),
        in_specs=[pl.BlockSpec(memory_space=pltpu.HBM)] * 2,
        out_specs=(place,) * 3,
        scratch_shapes=scratch,
        compiler_params=pltpu.CompilerParams(
            collective_id=0, has_side_effects=True, vmem_limit_bytes=48 * 1024 * 1024
        ),
    )(*[pltpu.with_memory_space_constraint(values, pltpu.HBM) for values in (right_side, mass_field)])
    return pl.pallas_call(
        last_kernel,
        out_shape=(block, block),
        in_specs=[place] * 3,
        out_specs=(pl.BlockSpec(memory_space=pltpu.HBM),) * 2,
        scratch_shapes=[vmem(size_t, size_z, rows, lanes), dma(3)],
        compiler_params=pltpu.CompilerParams(vmem_limit_bytes=8 * 1024 * 1024),
    )(*kept)


def solution(mesh):
    sizes = tuple(mesh.shape[axis] for axis in ("ta", "gz", "gy"))
    spec = P("ta", "gz", "gy", None)
    return jax.shard_map(
        functools.partial(per_device, sizes),
        mesh=mesh,
        in_specs=(spec, spec),
        out_specs=(spec, spec),
        check_vma=False,
    )
```

```python
import functools

import jax
import jax.numpy as jnp
from jax import lax
from jax.experimental import pallas as pl
from jax.experimental.pallas import tpu as pltpu
from jax.sharding import PartitionSpec as P

DAMPING = 0.7
KEEP = 1.0 - DAMPING
PAD0, PAD_T, PAD_Z = 2, 3, 2
MESH = pl.DeviceIdType.MESH


def rolled(values, shift, axis):
    return pltpu.roll(values, shift % values.shape[axis], axis)


def odd_lane(values):
    return lax.broadcasted_iota(jnp.int32, values.shape, values.ndim - 1) % 2 == 1


def pair_swap(values, step, axis):
    index = lax.broadcasted_iota(jnp.int32, values.shape, axis)
    return jnp.where((index // step) % 2 == 0, rolled(values, -step, axis), rolled(values, step, axis))


def z_pairs(summed):
    count, rows, lanes = summed.shape
    summed = summed.reshape(count // 2, 2, rows, lanes)
    return summed[:, 0] + summed[:, 1]


def refined_z(slab):
    return jnp.repeat(slab, 2, axis=0)


def neighbours0(field, low, high, t, start=0, count=None):
    count = count or field.shape[1] - 2 * PAD0
    at = lambda dt, dz: field[PAD0 + t + dt, pl.ds(PAD0 + start + dz, count)]
    slab = at(0, 0)
    row = lax.broadcasted_iota(jnp.int32, slab.shape, 1)
    summed = at(-1, 0) + at(1, 0) + at(0, -1) + at(0, 1)
    summed = summed + jnp.where(row == 0, low, rolled(slab, 1, 1))
    summed = summed + jnp.where(row == slab.shape[1] - 1, high, rolled(slab, -1, 1))
    return slab, summed + rolled(slab, 1, 2) + rolled(slab, -1, 2)


def last_kernel(v0s, yl, base, sol_hbm, res_hbm, res, written):
    size_t, size_z = base.shape[:2]
    copies = [pltpu.make_async_copy(v0s.at[pl.ds(PAD0, size_t), pl.ds(PAD0, size_z)], sol_hbm, written.at[0])]
    copies[0].start()
    for part in range(2):
        own = pl.ds(part * (size_t // 2), size_t // 2)
        for t in range(part * (size_t // 2), (part + 1) * (size_t // 2)):
            _, summed = neighbours0(v0s, yl[0, t], yl[1, t], t)
            res[t] = base[t] + summed
        copies.append(pltpu.make_async_copy(res.at[own], res_hbm.at[own], written.at[1 + part]))
        copies[-1].start()
    for copy in copies:
        copy.wait()


def kernel(sizes, s_hbm, m_hbm, v0s, yl, base, *scratch):
    nta, ngz, ngy = sizes
    (g0, v0a, v0b, v0w, v0x, y0, ys0, y2, ys2, yg, ysg, fold,
     s1, m1, g1, v1a, v1b, v1h, v1w, v1x, e1, e2,
     m2, s2, g2, u2, w2, m3, s3, u3, w3,
     s_ref, m_ref, tally, departed, arrived, loaded) = scratch
    size_t, size_z, rows, lanes = s_ref.shape
    size_t1, pairs1, rows1 = size_t // 2, size_z // 4, rows // 2
    part_t, part_z, rows2 = size_t // 4, size_z // 4, rows // 4
    stages = plan(nta, ngz)
    slots = {cell: number for number, cell in enumerate(stages["source"])}
    slots3 = {cell: number for number, cell in enumerate(stages["coarse"][3])}
    ta, gz, gy = lax.axis_index("ta"), lax.axis_index("gz"), lax.axis_index("gy")

    places = {}

    def place_of(axis, at, step, count):
        key = axis, step % count
        if key not in places:
            places[key] = at if key[1] == 0 else lax.rem(at + key[1], count)
        return places[key]

    def device(dt, dz, dy):
        return {
            "ta": place_of("ta", ta, dt, nta), "gz": place_of("gz", gz, dz, ngz), "gy": place_of("gy", gy, dy, ngy),
        }

    near = [(dt, dz, dy) for dt in (-1, 0, 1) for dz in (-1, 0, 1) for dy in range(ngy)]
    centred = lambda d, n: (d + n // 2) % n - n // 2
    across = sorted(
        (cell for cell in slots if cell != (0, 0)),
        key=lambda c: -(abs(centred(c[0], nta)) + 2 * abs(centred(c[1], ngz))),
    )
    half = size_t // 2
    loads = [
        [
            pltpu.make_async_copy(source.at[pl.ds(part * half, half)], target.at[pl.ds(part * half, half)], loaded.at[part, place])
            for place, (source, target) in enumerate(((m_hbm, m_ref), (s_hbm, s_ref)))
        ]
        for part in range(2)
    ]
    met = {(dt % nta, dz % ngz, dy % ngy) for dt, dz, dy in near + [(-t, -z, 0) for t, z in across]} - {(0, 0, 0)}
    met = sorted(met, key=lambda d: (-abs(centred(d[0], nta)) - 2 * abs(centred(d[1], ngz)) - 2 * d[2], d))
    barrier = pltpu.get_barrier_semaphore()
    for offset in met:
        pl.semaphore_signal(barrier, inc=1, device_id=device(*offset), device_id_type=MESH)
    for load in loads[0] + loads[1]:
        load.start()

    rows_of, all_rows = {}, []

    def send(group, moves):
        for source, target, offset in moves:
            pltpu.make_async_remote_copy(
                src_ref=source, dst_ref=target, send_sem=departed, recv_sem=arrived.at[group],
                device_id=offset if isinstance(offset, dict) else device(*offset), device_id_type=MESH,
            ).start()
            count = 1
            for extent in source.shape[:-1]:
                count *= extent
            rows_of[group] = rows_of.get(group, 0) + count
            all_rows.append(count)
        return group

    def whole(group, count):
        view = tally.at[pl.ds(0, count)]
        return pltpu.make_async_remote_copy(
            src_ref=view, dst_ref=view, send_sem=departed, recv_sem=arrived.at[group],
            device_id=device(1, 0, 0), device_id_type=MESH,
        )

    def finish(group):
        whole(group, rows_of[group]).wait_recv()

    inner_t, inner_z = pl.ds(PAD0, size_t), pl.ds(PAD0, size_z)

    def faces0(field, depth):
        one = lambda at: pl.ds(PAD0 + at, 1)
        return [
            (field.at[inner_t, one(size_z - depth)], field.at[inner_t, one(-depth)], (0, 1, 0)),
            (field.at[inner_t, one(depth - 1)], field.at[inner_t, one(size_z - 1 + depth)], (0, -1, 0)),
            (field.at[one(size_t - depth), inner_z], field.at[one(-depth), inner_z], (1, 0, 0)),
            (field.at[one(depth - 1), inner_z], field.at[one(size_t - 1 + depth), inner_z], (-1, 0, 0)),
        ]

    own_t, own_z = pl.ds(1, size_t), pl.ds(1, size_z)

    def exchange(number, field):
        faces = ys0.at[number]
        low, high = [y0.at[number, side, own_t, own_z] if number < 2 else yl.at[side] for side in range(2)]
        moves = [(faces.at[1], low, (0, 0, 1)), (faces.at[0], high, (0, 0, -1))] + faces0(field, 1)
        return send(2 * number, moves[:4]), send(2 * number + 1, moves[4:])

    def weights_behind():
        moves = [(ysg.at[1], yg.at[0], (0, 0, 1)), (ysg.at[0], yg.at[1], (0, 0, -1))]
        return send(6, moves + faces0(g0, 1))

    def second_behind():
        one = lambda at: pl.ds(at, 1)
        moves = [(ys2.at[1], y2.at[0, 0], (0, 0, 1)), (ys2.at[0], y2.at[0, 1], (0, 0, -1))]
        for up_t in (1, 0):
            for up_z in (1, 0):
                moves.append((
                    v0b.at[one(PAD0 + (size_t - 1) * up_t), one(PAD0 + (size_z - 1) * up_z)],
                    v0b.at[one(PAD0 - 1 + (size_t + 1) * (1 - up_t)), one(PAD0 - 1 + (size_z + 1) * (1 - up_z))],
                    (2 * up_t - 1, 2 * up_z - 1, 0),
                ))
        for up_y in (1, 0):
            faces, halos = ys0.at[1, up_y], y0.at[1, 1 - up_y]
            for up in (1, 0):
                moves.append((
                    faces.at[one((size_t - 1) * up)], halos.at[one((size_t + 1) * (1 - up)), own_z],
                    (2 * up - 1, 0, 2 * up_y - 1),
                ))
                moves.append((
                    faces.at[:, one((size_z - 1) * up)], halos.at[own_t, one((size_z + 1) * (1 - up))],
                    (0, 2 * up - 1, 2 * up_y - 1),
                ))
        return send(7, moves + faces0(v0b, 2))

    def layers1(deep_t, deep_z, corner_t):
        own_t, own_z = pl.ds(PAD_T, size_t1), pl.ds(PAD_Z, pairs1)

        def span(pad, size, deep, up):
            return pl.ds(pad + (size - deep) * up, deep), pl.ds(pad + size - (size + deep) * up, deep)

        moves = []
        for up in (1, 0):
            for up_z in (1, 0):
                here_t, there_t = span(PAD_T, size_t1, corner_t, up)
                here_z, there_z = span(PAD_Z, pairs1, 1, up_z)
                moves.append((here_t, here_z, there_t, there_z, 2 * up - 1, 2 * up_z - 1))
        for up in (1, 0):
            here, there = span(PAD_T, size_t1, deep_t, up)
            moves.append((here, own_z, there, own_z, 2 * up - 1, 0))
            here, there = span(PAD_Z, pairs1, deep_z, up)
            moves.append((own_t, here, own_t, there, 0, 2 * up - 1))
        return moves

    def spread1(number, field):
        part = pl.ds(gy, 1)
        own = field.at[pl.ds(PAD_T, size_t1), pl.ds(PAD_Z, pairs1), part]
        moves = [(own, own, (0, 0, dy)) for dy in range(1, ngy)]
        for dy in reversed(range(ngy)):
            for here_t, here_z, there_t, there_z, dt, dz in layers1(2, 1, 2):
                moves.append((field.at[here_t, here_z, part], field.at[there_t, there_z, part], (dt, dz, dy)))
        return send(8 + number, moves)

    def widen1(field):
        moves = [
            (field.at[here_t, here_z], field.at[there_t, there_z], (dt, dz, 0))
            for here_t, here_z, there_t, there_z, dt, dz in layers1(3, 2, 3)
        ]
        one = lambda at: pl.ds(at, 1)
        for up in (1, 0):
            for up_z in (1, 0):
                moves.append((
                    field.at[one(PAD_T + (size_t1 - 1) * up), one(PAD_Z + 1 + (pairs1 - 3) * up_z)],
                    field.at[one(PAD_T - 1 + (size_t1 + 1) * (1 - up)), one(PAD_Z - 2 + (pairs1 + 3) * (1 - up_z))],
                    (2 * up - 1, 2 * up_z - 1, 0),
                ))
        return send(10, moves)

    def gather(number, field, cells):
        own = field.at[slots[0, 0]]
        return send(11 + number, [(own, field.at[slots[cell]], (-cell[0], -cell[1], 0)) for cell in cells])

    core = lax.rem(ta, 2)
    even = [cell for cell in across if cell[0] % 2 == 0]

    def relay(field):
        sibling = {"ta": ta + 1 - 2 * core, "gz": gz, "gy": gy}
        count = len(slots) // ngz // 2
        return send(13, [
            (
                field.at[pl.ds((2 * number + 2 - 2 * core) * ngz, ngz)],
                field.at[pl.ds((2 * number + 1) * ngz, ngz)], sibling,
            )
            for number in range(count)
        ])

    def put(field, faces, t, slab):
        field[PAD0 + t, inner_z] = slab
        faces[0, t] = slab[:, :1]
        faces[1, t] = slab[:, rows - 1:]

    def sum0(field, halos, t, reach=0):
        count = size_z + 2 * reach
        out = pl.ds(1 - reach, count)
        return neighbours0(field, halos[0, 1 + t, out], halos[1, 1 + t, out], t, -reach, count)

    def folded(summed, place):
        count, high, _ = summed.shape
        view = fold.at[place, pl.ds(0, count)]
        view[...] = summed
        return view[:, pl.ds(0, high // 2, stride=2), :] + view[:, pl.ds(1, high // 2, stride=2), :]

    def to_level1(summed, place):
        summed = folded(z_pairs(summed), place)
        summed = summed.reshape(summed.shape[0] // 2, 2, *summed.shape[1:])
        even, odd = summed[:, 0], summed[:, 1]
        even, odd = even + rolled(even, -1, 2), odd + rolled(odd, 1, 2)
        return jnp.where(odd_lane(even), odd, even) * 0.0625

    def doubled(slab, place):
        count, high, _ = slab.shape
        view = fold.at[place, pl.ds(0, count)]
        view[:, pl.ds(0, high, stride=2), :] = slab
        view[:, pl.ds(1, high, stride=2), :] = slab
        return view[...]

    full = ngy * rows1

    def area1(*reaches):
        far = len(reaches) - 1
        for t in range(-far, size_t1 + far):
            reach = reaches[max(-t, t - size_t1 + 1, 0)]
            yield t, -reach, pairs1 + 2 * reach

    def read1(field, t, z, count):
        return field[PAD_T + t, pl.ds(PAD_Z + z, count)].reshape(count, full, lanes)

    def write1(field, t, z, slab):
        field[PAD_T + t, pl.ds(PAD_Z + z, slab.shape[0])] = slab.reshape(slab.shape[0], ngy, rows1, lanes)

    def sum1(field, t, z, count, held):
        slab = read1(field, t, z, count)
        summed = read1(field, t - 1, z, count) + read1(field, t + 1, z, count)
        if held[t][0] < z:
            before, after = read1(field, t, z - 1, count), read1(field, t, z + 1, count)
        else:
            before = jnp.concatenate([slab[:1], slab[:-1]], axis=0)
            after = jnp.concatenate([slab[1:], slab[-1:]], axis=0)
        summed = summed + jnp.where(odd_lane(slab), rolled(slab + after, 1, 2), rolled(slab + before, -1, 2))
        summed = summed + rolled(slab, 1, 1) + rolled(slab, -1, 1)
        return slab, summed + rolled(slab, 2, 2) + rolled(slab, -2, 2)

    def sweep1(field, out, area, held):
        held = {t: (z, count) for t, z, count in area1(*held)}
        for t, z, count in area1(*area):
            slab, summed = sum1(field, t, z, count, held)
            fresh = KEEP * slab + read1(g1, t, z, count) * (read1(s1, t, z, count) + 0.5 * summed)
            write1(out, t, z, fresh)

    def packed(out, slabs):
        parts = [slab[z] for slab in slabs for z in range(part_z)]
        lane = lax.broadcasted_iota(jnp.int32, parts[0].shape, 1)
        values = parts[0]
        for k in range(1, len(parts)):
            values = jnp.where(lane % 4 == k, parts[k], values)
        out[slots[0, 0]] = values

    inside = list(range(1, size_t - 1))
    ends = [0, size_t - 1]

    for part in range(2):
        for load in loads[part]:
            load.wait()
        for t in range(part * half, (part + 1) * half):
            weight = DAMPING / (8.0 + m_ref[t])
            put(g0, ysg, t, weight)
            put(v0a, ys0.at[0], t, weight * s_ref[t])

    pl.semaphore_wait(barrier, len(met))
    sides, over_t = exchange(0, v0a)
    for t in range(size_t1):
        m1[PAD_T + t, pl.ds(PAD_Z, pairs1), gy] = to_level1(m_ref[2 * t] + m_ref[2 * t + 1], t)

    def sweep0(field, halos, out, faces, ts):
        for t in ts:
            slab, summed = sum0(field, halos, t)
            fresh = KEEP * slab + g0[PAD0 + t, inner_z] * (s_ref[t] + summed)
            put(out, faces, t, fresh)

    finish(sides)
    sweep0(v0a, y0.at[0], v0b, ys0.at[1], inside)
    finish(over_t)
    sweep0(v0a, y0.at[0], v0b, ys0.at[1], ends)
    for t in range(size_t):
        ys2[0, t] = v0b[PAD0 + t, inner_z, pl.ds(1, 1)]
        ys2[1, t] = v0b[PAD0 + t, inner_z, pl.ds(rows - 2, 1)]
    sides, over_t = exchange(1, v0b)
    mass_copies = spread1(0, m1)

    def to_level2(slabs):
        out = []
        for t in range(part_t):
            summed = folded(slabs[2 * t] + slabs[2 * t + 1], t)
            summed = summed + pair_swap(summed, 1, 2)
            out.append((summed + pair_swap(summed, 2, 2)) * 0.0625)
        return out


    def remainder0(ts):
        for t in ts:
            remainder = []
            for odd in range(2):
                slab, summed = sum0(v0b, y0.at[1], 2 * t + odd)
                remainder.append(s_ref[2 * t + odd] + summed - (8.0 + m_ref[2 * t + odd]) * slab)
            s1[PAD_T + t, pl.ds(PAD_Z, pairs1), gy] = to_level1(remainder[0] + remainder[1], t)

    finish(sides)
    remainder0(range(1, size_t1 - 1))
    finish(over_t)
    remainder0((0, size_t1 - 1))
    source_copies = spread1(1, s1)
    finish(mass_copies)
    for a, b, count in area1(1, 1, 1):
        write1(g1, a, b, DAMPING / (4.0 + read1(m1, a, b, count)))
    packed(m2, to_level2([read1(m1, t, 0, pairs1) for t in range(size_t1)]))
    mass_copies = gather(0, m2, even)
    weight_copies = weights_behind()
    def take(field, places, cells):
        return jnp.stack([field[places[cell]] for cell in cells])

    def put3(field, cells, values):
        field[pl.ds(slots3[cells[0]], len(cells))] = values

    finish(source_copies)

    for a, b, count in area1(1, 1, 0):
        write1(v1a, a, b, read1(g1, a, b, count) * read1(s1, a, b, count))
    sweep1(v1a, v1b, (1, 0), (1, 1, 0))
    remainder = []
    held = {t: (z, count) for t, z, count in area1(1, 0)}
    for a, b, count in area1(0):
        slab, summed = sum1(v1b, a, b, count, held)
        write1(v1h, a, b, slab)
        remainder.append(
            read1(s1, a, b, count) + 0.5 * summed - (4.0 + read1(m1, a, b, count)) * slab
        )
    packed(s2, to_level2(remainder))
    source_copies = gather(1, s2, across)
    wide_copies = widen1(v1h)
    finish(mass_copies)
    mass_copies = relay(m2)
    behind_copies = second_behind()
    finish(mass_copies)
    for cell in stages["source"]:
        g2[slots[cell]] = DAMPING / (2.0 + m2[slots[cell]])
    for cells in batches(stages["coarse"][3], 24):
        put3(m3, cells, DAMPING / (1.0 + coarsened3(take(m2, slots, cells))))
    finish(source_copies)

    def around2(cell):
        t, z = cell
        return [((t + dt) % nta, (z + dz) % ngz) for dt, dz in ((-1, 0), (1, 0), (0, -1), (0, 1))]

    def sum2(field, cell):
        slab = field[slots[cell]]
        before_t, after_t, before_z, after_z = [
            slab + field[slots[other]] if other in slots else slab for other in around2(cell)
        ]
        lane = place_in(slab, 1)
        summed = jnp.where(lane % 4 >= 2, rolled(after_t, 2, 1), rolled(before_t, -2, 1))
        summed = summed + jnp.where(lane % 2 == 1, rolled(after_z, 1, 1), rolled(before_z, -1, 1))
        summed = summed + rolled(slab, 1, 0) + rolled(slab, -1, 0)
        return slab, summed + rolled(slab, 4, 1) + rolled(slab, -4, 1)

    def sweep2(field, out, cells):
        for cell in cells:
            slab, summed = sum2(field, cell)
            at = slots[cell]
            out[at] = KEEP * slab + g2[at] * (s2[at] + 0.25 * summed)

    for cell in stages["source"]:
        at = slots[cell]
        u2[at] = g2[at] * s2[at]
        w2[at] = u2[at]
    sweep2(u2, w2, stages["swept"])
    for cell in stages["coarse"][3]:
        slab, summed = sum2(w2, cell)
        at = slots[cell]
        s3[slots3[cell]] = s2[at] + 0.25 * summed - (2.0 + m2[at]) * slab
    for cells in batches(stages["coarse"][3], 24):
        source = coarsened3(take(s3, slots3, cells))
        put3(s3, cells, source)
        put3(u3, cells, take(m3, slots3, cells) * source)
    old, new = u3, w3
    for steps in (2, 1, 0):
        for cells in batches(stages["coarse"][steps], 13):
            slab = take(old, slots3, cells)
            near3 = list(zip(*[around2(cell) for cell in cells]))
            summed = take(old, slots3, near3[0]) + take(old, slots3, near3[1])
            summed = summed + take(old, slots3, near3[2]) + take(old, slots3, near3[3])
            summed = summed + rolled(slab, 2, 1) + rolled(slab, -2, 1)
            summed = summed + rolled(slab, 8, 2) + rolled(slab, -8, 2)
            fresh = KEEP * slab + take(m3, slots3, cells) * (take(s3, slots3, cells) + 0.125 * summed)
            for number, cell in enumerate(cells):
                new[slots3[cell]] = fresh[number]
        old, new = new, old
    for cells in batches(stages["base"], 24):
        fine = refined3(take(old, slots3, cells))
        for number, cell in enumerate(cells):
            w2[slots[cell]] = w2[slots[cell]] + fine[number]
    for cell in stages["base"]:
        u2[slots[cell]] = w2[slots[cell]]
    sweep2(w2, u2, stages["first"])
    sweep2(u2, w2, stages["last"])

    def correct1(t, z):
        piece = piece2(w2[slots[t // 2 % nta, z // 2 % ngz]], t % 2, z % 2)
        e2[t + 2, z + 2, pl.ds(0, full // 2, stride=2), :] = piece
        e2[t + 2, z + 2, pl.ds(1, full // 2, stride=2), :] = piece

    for t in range(-2, part_t + 2):
        for z in range(-2, part_z + 2):
            if max(-t, t - part_t + 1, 0) + max(-z, z - part_z + 1, 0) <= 3:
                correct1(t, z)
    finish(wide_copies)
    for t, z, count in area1(2, 2, 1, 1):
        write1(v1w, t, z, read1(v1h, t, z, count) + e2[t // 2 + 2, pl.ds(z + 2, count)])
    sweep1(v1w, v1x, (1, 1, 1), (2, 2, 1, 1))
    sweep1(v1x, e1, (1, 1), (1, 1, 1))

    under = lax.rem(gy + ngy - 1, ngy)
    over = lax.rem(gy + 1, ngy)

    def split1(slab):
        even = jnp.where(odd_lane(slab), rolled(slab, 1, 2), slab)
        odd = jnp.where(odd_lane(slab), slab, rolled(slab, -1, 2))
        return jnp.stack([even, odd], axis=1).reshape(2 * slab.shape[0], *slab.shape[1:])

    def corrected0(level):
        fine = split1(e1[PAD_T + level, pl.ds(PAD_Z - 1, pairs1 + 2), gy])[1:-1]
        fine = refined_z(doubled(fine, level % 4))
        beyond = [
            refined_z(split1(e1[PAD_T + level, pl.ds(PAD_Z - 1, pairs1 + 2), side, pl.ds(row, 1)])[1:-1])
            for side, row in ((under, rows1 - 1), (over, 0))
        ]
        for t in (2 * level, 2 * level + 1):
            reach = 2 - max(-t, t - size_t + 1, 0)
            out = pl.ds(PAD0 - reach, size_z + 2 * reach)
            v0w[PAD0 + t, out] = v0b[PAD0 + t, out] + fine[2 - reach:size_z + 2 + reach]
            reach -= 1
            if reach < 0:
                continue
            out = pl.ds(1 - reach, size_z + 2 * reach)
            for side in range(2):
                shifted = beyond[side][2 - reach:size_z + 2 + reach]
                y0[2, side, 1 + t, out] = y0[1, side, 1 + t, out] + shifted
                if reach == 1:
                    y2[1, side, t] = y2[0, side, t] + beyond[side][2:size_z + 2]

    finish(weight_copies)
    finish(behind_copies)
    for level in range(-1, size_t1 + 1):
        corrected0(level)
    for t in range(-1, size_t + 1):
        reach = 1 if 0 <= t < size_t else 0
        out = pl.ds(PAD0 - reach, size_z + 2 * reach)
        slab, summed = sum0(v0w, y0.at[2], t, reach)
        v0x[PAD0 + t, out] = KEEP * slab + v0a[PAD0 + t, out] + g0[PAD0 + t, out] * summed
    for t in range(size_t):
        for side, row in ((0, 0), (1, rows - 1)):
            at = lambda dt, dz: y0[2, side, 1 + t + dt, pl.ds(1 + dz, size_z)]
            slab = at(0, 0)
            summed = at(-1, 0) + at(1, 0) + at(0, -1) + at(0, 1)
            summed = summed + y2[1, side, t] + v0w[PAD0 + t, inner_z, pl.ds(row, 1)]
            summed = summed + rolled(slab, 1, 2) + rolled(slab, -1, 2)
            y0[3, side, 1 + t, own_z] = KEEP * slab + y0[0, side, 1 + t, own_z] + yg[side, t] * summed
    sweep0(v0x, y0.at[3], v0s, ys0.at[2], range(size_t))
    sides, over_t = exchange(2, v0s)

    for t in range(size_t):
        base[t] = s_ref[t] - (8.0 + m_ref[t]) * v0s[PAD0 + t, inner_z]
    finish(sides)
    finish(over_t)
    whole(0, sum(all_rows)).wait_send()


def place_in(values, axis):
    return lax.broadcasted_iota(jnp.int32, values.shape, axis)


def coarsened3(values):
    for step in (1, 2, 4):
        values = values + rolled(values, -step, 2)
    return (values + rolled(values, -1, 1)) * 0.0625


def refined3(values):
    corner = (place_in(values, 2) % 8 == 0) & (place_in(values, 1) % 2 == 0)
    values = jnp.where(corner, values, 0.0)
    values = values + rolled(values, 1, 1)
    for step in (1, 2, 4):
        values = values + rolled(values, step, 2)
    return values


def piece2(values, odd_t, odd_z):
    values = jnp.where(place_in(values, 1) % 4 == 2 * odd_t + odd_z, values, 0.0)
    values = values + rolled(values, -1 if odd_z else 1, 1)
    return values + rolled(values, -2 if odd_t else 2, 1)


def batches(cells, most):
    count = -(-len(cells) // most)
    size = -(-len(cells) // count)
    return [cells[at:at + size] for at in range(0, len(cells), size)]


def grown(cells, steps, count_t, count_z):
    for _ in range(steps):
        cells = cells | {
            ((t + dt) % count_t, (z + dz) % count_z)
            for t, z in cells for dt, dz in ((-1, 0), (1, 0), (0, -1), (0, 1))
        }
    return cells


def plan(nta, ngz):
    sites = lambda cells, steps: grown(cells, steps, 2 * nta, 2 * ngz)
    blocks = lambda cells: {(t // 2, z // 2) for t, z in cells}
    inner = lambda cells: {(2 * t + a, 2 * z + b) for t, z in cells for a in (0, 1) for b in (0, 1)}
    box = {(t % (2 * nta), z % (2 * ngz)) for t in range(-2, 4) for z in range(-2, 4)}
    last = sites(inner({(0, 0)}), 3) & box
    first, base = sites(last, 1), sites(last, 2)
    coarse = [grown(blocks(base), steps, nta, ngz) for steps in range(4)]
    swept = sites(inner(coarse[3]), 1) | base
    ordered = lambda cells: sorted(cells, key=lambda c: ((c[0] + nta // 2) % nta, (c[1] + ngz // 2) % ngz))
    return {
        "last": ordered(blocks(last)), "first": ordered(blocks(first)), "base": ordered(blocks(base)),
        "coarse": [ordered(cells) for cells in coarse], "swept": ordered(blocks(swept)),
        "source": ordered(blocks(sites(swept, 1))),
    }


def per_device(sizes, right_side, mass_field):
    nta, ngz, ngy = sizes
    size_t, size_z, rows, lanes = right_side.shape
    size_t1, pairs1, rows1 = size_t // 2, size_z // 4, rows // 2
    part_t, part_z, rows2 = size_t // 4, size_z // 4, rows // 4
    vmem = lambda *shape: pltpu.VMEM(shape, jnp.float32)
    dma = lambda *shape: pltpu.SemaphoreType.DMA(shape)
    padded0 = vmem(size_t + 2 * PAD0, size_z + 2 * PAD0, rows, lanes)
    faces = vmem(2, size_t, size_z, 1, lanes)
    padded1 = vmem(size_t1 + 2 * PAD_T, pairs1 + 2 * PAD_Z, ngy, rows1, lanes)
    window = len(plan(nta, ngz)["source"])
    packs = vmem(window, rows2 * ngy, lanes)
    packs3 = vmem(len(plan(nta, ngz)["coarse"][3]), rows2 * ngy, lanes)
    scratch = [
        *[padded0] * 5,
        vmem(4, 2, size_t + 2, size_z + 2, 1, lanes), vmem(3, 2, size_t, size_z, 1, lanes),
        vmem(2, 2, size_t, size_z, 1, lanes), faces, faces, faces,
        vmem(max(size_t1, part_t + 2), size_z, max(rows, ngy * rows1), lanes),
        *[padded1] * 9, vmem(part_t + 4, part_z + 4, ngy * rows1, lanes),
        *[packs] * 5, *[packs3] * 4,
        vmem(size_t, size_z, rows, lanes), vmem(size_t, size_z, rows, lanes),
        vmem(8192, 1, lanes), pltpu.SemaphoreType.DMA, dma(15), dma(2, 2),
    ]
    array = lambda *shape: jax.ShapeDtypeStruct(shape, jnp.float32)
    block, place = array(*right_side.shape), pl.BlockSpec(memory_space=pltpu.VMEM)
    kept = pl.pallas_call(
        functools.partial(kernel, sizes),
        out_shape=(
            array(size_t + 2 * PAD0, size_z + 2 * PAD0, rows, lanes), array(2, size_t, size_z, 1, lanes), block,
        ),
        in_specs=[pl.BlockSpec(memory_space=pltpu.HBM)] * 2,
        out_specs=(place,) * 3,
        scratch_shapes=scratch,
        compiler_params=pltpu.CompilerParams(
            collective_id=0, has_side_effects=True, vmem_limit_bytes=48 * 1024 * 1024
        ),
    )(*[pltpu.with_memory_space_constraint(values, pltpu.HBM) for values in (right_side, mass_field)])
    return pl.pallas_call(
        last_kernel,
        out_shape=(block, block),
        in_specs=[place] * 3,
        out_specs=(pl.BlockSpec(memory_space=pltpu.HBM),) * 2,
        scratch_shapes=[vmem(size_t, size_z, rows, lanes), dma(3)],
        compiler_params=pltpu.CompilerParams(vmem_limit_bytes=8 * 1024 * 1024),
    )(*kept)


def solution(mesh):
    sizes = tuple(mesh.shape[axis] for axis in ("ta", "gz", "gy"))
    spec = P("ta", "gz", "gy", None)
    return jax.shard_map(
        functools.partial(per_device, sizes),
        mesh=mesh,
        in_specs=(spec, spec),
        out_specs=(spec, spec),
        check_vma=False,
    )
```

```python
import functools

import jax
import jax.numpy as jnp
from jax import lax
from jax.experimental import pallas as pl
from jax.experimental.pallas import tpu as pltpu
from jax.sharding import PartitionSpec as P

DAMPING = 0.7
KEEP = 1.0 - DAMPING
PAD0, PAD_T, PAD_Z = 2, 3, 2
MESH = pl.DeviceIdType.MESH


def rolled(values, shift, axis):
    return pltpu.roll(values, shift % values.shape[axis], axis)


def odd_lane(values):
    return lax.broadcasted_iota(jnp.int32, values.shape, values.ndim - 1) % 2 == 1


def pair_swap(values, step, axis):
    index = lax.broadcasted_iota(jnp.int32, values.shape, axis)
    return jnp.where((index // step) % 2 == 0, rolled(values, -step, axis), rolled(values, step, axis))


def z_pairs(summed):
    count, rows, lanes = summed.shape
    summed = summed.reshape(count // 2, 2, rows, lanes)
    return summed[:, 0] + summed[:, 1]


def refined_z(slab):
    return jnp.repeat(slab, 2, axis=0)


def neighbours0(field, low, high, t, start=0, count=None):
    count = count or field.shape[1] - 2 * PAD0
    at = lambda dt, dz: field[PAD0 + t + dt, pl.ds(PAD0 + start + dz, count)]
    slab = at(0, 0)
    row = lax.broadcasted_iota(jnp.int32, slab.shape, 1)
    summed = at(-1, 0) + at(1, 0) + at(0, -1) + at(0, 1)
    summed = summed + jnp.where(row == 0, low, rolled(slab, 1, 1))
    summed = summed + jnp.where(row == slab.shape[1] - 1, high, rolled(slab, -1, 1))
    return slab, summed + rolled(slab, 1, 2) + rolled(slab, -1, 2)


def last_kernel(v0s, yl, base, sol_hbm, res_hbm, res, written):
    size_t, size_z = base.shape[:2]
    copies = [pltpu.make_async_copy(v0s.at[pl.ds(PAD0, size_t), pl.ds(PAD0, size_z)], sol_hbm, written.at[0])]
    copies[0].start()
    quarter = size_t // 4
    for part in range(4):
        own = pl.ds(part * quarter, quarter)
        for t in range(part * quarter, (part + 1) * quarter):
            _, summed = neighbours0(v0s, yl[0, t], yl[1, t], t)
            res[t] = base[t] + summed
        copies.append(pltpu.make_async_copy(res.at[own], res_hbm.at[own], written.at[1 + part]))
        copies[-1].start()
    for copy in copies:
        copy.wait()


def kernel(sizes, s_hbm, m_hbm, v0s, yl, base, *scratch):
    nta, ngz, ngy = sizes
    (g0, v0a, v0b, v0w, v0x, y0, ys0, y2, ys2, yg, ysg, fold,
     s1, m1, g1, v1a, v1b, v1h, v1w, v1x, e1, e2,
     m2, s2, g2, u2, w2, m3, s3, u3, w3,
     s_ref, m_ref, tally, departed, arrived, loaded) = scratch
    size_t, size_z, rows, lanes = s_ref.shape
    size_t1, pairs1, rows1 = size_t // 2, size_z // 4, rows // 2
    part_t, part_z, rows2 = size_t // 4, size_z // 4, rows // 4
    stages = plan(nta, ngz)
    slots = {cell: number for number, cell in enumerate(stages["source"])}
    centred = lambda d, n: (d + n // 2) % n - n // 2
    around2 = lambda cell: [
        ((cell[0] + dt) % nta, (cell[1] + dz) % ngz) for dt, dz in ((-1, 0), (1, 0), (0, -1), (0, 1))
    ]
    close = {cell for cell in slots if abs(centred(cell[0], nta)) <= 4}
    early2 = [cell for cell in stages["swept"] if {cell, *around2(cell)} & set(slots) <= close]
    late2 = [cell for cell in stages["swept"] if cell not in early2]
    early3 = [cell for cell in stages["coarse"][3] if not {cell, *around2(cell)} & set(late2)]
    late3 = [cell for cell in stages["coarse"][3] if cell not in early3]
    slots3 = {cell: number for number, cell in enumerate(early3 + late3)}
    ta, gz, gy = lax.axis_index("ta"), lax.axis_index("gz"), lax.axis_index("gy")

    places = {}

    def place_of(axis, at, step, count):
        key = axis, step % count
        if key not in places:
            places[key] = at if key[1] == 0 else lax.rem(at + key[1], count)
        return places[key]

    def device(dt, dz, dy):
        return {
            "ta": place_of("ta", ta, dt, nta), "gz": place_of("gz", gz, dz, ngz), "gy": place_of("gy", gy, dy, ngy),
        }

    near = [(dt, dz, dy) for dt in (-1, 0, 1) for dz in (-1, 0, 1) for dy in range(ngy)]
    across = sorted(
        (cell for cell in slots if cell != (0, 0)),
        key=lambda c: -(abs(centred(c[0], nta)) + 2 * abs(centred(c[1], ngz))),
    )
    half = size_t // 2
    loads = [
        [
            pltpu.make_async_copy(source.at[pl.ds(part * half, half)], target.at[pl.ds(part * half, half)], loaded.at[part, place])
            for place, (source, target) in enumerate(((m_hbm, m_ref), (s_hbm, s_ref)))
        ]
        for part in range(2)
    ]
    met = {(dt % nta, dz % ngz, dy % ngy) for dt, dz, dy in near + [(-t, -z, 0) for t, z in across]} - {(0, 0, 0)}
    met = sorted(met, key=lambda d: (-abs(centred(d[0], nta)) - 2 * abs(centred(d[1], ngz)) - 2 * d[2], d))
    barrier = pltpu.get_barrier_semaphore()
    for offset in met:
        pl.semaphore_signal(barrier, inc=1, device_id=device(*offset), device_id_type=MESH)
    for load in loads[0] + loads[1]:
        load.start()

    rows_of, all_rows = {}, []

    def send(group, moves):
        for source, target, offset in moves:
            pltpu.make_async_remote_copy(
                src_ref=source, dst_ref=target, send_sem=departed, recv_sem=arrived.at[group],
                device_id=offset if isinstance(offset, dict) else device(*offset), device_id_type=MESH,
            ).start()
            count = 1
            for extent in source.shape[:-1]:
                count *= extent
            rows_of[group] = rows_of.get(group, 0) + count
            all_rows.append(count)
        return group

    def whole(group, count):
        view = tally.at[pl.ds(0, count)]
        return pltpu.make_async_remote_copy(
            src_ref=view, dst_ref=view, send_sem=departed, recv_sem=arrived.at[group],
            device_id=device(1, 0, 0), device_id_type=MESH,
        )

    def finish(group):
        whole(group, rows_of[group]).wait_recv()

    inner_t, inner_z = pl.ds(PAD0, size_t), pl.ds(PAD0, size_z)

    def faces0(field, depth):
        one = lambda at: pl.ds(PAD0 + at, 1)
        return [
            (field.at[inner_t, one(size_z - depth)], field.at[inner_t, one(-depth)], (0, 1, 0)),
            (field.at[inner_t, one(depth - 1)], field.at[inner_t, one(size_z - 1 + depth)], (0, -1, 0)),
            (field.at[one(size_t - depth), inner_z], field.at[one(-depth), inner_z], (1, 0, 0)),
            (field.at[one(depth - 1), inner_z], field.at[one(size_t - 1 + depth), inner_z], (-1, 0, 0)),
        ]

    own_t, own_z = pl.ds(1, size_t), pl.ds(1, size_z)

    def exchange(number, field):
        faces = ys0.at[number]
        low, high = [y0.at[number, side, own_t, own_z] if number < 2 else yl.at[side] for side in range(2)]
        moves = [(faces.at[1], low, (0, 0, 1)), (faces.at[0], high, (0, 0, -1))] + faces0(field, 1)
        return send(2 * number, moves[:4]), send(2 * number + 1, moves[4:])

    def weights_behind():
        moves = [(ysg.at[1], yg.at[0], (0, 0, 1)), (ysg.at[0], yg.at[1], (0, 0, -1))]
        return send(6, moves + faces0(g0, 1))

    def second_behind():
        one = lambda at: pl.ds(at, 1)
        moves = [(ys2.at[1], y2.at[0, 0], (0, 0, 1)), (ys2.at[0], y2.at[0, 1], (0, 0, -1))]
        for up_t in (1, 0):
            for up_z in (1, 0):
                moves.append((
                    v0b.at[one(PAD0 + (size_t - 1) * up_t), one(PAD0 + (size_z - 1) * up_z)],
                    v0b.at[one(PAD0 - 1 + (size_t + 1) * (1 - up_t)), one(PAD0 - 1 + (size_z + 1) * (1 - up_z))],
                    (2 * up_t - 1, 2 * up_z - 1, 0),
                ))
        for up_y in (1, 0):
            faces, halos = ys0.at[1, up_y], y0.at[1, 1 - up_y]
            for up in (1, 0):
                moves.append((
                    faces.at[one((size_t - 1) * up)], halos.at[one((size_t + 1) * (1 - up)), own_z],
                    (2 * up - 1, 0, 2 * up_y - 1),
                ))
                moves.append((
                    faces.at[:, one((size_z - 1) * up)], halos.at[own_t, one((size_z + 1) * (1 - up))],
                    (0, 2 * up - 1, 2 * up_y - 1),
                ))
        return send(7, moves + faces0(v0b, 2))

    def layers1(deep_t, deep_z, corner_t):
        own_t, own_z = pl.ds(PAD_T, size_t1), pl.ds(PAD_Z, pairs1)

        def span(pad, size, deep, up):
            return pl.ds(pad + (size - deep) * up, deep), pl.ds(pad + size - (size + deep) * up, deep)

        moves = []
        for up in (1, 0):
            for up_z in (1, 0):
                here_t, there_t = span(PAD_T, size_t1, corner_t, up)
                here_z, there_z = span(PAD_Z, pairs1, 1, up_z)
                moves.append((here_t, here_z, there_t, there_z, 2 * up - 1, 2 * up_z - 1))
        for up in (1, 0):
            here, there = span(PAD_T, size_t1, deep_t, up)
            moves.append((here, own_z, there, own_z, 2 * up - 1, 0))
            here, there = span(PAD_Z, pairs1, deep_z, up)
            moves.append((own_t, here, own_t, there, 0, 2 * up - 1))
        return moves

    def spread1(number, field):
        part = pl.ds(gy, 1)
        own = field.at[pl.ds(PAD_T, size_t1), pl.ds(PAD_Z, pairs1), part]
        spread = [
            (field.at[here_t, here_z, part], field.at[there_t, there_z, part], (dt, dz, dy))
            for dy in reversed(range(ngy)) for here_t, here_z, there_t, there_z, dt, dz in layers1(2, 1, 2)
        ]
        pair = [(own, own, (0, 0, dy)) for dy in range(1, ngy)]
        moves = spread[:4] + pair + spread[4:]
        return send(8 + number, moves)

    def widen1(field):
        moves = [
            (field.at[here_t, here_z], field.at[there_t, there_z], (dt, dz, 0))
            for here_t, here_z, there_t, there_z, dt, dz in layers1(3, 2, 3)
        ]
        one = lambda at: pl.ds(at, 1)
        for up in (1, 0):
            for up_z in (1, 0):
                moves.append((
                    field.at[one(PAD_T + (size_t1 - 1) * up), one(PAD_Z + 1 + (pairs1 - 3) * up_z)],
                    field.at[one(PAD_T - 1 + (size_t1 + 1) * (1 - up)), one(PAD_Z - 2 + (pairs1 + 3) * (1 - up_z))],
                    (2 * up - 1, 2 * up_z - 1, 0),
                ))
        return send(10, moves)

    def gather(group, field, cells):
        own = field.at[slots[0, 0]]
        return send(group, [(own, field.at[slots[cell]], (-cell[0], -cell[1], 0)) for cell in cells])

    core = lax.rem(ta, 2)
    even = [cell for cell in across if cell[0] % 2 == 0]

    def relay(field):
        sibling = {"ta": ta + 1 - 2 * core, "gz": gz, "gy": gy}
        count = len(slots) // ngz // 2
        return send(13, [
            (
                field.at[pl.ds((2 * number + 2 - 2 * core) * ngz, ngz)],
                field.at[pl.ds((2 * number + 1) * ngz, ngz)], sibling,
            )
            for number in range(count)
        ])

    def put(field, faces, t, slab):
        field[PAD0 + t, inner_z] = slab
        faces[0, t] = slab[:, :1]
        faces[1, t] = slab[:, rows - 1:]

    def sum0(field, halos, t, reach=0):
        count = size_z + 2 * reach
        out = pl.ds(1 - reach, count)
        return neighbours0(field, halos[0, 1 + t, out], halos[1, 1 + t, out], t, -reach, count)

    def folded(summed, place):
        count, high, _ = summed.shape
        view = fold.at[place, pl.ds(0, count)]
        view[...] = summed
        return view[:, pl.ds(0, high // 2, stride=2), :] + view[:, pl.ds(1, high // 2, stride=2), :]

    def to_level1(summed, place):
        summed = folded(z_pairs(summed), place)
        summed = summed.reshape(summed.shape[0] // 2, 2, *summed.shape[1:])
        even, odd = summed[:, 0], summed[:, 1]
        even, odd = even + rolled(even, -1, 2), odd + rolled(odd, 1, 2)
        return jnp.where(odd_lane(even), odd, even) * 0.0625

    def doubled(slab, place):
        count, high, _ = slab.shape
        view = fold.at[place, pl.ds(0, count)]
        view[:, pl.ds(0, high, stride=2), :] = slab
        view[:, pl.ds(1, high, stride=2), :] = slab
        return view[...]

    full = ngy * rows1

    def area1(*reaches):
        far = len(reaches) - 1
        for t in range(-far, size_t1 + far):
            reach = reaches[max(-t, t - size_t1 + 1, 0)]
            yield t, -reach, pairs1 + 2 * reach

    def read1(field, t, z, count):
        return field[PAD_T + t, pl.ds(PAD_Z + z, count)].reshape(count, full, lanes)

    def write1(field, t, z, slab):
        field[PAD_T + t, pl.ds(PAD_Z + z, slab.shape[0])] = slab.reshape(slab.shape[0], ngy, rows1, lanes)

    def sum1(field, t, z, count, held):
        slab = read1(field, t, z, count)
        summed = read1(field, t - 1, z, count) + read1(field, t + 1, z, count)
        if held[t][0] < z:
            before, after = read1(field, t, z - 1, count), read1(field, t, z + 1, count)
        else:
            before = jnp.concatenate([slab[:1], slab[:-1]], axis=0)
            after = jnp.concatenate([slab[1:], slab[-1:]], axis=0)
        summed = summed + jnp.where(odd_lane(slab), rolled(slab + after, 1, 2), rolled(slab + before, -1, 2))
        summed = summed + rolled(slab, 1, 1) + rolled(slab, -1, 1)
        return slab, summed + rolled(slab, 2, 2) + rolled(slab, -2, 2)

    def sweep1(field, out, area, held):
        held = {t: (z, count) for t, z, count in area1(*held)}
        for t, z, count in area1(*area):
            slab, summed = sum1(field, t, z, count, held)
            fresh = KEEP * slab + read1(g1, t, z, count) * (read1(s1, t, z, count) + 0.5 * summed)
            write1(out, t, z, fresh)

    def packed(out, slabs):
        parts = [slab[z] for slab in slabs for z in range(part_z)]
        lane = lax.broadcasted_iota(jnp.int32, parts[0].shape, 1)
        values = parts[0]
        for k in range(1, len(parts)):
            values = jnp.where(lane % 4 == k, parts[k], values)
        out[slots[0, 0]] = values

    inside = list(range(1, size_t - 1))
    ends = [0, size_t - 1]

    for part in range(2):
        for load in loads[part]:
            load.wait()
        for t in range(part * half, (part + 1) * half):
            weight = DAMPING / (8.0 + m_ref[t])
            put(g0, ysg, t, weight)
            put(v0a, ys0.at[0], t, weight * s_ref[t])

    pl.semaphore_wait(barrier, len(met))
    sides, over_t = exchange(0, v0a)
    for t in range(size_t1):
        m1[PAD_T + t, pl.ds(PAD_Z, pairs1), gy] = to_level1(m_ref[2 * t] + m_ref[2 * t + 1], t)

    def sweep0(field, halos, out, faces, ts):
        for t in ts:
            slab, summed = sum0(field, halos, t)
            fresh = KEEP * slab + g0[PAD0 + t, inner_z] * (s_ref[t] + summed)
            put(out, faces, t, fresh)

    finish(sides)
    sweep0(v0a, y0.at[0], v0b, ys0.at[1], inside)
    finish(over_t)
    sweep0(v0a, y0.at[0], v0b, ys0.at[1], ends)
    for t in range(size_t):
        ys2[0, t] = v0b[PAD0 + t, inner_z, pl.ds(1, 1)]
        ys2[1, t] = v0b[PAD0 + t, inner_z, pl.ds(rows - 2, 1)]
    sides, over_t = exchange(1, v0b)
    mass_copies = spread1(0, m1)

    def to_level2(slabs):
        out = []
        for t in range(part_t):
            summed = folded(slabs[2 * t] + slabs[2 * t + 1], t)
            summed = summed + pair_swap(summed, 1, 2)
            out.append((summed + pair_swap(summed, 2, 2)) * 0.0625)
        return out


    def remainder0(ts):
        for t in ts:
            remainder = []
            for odd in range(2):
                slab, summed = sum0(v0b, y0.at[1], 2 * t + odd)
                remainder.append(s_ref[2 * t + odd] + summed - (8.0 + m_ref[2 * t + odd]) * slab)
            s1[PAD_T + t, pl.ds(PAD_Z, pairs1), gy] = to_level1(remainder[0] + remainder[1], t)

    finish(sides)
    remainder0(range(1, size_t1 - 1))
    finish(over_t)
    remainder0((0, size_t1 - 1))
    source_copies = spread1(1, s1)
    finish(mass_copies)
    for a, b, count in area1(1, 1, 1):
        write1(g1, a, b, DAMPING / (4.0 + read1(m1, a, b, count)))
    packed(m2, to_level2([read1(m1, t, 0, pairs1) for t in range(size_t1)]))
    mass_copies = gather(11, m2, even)
    weight_copies = weights_behind()
    def take(field, places, cells):
        return jnp.stack([field[places[cell]] for cell in cells])

    def put3(field, cells, values):
        field[pl.ds(slots3[cells[0]], len(cells))] = values

    finish(source_copies)

    for a, b, count in area1(1, 1, 0):
        write1(v1a, a, b, read1(g1, a, b, count) * read1(s1, a, b, count))
    sweep1(v1a, v1b, (1, 0), (1, 1, 0))
    remainder = []
    held = {t: (z, count) for t, z, count in area1(1, 0)}
    for a, b, count in area1(0):
        slab, summed = sum1(v1b, a, b, count, held)
        write1(v1h, a, b, slab)
        remainder.append(
            read1(s1, a, b, count) + 0.5 * summed - (4.0 + read1(m1, a, b, count)) * slab
        )
    packed(s2, to_level2(remainder))
    late_copies = gather(12, s2, [cell for cell in across if cell not in close])
    source_copies = gather(14, s2, [cell for cell in across if cell in close])
    wide_copies = widen1(v1h)
    finish(mass_copies)
    mass_copies = relay(m2)
    behind_copies = second_behind()
    finish(mass_copies)
    for cell in stages["source"]:
        g2[slots[cell]] = DAMPING / (2.0 + m2[slots[cell]])
    for cells in batches(early3 + late3, 24):
        put3(m3, cells, DAMPING / (1.0 + coarsened3(take(m2, slots, cells))))

    def sum2(field, cell):
        slab = field[slots[cell]]
        before_t, after_t, before_z, after_z = [
            slab + field[slots[other]] if other in slots else slab for other in around2(cell)
        ]
        lane = place_in(slab, 1)
        summed = jnp.where(lane % 4 >= 2, rolled(after_t, 2, 1), rolled(before_t, -2, 1))
        summed = summed + jnp.where(lane % 2 == 1, rolled(after_z, 1, 1), rolled(before_z, -1, 1))
        summed = summed + rolled(slab, 1, 0) + rolled(slab, -1, 0)
        return slab, summed + rolled(slab, 4, 1) + rolled(slab, -4, 1)

    def sweep2(field, out, cells):
        for cell in cells:
            slab, summed = sum2(field, cell)
            at = slots[cell]
            out[at] = KEEP * slab + g2[at] * (s2[at] + 0.25 * summed)

    def down(cells, swept, coarse):
        for cell in cells:
            at = slots[cell]
            u2[at] = g2[at] * s2[at]
            w2[at] = u2[at]
        sweep2(u2, w2, swept)
        for cell in coarse:
            slab, summed = sum2(w2, cell)
            at = slots[cell]
            s3[slots3[cell]] = s2[at] + 0.25 * summed - (2.0 + m2[at]) * slab
        for part in batches(coarse, 24):
            source = coarsened3(take(s3, slots3, part))
            put3(s3, part, source)
            put3(u3, part, take(m3, slots3, part) * source)

    finish(source_copies)
    down([cell for cell in slots if cell in close], early2, early3)
    finish(late_copies)
    down([cell for cell in slots if cell not in close], late2, late3)
    old, new = u3, w3
    for steps in (2, 1, 0):
        for cells in batches(stages["coarse"][steps], 13):
            slab = take(old, slots3, cells)
            near3 = list(zip(*[around2(cell) for cell in cells]))
            summed = take(old, slots3, near3[0]) + take(old, slots3, near3[1])
            summed = summed + take(old, slots3, near3[2]) + take(old, slots3, near3[3])
            summed = summed + rolled(slab, 2, 1) + rolled(slab, -2, 1)
            summed = summed + rolled(slab, 8, 2) + rolled(slab, -8, 2)
            fresh = KEEP * slab + take(m3, slots3, cells) * (take(s3, slots3, cells) + 0.125 * summed)
            for number, cell in enumerate(cells):
                new[slots3[cell]] = fresh[number]
        old, new = new, old
    for cells in batches(stages["base"], 24):
        fine = refined3(take(old, slots3, cells))
        for number, cell in enumerate(cells):
            w2[slots[cell]] = w2[slots[cell]] + fine[number]
    for cell in stages["base"]:
        u2[slots[cell]] = w2[slots[cell]]
    sweep2(w2, u2, stages["first"])
    sweep2(u2, w2, stages["last"])

    def correct1(t, z):
        piece = piece2(w2[slots[t // 2 % nta, z // 2 % ngz]], t % 2, z % 2)
        e2[t + 2, z + 2, pl.ds(0, full // 2, stride=2), :] = piece
        e2[t + 2, z + 2, pl.ds(1, full // 2, stride=2), :] = piece

    for t in range(-2, part_t + 2):
        for z in range(-2, part_z + 2):
            if max(-t, t - part_t + 1, 0) + max(-z, z - part_z + 1, 0) <= 3:
                correct1(t, z)
    finish(wide_copies)
    for t, z, count in area1(2, 2, 1, 1):
        write1(v1w, t, z, read1(v1h, t, z, count) + e2[t // 2 + 2, pl.ds(z + 2, count)])
    sweep1(v1w, v1x, (1, 1, 1), (2, 2, 1, 1))
    sweep1(v1x, e1, (1, 1), (1, 1, 1))

    under = lax.rem(gy + ngy - 1, ngy)
    over = lax.rem(gy + 1, ngy)

    def split1(slab):
        even = jnp.where(odd_lane(slab), rolled(slab, 1, 2), slab)
        odd = jnp.where(odd_lane(slab), slab, rolled(slab, -1, 2))
        return jnp.stack([even, odd], axis=1).reshape(2 * slab.shape[0], *slab.shape[1:])

    def corrected0(level):
        fine = split1(e1[PAD_T + level, pl.ds(PAD_Z - 1, pairs1 + 2), gy])[1:-1]
        fine = refined_z(doubled(fine, level % 4))
        beyond = [
            refined_z(split1(e1[PAD_T + level, pl.ds(PAD_Z - 1, pairs1 + 2), side, pl.ds(row, 1)])[1:-1])
            for side, row in ((under, rows1 - 1), (over, 0))
        ]
        for t in (2 * level, 2 * level + 1):
            reach = 2 - max(-t, t - size_t + 1, 0)
            out = pl.ds(PAD0 - reach, size_z + 2 * reach)
            v0w[PAD0 + t, out] = v0b[PAD0 + t, out] + fine[2 - reach:size_z + 2 + reach]
            reach -= 1
            if reach < 0:
                continue
            out = pl.ds(1 - reach, size_z + 2 * reach)
            for side in range(2):
                shifted = beyond[side][2 - reach:size_z + 2 + reach]
                y0[2, side, 1 + t, out] = y0[1, side, 1 + t, out] + shifted
                if reach == 1:
                    y2[1, side, t] = y2[0, side, t] + beyond[side][2:size_z + 2]

    finish(weight_copies)
    finish(behind_copies)
    for level in range(-1, size_t1 + 1):
        corrected0(level)
    for t in range(-1, size_t + 1):
        reach = 1 if 0 <= t < size_t else 0
        out = pl.ds(PAD0 - reach, size_z + 2 * reach)
        slab, summed = sum0(v0w, y0.at[2], t, reach)
        v0x[PAD0 + t, out] = KEEP * slab + v0a[PAD0 + t, out] + g0[PAD0 + t, out] * summed
    for t in range(size_t):
        for side, row in ((0, 0), (1, rows - 1)):
            at = lambda dt, dz: y0[2, side, 1 + t + dt, pl.ds(1 + dz, size_z)]
            slab = at(0, 0)
            summed = at(-1, 0) + at(1, 0) + at(0, -1) + at(0, 1)
            summed = summed + y2[1, side, t] + v0w[PAD0 + t, inner_z, pl.ds(row, 1)]
            summed = summed + rolled(slab, 1, 2) + rolled(slab, -1, 2)
            y0[3, side, 1 + t, own_z] = KEEP * slab + y0[0, side, 1 + t, own_z] + yg[side, t] * summed
    sweep0(v0x, y0.at[3], v0s, ys0.at[2], range(size_t))
    sides, over_t = exchange(2, v0s)

    for t in range(size_t):
        base[t] = s_ref[t] - (8.0 + m_ref[t]) * v0s[PAD0 + t, inner_z]
    finish(sides)
    finish(over_t)
    whole(0, sum(all_rows)).wait_send()


def place_in(values, axis):
    return lax.broadcasted_iota(jnp.int32, values.shape, axis)


def coarsened3(values):
    for step in (1, 2, 4):
        values = values + rolled(values, -step, 2)
    return (values + rolled(values, -1, 1)) * 0.0625


def refined3(values):
    corner = (place_in(values, 2) % 8 == 0) & (place_in(values, 1) % 2 == 0)
    values = jnp.where(corner, values, 0.0)
    values = values + rolled(values, 1, 1)
    for step in (1, 2, 4):
        values = values + rolled(values, step, 2)
    return values


def piece2(values, odd_t, odd_z):
    values = jnp.where(place_in(values, 1) % 4 == 2 * odd_t + odd_z, values, 0.0)
    values = values + rolled(values, -1 if odd_z else 1, 1)
    return values + rolled(values, -2 if odd_t else 2, 1)


def batches(cells, most):
    count = -(-len(cells) // most)
    size = -(-len(cells) // count)
    return [cells[at:at + size] for at in range(0, len(cells), size)]


def grown(cells, steps, count_t, count_z):
    for _ in range(steps):
        cells = cells | {
            ((t + dt) % count_t, (z + dz) % count_z)
            for t, z in cells for dt, dz in ((-1, 0), (1, 0), (0, -1), (0, 1))
        }
    return cells


def plan(nta, ngz):
    sites = lambda cells, steps: grown(cells, steps, 2 * nta, 2 * ngz)
    blocks = lambda cells: {(t // 2, z // 2) for t, z in cells}
    inner = lambda cells: {(2 * t + a, 2 * z + b) for t, z in cells for a in (0, 1) for b in (0, 1)}
    box = {(t % (2 * nta), z % (2 * ngz)) for t in range(-2, 4) for z in range(-2, 4)}
    last = sites(inner({(0, 0)}), 3) & box
    first, base = sites(last, 1), sites(last, 2)
    coarse = [grown(blocks(base), steps, nta, ngz) for steps in range(4)]
    swept = sites(inner(coarse[3]), 1) | base
    ordered = lambda cells: sorted(cells, key=lambda c: ((c[0] + nta // 2) % nta, (c[1] + ngz // 2) % ngz))
    return {
        "last": ordered(blocks(last)), "first": ordered(blocks(first)), "base": ordered(blocks(base)),
        "coarse": [ordered(cells) for cells in coarse], "swept": ordered(blocks(swept)),
        "source": ordered(blocks(sites(swept, 1))),
    }


def per_device(sizes, right_side, mass_field):
    nta, ngz, ngy = sizes
    size_t, size_z, rows, lanes = right_side.shape
    size_t1, pairs1, rows1 = size_t // 2, size_z // 4, rows // 2
    part_t, part_z, rows2 = size_t // 4, size_z // 4, rows // 4
    vmem = lambda *shape: pltpu.VMEM(shape, jnp.float32)
    dma = lambda *shape: pltpu.SemaphoreType.DMA(shape)
    padded0 = vmem(size_t + 2 * PAD0, size_z + 2 * PAD0, rows, lanes)
    faces = vmem(2, size_t, size_z, 1, lanes)
    padded1 = vmem(size_t1 + 2 * PAD_T, pairs1 + 2 * PAD_Z, ngy, rows1, lanes)
    window = len(plan(nta, ngz)["source"])
    packs = vmem(window, rows2 * ngy, lanes)
    packs3 = vmem(len(plan(nta, ngz)["coarse"][3]), rows2 * ngy, lanes)
    scratch = [
        *[padded0] * 5,
        vmem(4, 2, size_t + 2, size_z + 2, 1, lanes), vmem(3, 2, size_t, size_z, 1, lanes),
        vmem(2, 2, size_t, size_z, 1, lanes), faces, faces, faces,
        vmem(max(size_t1, part_t + 2), size_z, max(rows, ngy * rows1), lanes),
        *[padded1] * 9, vmem(part_t + 4, part_z + 4, ngy * rows1, lanes),
        *[packs] * 5, *[packs3] * 4,
        vmem(size_t, size_z, rows, lanes), vmem(size_t, size_z, rows, lanes),
        vmem(8192, 1, lanes), pltpu.SemaphoreType.DMA, dma(15), dma(2, 2),
    ]
    array = lambda *shape: jax.ShapeDtypeStruct(shape, jnp.float32)
    block, place = array(*right_side.shape), pl.BlockSpec(memory_space=pltpu.VMEM)
    kept = pl.pallas_call(
        functools.partial(kernel, sizes),
        out_shape=(
            array(size_t + 2 * PAD0, size_z + 2 * PAD0, rows, lanes), array(2, size_t, size_z, 1, lanes), block,
        ),
        in_specs=[pl.BlockSpec(memory_space=pltpu.HBM)] * 2,
        out_specs=(place,) * 3,
        scratch_shapes=scratch,
        compiler_params=pltpu.CompilerParams(
            collective_id=0, has_side_effects=True, vmem_limit_bytes=48 * 1024 * 1024
        ),
    )(*[pltpu.with_memory_space_constraint(values, pltpu.HBM) for values in (right_side, mass_field)])
    return pl.pallas_call(
        last_kernel,
        out_shape=(block, block),
        in_specs=[place] * 3,
        out_specs=(pl.BlockSpec(memory_space=pltpu.HBM),) * 2,
        scratch_shapes=[vmem(size_t, size_z, rows, lanes), dma(5)],
        compiler_params=pltpu.CompilerParams(vmem_limit_bytes=8 * 1024 * 1024),
    )(*kept)


def solution(mesh):
    sizes = tuple(mesh.shape[axis] for axis in ("ta", "gz", "gy"))
    spec = P("ta", "gz", "gy", None)
    return jax.shard_map(
        functools.partial(per_device, sizes),
        mesh=mesh,
        in_specs=(spec, spec),
        out_specs=(spec, spec),
        check_vma=False,
    )
```
